32 devices in a mesh: tok: 16 (over z, y, core), tp: 2 (over x).
Axes of the slice: x: 2, y: 2, z: 4, core: 2. Of those that a mesh axis runs over, the one named last changes fastest.
Arguments:
- hidden: bfloat16 [1536, 8192], P('tok'), may hold values from -2600 to 2600
- norm_gain: float32 [8192], replicated, may hold values from 0.5 to 1.5
- w_query: bfloat16 [8192, 4096], P('tok', 'tp'), may hold values from -1 to 1
- w_key: bfloat16 [8192, 1024], P('tok', 'tp'), may hold values from -1 to 1
- w_value: bfloat16 [8192, 1024], P('tok', 'tp'), may hold values from -0.0625 to 0.0625
- doc_ids: int32 [1536], P('tok'), may hold values from 0 to 3, as said below
Outputs:
- attended: bfloat16 [1536, 4096], P('tok', 'tp')
- out_scale: float32 [4096], P('tp')
- folded_gain: float32 [8192], P(('tok', 'tp'))
- codes_query: float32 [8192, 4096], P(('tok', 'tp'))
- codes_key: float32 [8192, 1024], P(('tok', 'tp'))
- codes_value: float32 [8192, 1024], P(('tok', 'tp'))
- scale_query: float32 [4096], P('tp')
- scale_key: float32 [1024], P('tp')
- scale_value: float32 [1024], P('tp')
The draws below stay inside these ranges and needn't reach their ends.
Inputs may be any that keep to these rules, and one draw needn't show every extreme that they name: doc_ids never falls along the tokens; each of the 4 documents holds 1 to 1152 tokens and one holds exactly 1152.
All inputs are finite; a program needn't handle non-finite values. Where the reference program divides by a largest or mean magnitude, that divisor is 1e-20 or more.
Results may differ from the reference program's by a relative error of at most 0.005.
The reference program's roundings to bfloat16 on the way (of `normed` and `value`) count: a program that leaves them out, or rounds other values in their place, can miss the bound.
Values may be sent and summed in bfloat16 or wider, within the bound.
A program may use at most 128 MiB of HBM per device.

```python
import math
import jax
import jax.numpy as jnp
from jax import lax

D = 8192
HEAD = 128
KVH = 8
QHEADS = 32
DOCS = 4
TOKENS = 1536
DOC_MOST = 1152


pair_count = 6


strengths = (0.75, 0.55, 0.35, 0.75, 0.55, 0.35)


planted_entry = 1.0


def document_layout(key):
    folded = jax.random.fold_in(key, 5151)
    key_where, key_cuts = jax.random.split(folded, 2)
    short_total = TOKENS - DOC_MOST
    long_place = jax.random.randint(key_where, (), 0, DOCS)
    cut_order = jax.random.permutation(key_cuts, short_total - 1)[:DOCS - 2] + 1
    cuts = jnp.sort(cut_order)
    bounds = jnp.concatenate([jnp.zeros((1,), jnp.int32), cuts.astype(jnp.int32), jnp.full((1,), short_total, jnp.int32)])
    shorts = bounds[1:] - bounds[:-1]
    order = jnp.arange(DOCS, dtype=jnp.int32)
    short_index = jnp.clip(order - (order > long_place).astype(jnp.int32), 0, DOCS - 2)
    lengths = jnp.where(order == long_place, DOC_MOST, shorts[short_index]).astype(jnp.int32)
    ends = jnp.cumsum(lengths).astype(jnp.int32)
    long_start = ends[long_place] - DOC_MOST
    return (ends, long_start)


def planted_layout(key):
    folded = jax.random.fold_in(key, 4242)
    key_perm, key_place, key_sign = jax.random.split(folded, 3)
    channels = jax.random.permutation(key_perm, D)[:3 * pair_count]
    ends, long_start = document_layout(key)
    stride = TOKENS // 4 // pair_count
    offsets = jax.random.randint(key_place, (pair_count,), 1, stride)
    later = long_start + TOKENS // 2 + jnp.arange(pair_count, dtype=jnp.int32) * stride + offsets
    reach = jnp.where(jnp.arange(pair_count) % 2 == 0, TOKENS // 2, 1)
    earlier = later - reach
    signs = jnp.where(jax.random.bernoulli(key_sign, 0.5, (KVH, HEAD)), 1.0, -1.0)
    half_head = HEAD // 2
    band_size = max(HEAD // 32, 2)
    band_start = half_head - band_size
    within = jnp.arange(HEAD) % half_head
    band = ((within >= band_start) & (within < band_start + band_size)).astype(jnp.float32)
    return (channels, later, earlier, signs * band[None, :])


def draw_doc_ids(key, part):
    ends, long_start = document_layout(key)
    token_index = jnp.arange(TOKENS, dtype=jnp.int32)
    return jnp.sum((token_index[:, None] >= ends[None, :DOCS - 1]).astype(jnp.int32), axis=1).astype(jnp.int32)


def main_rows(channels):
    row_index = jnp.arange(D)[:, None]
    is_main = jnp.any(row_index == channels[None, :pair_count], axis=1)
    is_extra = jnp.any(row_index == channels[None, pair_count:], axis=1)
    return (is_main, is_extra)


def drawn_weight(key, salt, columns):
    values = jnp.clip(jax.random.normal(jax.random.fold_in(key, salt), (D, columns), jnp.float32), -4.0, 4.0) / math.sqrt(D)
    return jnp.clip(values, -planted_entry, planted_entry)


def draw_w_query(key, part):
    values = drawn_weight(key, 11, QHEADS * HEAD)
    channels, later, earlier, pattern = planted_layout(key)
    is_main, is_extra = main_rows(channels)
    pattern_row = jnp.repeat(pattern, QHEADS // KVH, axis=0).reshape(QHEADS * HEAD)
    values = jnp.where(is_main[:, None], pattern_row[None, :], jnp.where(is_extra[:, None], 0.0, values))
    return values.astype(jnp.bfloat16)


def draw_w_key(key, part):
    values = drawn_weight(key, 12, KVH * HEAD)
    channels, later, earlier, pattern = planted_layout(key)
    is_main, is_extra = main_rows(channels)
    pattern_row = pattern.reshape(KVH * HEAD)
    values = jnp.where(is_main[:, None], pattern_row[None, :], jnp.where(is_extra[:, None], 0.0, values))
    return values.astype(jnp.bfloat16)


def draw_norm_gain(key, part):
    key_gain = jax.random.fold_in(key, 31)
    channels, later, earlier, pattern = planted_layout(key)
    is_main, is_extra = main_rows(channels)
    nearby = jax.random.uniform(jax.random.fold_in(key, 32), (D,), jnp.float32, 0.95, 1.05)
    spread = 1.0 + 0.1 * jnp.clip(jax.random.normal(key_gain, (D,), jnp.float32), -5.0, 5.0)
    return jnp.where(is_main, nearby, spread)


def draw_hidden(key, part):
    key_base, key_channel = jax.random.split(key, 2)
    base = jnp.clip(jax.random.normal(key_base, (TOKENS, D), jnp.float32), -4.0, 4.0)
    channels, later, earlier, pattern = planted_layout(key)
    column_index = jnp.arange(D)[None, :]
    main_hot = (column_index == channels[:pair_count, None]).astype(jnp.float32)
    is_main_column = jnp.sum(main_hot, axis=0, keepdims=True) > 0.5
    channel = jnp.exp(jax.random.uniform(key_channel, (1, D), jnp.float32, 0.0, math.log(30.0)))
    channel = jnp.where(is_main_column, 1.0, channel)
    values = base * channel
    token_index = jnp.arange(TOKENS)[:, None]
    is_later = (token_index == later[None, :]).astype(jnp.float32)
    is_earlier = (token_index == earlier[None, :]).astype(jnp.float32)
    late_hot = (column_index == channels[pair_count:2 * pair_count, None]).astype(jnp.float32)
    early_hot = (column_index == channels[2 * pair_count:, None]).astype(jnp.float32)
    levels = jnp.array(strengths, jnp.float32)
    main_amp = jnp.sqrt(levels)[:, None]
    rest_amp = jnp.sqrt(1.0 - levels - 0.0025)[:, None]
    late_rows = main_amp * main_hot + rest_amp * late_hot
    early_rows = main_amp * main_hot + rest_amp * early_hot
    planted = math.sqrt(D) * (jnp.dot(is_later, late_rows, precision=lax.Precision.HIGHEST) + jnp.dot(is_earlier, early_rows, precision=lax.Precision.HIGHEST))
    chosen = jnp.sum(is_later + is_earlier, axis=1) > 0.5
    values = jnp.where(chosen[:, None], 0.05 * base + planted, values)
    return jnp.clip(values, -2600.0, 2600.0).astype(jnp.bfloat16)


def block_levels(key, shape, shards, smallest, top_value):
    def one(position, shards_of):
        heights = jax.random.uniform(jax.random.fold_in(jax.random.fold_in(key, 6), position), (shards_of,), jnp.float32, smallest / len(shards), top_value / len(shards))
        return jnp.repeat(jnp.exp(heights), shape[position] // shards_of).reshape((-1,) + (1,) * (len(shape) - position - 1))

    factor_of = one(*shards[0])
    for cut in shards[1:]:
        factor_of = factor_of * one(*cut)
    return factor_of


def normal_values(stream_key, shape, width, limit, shards=(), kind=jnp.bfloat16):
    values = jax.random.normal(stream_key, shape, jnp.float32) * width
    if len(shards) > 0:
        values = block_levels(stream_key, shape, shards, -0.22, 0.18) * values
    return jnp.clip(values, min=-limit, max=limit).astype(kind)


def setup_inputs(seed: int = 0) -> dict:
    key_list = jax.random.split(jax.random.key(seed), 7)
    hidden = draw_hidden(jax.random.fold_in(key_list[6], 71), 0)
    norm_gain = draw_norm_gain(jax.random.fold_in(key_list[6], 71), 0)
    w_query = draw_w_query(jax.random.fold_in(key_list[6], 71), 0)
    w_key = draw_w_key(jax.random.fold_in(key_list[6], 71), 0)
    w_value = normal_values(key_list[4], (D, KVH * HEAD), D ** -0.5, 0.0625, ((0, 16), (1, 2)))
    doc_ids = draw_doc_ids(jax.random.fold_in(key_list[6], 71), 0)
    return dict(hidden=hidden, norm_gain=norm_gain, w_query=w_query, w_key=w_key, w_value=w_value, doc_ids=doc_ids)


def rotate(states, positions):
    half = states.shape[-1] // 2
    inverse = jnp.exp(jnp.arange(half, dtype=jnp.float32) * (-2.0 * math.log(10000.0) / states.shape[-1]))
    angles = positions[:, None] * inverse[None, :]
    cosine = jnp.cos(angles)[:, None, :]
    sine = jnp.sin(angles)[:, None, :]
    first = states[..., :half]
    second = states[..., half:]
    return jnp.concatenate([first * cosine - second * sine, second * cosine + first * sine], axis=-1)

def quantize(smoothing, matrix):
    smoothed = smoothing[:, None] * matrix.astype(jnp.float32)
    column_scale = jnp.maximum(lax.optimization_barrier(jnp.max(jnp.abs(smoothed), axis=0)), 1e-05) / 127.0
    return (smoothed / column_scale[None, :], column_scale)

def reference(hidden, norm_gain, w_query, w_key, w_value, doc_ids):
    tokens = hidden.shape[0]
    states = hidden.astype(jnp.float32)
    normed = (states * lax.rsqrt(lax.optimization_barrier(jnp.mean(states * states, axis=1, keepdims=True)) + 1e-05) * norm_gain[None, :]).astype(jnp.bfloat16)
    input_peak = lax.optimization_barrier(jnp.max(jnp.abs(normed.astype(jnp.float32)), axis=0))
    positions = jnp.arange(tokens, dtype=jnp.float32)
    query = rotate(jnp.dot(normed, w_query, preferred_element_type=jnp.float32).reshape(tokens, QHEADS, HEAD), positions).astype(jnp.bfloat16)
    key = rotate(jnp.dot(normed, w_key, preferred_element_type=jnp.float32).reshape(tokens, KVH, HEAD), positions).astype(jnp.bfloat16)
    value = jnp.dot(normed, w_value, preferred_element_type=jnp.float32).astype(jnp.bfloat16).reshape(tokens, KVH, HEAD)
    group_size = QHEADS // KVH
    index = jnp.arange(tokens, dtype=jnp.int32)
    allowed = (doc_ids[:, None] == doc_ids[None, :]) & (index[None, :] <= index[:, None])
    score_scale = 1.0 / math.sqrt(HEAD)

    def one_head(head_index):
        query_head = lax.dynamic_index_in_dim(query, head_index, 1, keepdims=False)
        key_head = lax.dynamic_index_in_dim(key, head_index // group_size, 1, keepdims=False)
        value_head = lax.dynamic_index_in_dim(value, head_index // group_size, 1, keepdims=False)
        scores = jnp.dot(query_head, key_head.T, preferred_element_type=jnp.float32) * score_scale
        scores = jnp.where(allowed, scores, -1e+30)
        highest = lax.optimization_barrier(jnp.max(scores, axis=1, keepdims=True))
        weights = jnp.where(allowed, jnp.exp(scores - highest), 0.0)
        totals = lax.optimization_barrier(jnp.sum(weights, axis=1, keepdims=True))
        return jnp.dot(weights.astype(jnp.bfloat16), value_head, preferred_element_type=jnp.float32) / totals
    heads = lax.map(one_head, jnp.arange(QHEADS, dtype=jnp.int32))
    attended = heads.transpose(1, 0, 2).reshape(tokens, QHEADS * HEAD).astype(jnp.bfloat16)
    out_scale = lax.optimization_barrier(jnp.max(jnp.abs(attended.astype(jnp.float32)), axis=0))
    weight_peak = jnp.maximum(jnp.maximum(lax.optimization_barrier(jnp.max(jnp.abs(w_query.astype(jnp.float32)), axis=1)), lax.optimization_barrier(jnp.max(jnp.abs(w_key.astype(jnp.float32)), axis=1))), lax.optimization_barrier(jnp.max(jnp.abs(w_value.astype(jnp.float32)), axis=1)))
    smoothing = jnp.sqrt(jnp.maximum(input_peak, 1e-05)) / jnp.sqrt(jnp.maximum(weight_peak, 1e-05))
    folded_gain = norm_gain / smoothing
    codes_query, scale_query = quantize(smoothing, w_query)
    codes_key, scale_key = quantize(smoothing, w_key)
    codes_value, scale_value = quantize(smoothing, w_value)
    return (attended, out_scale, folded_gain, codes_query, codes_key, codes_value, scale_query, scale_key, scale_value)
```

```python
import functools
import math

import jax
import jax.numpy as jnp
from jax import lax
from jax.experimental import pallas as pl
from jax.experimental.pallas import tpu as pltpu
from jax.sharding import PartitionSpec as P

HEAD = 128
KVH = 8
QHEADS = 32
GROUP = QHEADS // KVH
LANES = 128
FAR = 1 << 30

MESH = pl.DeviceIdType.MESH
QUAD = 4


def column_chunks(widths, most=GROUP * HEAD):
    return [
        (which, start, min(most, widths[which] - start))
        for which in (1, 2, 0)
        for start in range(0, widths[which], most)
    ]


def as_column(row):
    return jnp.transpose(jnp.broadcast_to(row, (LANES, LANES)))

def main_kernel(
    chunks,
    line,
    tp_count,
    share,
    hidden_ref,
    gain_ref,
    doc_ref,
    inverse_ref,
    wq_ref,
    wk_ref,
    wv_ref,
    out_ref,
    out_peak_ref,
    scale_ref,
    folded_ref,
    smooth_ref,
    relaid_ref,
    normed,
    root,
    cosine,
    sine,
    doc_row,
    docs,
    bias,
    tokens,
    mine,
    theirs,
    held_q,
    held_k,
    held_v,
    partial,
    from_left,
    from_right,
    query,
    cache,
    relaid,
    channel,
    column,
    column_tp,
    column_line,
    out_mine,
    out_all,
    w_send,
    w_recv,
    t_send,
    t_recv,
    m_send,
    m_recv,
    x_send,
    x_recv,
    x_local,
    r_send,
    r_recv,
    l_send,
    l_recv,
    p_send,
    p_recv,
    d_send,
    d_recv,
    z_send,
    z_recv,
    y_send,
    y_recv,
    s_send,
    s_recv,
    c_send,
    c_recv,
    b_send,
    b_recv,
    a_send,
    a_recv,
    o_send,
    o_recv,
):
    me = lax.axis_index("tok")
    tp = lax.axis_index("tp")
    tok_count = line * QUAD
    quad = lax.rem(me, QUAD)
    place = me // QUAD
    rows = wq_ref.shape[0]
    tok_dev = hidden_ref.shape[0]
    depth = hidden_ref.shape[1]
    width = QUAD * rows
    keys = tok_dev * tok_count
    sib = me + 1 - 2 * lax.rem(me, 2)
    side = me + 2 - 4 * (quad // 2)
    side_sib = side + 1 - 2 * lax.rem(me, 2)
    own = (wq_ref, wk_ref, wv_ref)
    held = (held_q, held_k, held_v)
    widths = [ref.shape[1] for ref in own]
    sub = rows // tp_count
    count = len(chunks)
    kv_chunks = [c for c in range(count) if chunks[c][0] > 0]
    q_chunks = [c for c in range(count) if chunks[c][0] == 0]
    kv_here = widths[1] // HEAD

    def remote(src, dst, send, recv, tok, tp_to=None):
        return pltpu.make_async_remote_copy(
            src_ref=src,
            dst_ref=dst,
            send_sem=send,
            recv_sem=recv,
            device_id=(tok, tp if tp_to is None else tp_to),
            device_id_type=MESH,
        )

    def rows_of(tok):
        return pl.ds(pl.multiple_of(tok * tok_dev, 16), tok_dev)

    def meet(barrier):
        def greet(step, carry):
            other = lax.rem(me + step, tok_count)
            pl.semaphore_signal(
                barrier, inc=1, device_id=(other, tp), device_id_type=MESH
            )
            return carry

        lax.fori_loop(1, tok_count, greet, 0)
        for step in range(1, tp_count):
            other = lax.rem(tp + step, tp_count)
            pl.semaphore_signal(
                barrier, inc=1, device_id=(me, other), device_id_type=MESH
            )

    def w_copy(kind, c):
        which, start, size = chunks[c]
        cols = pl.ds(start, size)
        if kind == 2:
            src = held[which].at[1, :, cols]
        else:
            src = own[which].at[:, cols]
        return remote(
            src,
            held[which].at[kind, :, cols],
            w_send.at[kind, c],
            w_recv.at[kind, c],
            side if kind == 1 else sib,
        )

    part = tok_dev // share
    piece = lax.rem(tp, share)
    mate = tp + 1 - 2 * piece
    first = pl.multiple_of(piece * part, 16)

    def t_copy(step):
        to = lax.rem(place + step, line)
        return remote(
            normed.at[pl.ds(first, part), pl.ds(pl.multiple_of(to * width, 128), width)],
            tokens.at[pl.ds(pl.multiple_of(place * tok_dev + first, 16), part)],
            t_send.at[step],
            t_recv.at[step],
            to * QUAD + quad,
        )

    def m_copy(step):
        source = lax.rem(place - step + line, line)
        start = pl.multiple_of(source * tok_dev + piece * part, 16)
        got = tokens.at[pl.ds(start, part)]
        return remote(got, got, m_send.at[step], m_recv.at[step], me, mate)

    wide = [sum(widths[:i]) * tp_count for i in range(3)]

    def x_copy(which, step):
        to = lax.rem(tp + step, tp_count)
        size = widths[which]
        src = own[which].at[pl.ds(pl.multiple_of(to * sub, 16), sub)]
        dst = relaid.at[:, pl.ds(pl.multiple_of(wide[which] + tp * size, 128), size)]
        if step == 0:
            return pltpu.make_async_copy(src, dst, x_local.at[which])
        return remote(src, dst, x_send.at[which, step], x_recv.at[which, step], me, to)

    relaid_out = pltpu.make_async_copy(relaid, relaid_ref, x_local.at[3])

    def d_copy(step):
        return remote(
            doc_row,
            docs.at[me],
            d_send.at[step],
            d_recv.at[step],
            lax.rem(me + step, tok_count),
        )

    def p_copy(kind):
        return remote(
            mine,
            theirs.at[kind],
            p_send.at[kind],
            p_recv.at[kind],
            (sib, side, side_sib)[kind],
        )

    def each(copy, act):
        def go(step, carry):
            getattr(copy(step), act)()
            return carry

        lax.fori_loop(1, tok_count, go, 0)

    def normalise(start, size, base):
        def go(i, carry):
            for j in range(4):
                cols = pl.ds(pl.multiple_of(base + (4 * i + j) * LANES, LANES), LANES)
                block = hidden_ref[pl.ds(start, size), cols].astype(jnp.float32)
                block = block * root[pl.ds(start, size), :] * gain_ref[:, cols]
                normed[pl.ds(start, size), cols] = block.astype(jnp.bfloat16)
            return carry

        lax.fori_loop(0, width // (4 * LANES), go, 0)

    barrier = pltpu.get_barrier_semaphore()
    meet(barrier)
    doc_row[...] = jnp.full(doc_row.shape, FAR, jnp.int32)
    doc_row[:, :tok_dev] = doc_ref[...]
    docs[me] = doc_row[...]

    def squares(i, total):
        for j in range(4):
            cols = pl.ds(pl.multiple_of((4 * i + j) * LANES, LANES), LANES)
            block = hidden_ref[:, cols].astype(jnp.float32)
            total = total + block * block
        return total

    total = lax.fori_loop(
        0, depth // (4 * LANES), squares, jnp.zeros((tok_dev, LANES), jnp.float32)
    )
    mean = jnp.sum(total, axis=1, keepdims=True) / depth
    root[...] = jnp.broadcast_to(lax.rsqrt(mean + 1e-05), (tok_dev, LANES))
    pl.semaphore_wait(barrier, tok_count - 1 + tp_count - 1)

    for c in range(count):
        w_copy(1, c).start()
        w_copy(0, c).start()

    def send_tokens(i, carry):
        step = jnp.where(2 * place < line, line - i, i)
        normalise(first, part, lax.rem(place + step, line) * width)
        t_copy(step).start()
        return carry

    lax.fori_loop(1, line, send_tokens, 0)
    normalise(0, tok_dev, place * width)
    tokens[rows_of(place)] = normed[:, pl.ds(pl.multiple_of(place * width, 128), width)]
    each(d_copy, "start")

    positions = me * tok_dev + lax.broadcasted_iota(jnp.int32, (tok_dev, HEAD), 0)
    angles = positions.astype(jnp.float32) * inverse_ref[...]
    lane = lax.broadcasted_iota(jnp.int32, (tok_dev, HEAD), 1)
    cosine[...] = jnp.cos(angles)
    sine[...] = jnp.where(lane < HEAD // 2, -1.0, 1.0) * jnp.sin(angles)

    near = sorted(range(1, line), key=lambda step: min(step, line - step))
    for step in near:
        t_copy(step).wait_recv()
        if share == 2:
            m_copy(step).start()
    for which in (1, 2, 0):
        for step in range(tp_count):
            x_copy(which, step).start()
    if share == 2:
        for step in near:
            m_copy(step).wait_recv()

    base_of = [sum(size for _, _, size in chunks[:c]) for c in range(count)]

    def span(c):
        return slice(base_of[c], base_of[c] + chunks[c][2])

    def block(d):
        return pl.ds(pl.multiple_of(d * tok_dev, 8), tok_dev)

    def right(c, d):
        cols = span(c)
        return remote(
            partial.at[block(d), cols],
            from_left.at[block(d), cols],
            r_send.at[c, d],
            r_recv.at[c, d],
            me + QUAD,
        )

    def left(c, d):
        cols = span(c)
        return remote(
            partial.at[block(d), cols],
            from_right.at[block(d), cols],
            l_send.at[c, d],
            l_recv.at[c, d],
            me - QUAD,
        )

    def add_left(c, d):
        right(c, d).wait_recv()
        cols = span(c)
        partial[block(d), cols] = partial[block(d), cols] + from_left[block(d), cols]

    def add_right(c, d):
        left(c, d).wait_recv()
        cols = span(c)
        partial[block(d), cols] = partial[block(d), cols] + from_right[block(d), cols]

    def first_sends(c):
        @pl.when(place == 0)
        def _():
            def go(i, carry):
                right(c, line - 1 - i).start()
                return carry

            lax.fori_loop(0, line - 1, go, 0)

        @pl.when(place == line - 1)
        def _():
            def go(i, carry):
                left(c, i).start()
                return carry

            lax.fori_loop(0, line - 1, go, 0)

    def reduce_step(c, i):
        to_right = line - 1 - i

        @pl.when((place > 0) & (to_right > place))
        def _():
            add_left(c, to_right)
            right(c, to_right).start()

        @pl.when((place < line - 1) & (i < place))
        def _():
            add_right(c, i)
            left(c, i).start()

    def reduce(c):
        def go(i, carry):
            reduce_step(c, i)
            return carry

        lax.fori_loop(0, line, go, 0)

    def finish(c):
        @pl.when(place > 0)
        def _():
            add_left(c, place)

        @pl.when(place < line - 1)
        def _():
            add_right(c, place)

        which, start, size = chunks[c]
        for head in range(size // HEAD):
            base = base_of[c] + head * HEAD
            states = partial[block(place), base : base + HEAD]
            if which < 2:
                states = (
                    states * cosine[...]
                    + pltpu.roll(states, HEAD // 2, 1) * sine[...]
                )
            at = start + head * HEAD + (widths[1] if which == 2 else 0)
            if which == 0:
                query[:, at : at + HEAD] = states.astype(jnp.bfloat16)
            else:
                cache[rows_of(me), at : at + HEAD] = states.astype(jnp.bfloat16)

    def columns_of(tok):
        return pl.ds(pl.multiple_of(lax.rem(tok, QUAD) * rows, 128), rows)

    def project(c):
        which, start, size = chunks[c]
        cols = slice(start, start + size)
        w_copy(1, c).wait_recv()
        w_copy(2, c).start()
        total = jnp.dot(
            tokens[:, columns_of(me)],
            own[which][:, cols],
            preferred_element_type=jnp.float32,
        )
        total += jnp.dot(
            tokens[:, columns_of(side)],
            held[which][1, :, cols],
            preferred_element_type=jnp.float32,
        )
        w_copy(0, c).wait_recv()
        total += jnp.dot(
            tokens[:, columns_of(sib)],
            held[which][0, :, cols],
            preferred_element_type=jnp.float32,
        )
        w_copy(2, c).wait_recv()
        total += jnp.dot(
            tokens[:, columns_of(side_sib)],
            held[which][2, :, cols],
            preferred_element_type=jnp.float32,
        )
        partial[:, span(c)] = total
        first_sends(c)

    def kv_rows(spot, of_side=False):
        at = lax.rem(side, QUAD) if of_side else quad
        return cache.at[rows_of(spot * QUAD + at)]

    def z_copy(way, step):
        spot = place - step if way == 0 else place + step
        to = me + QUAD if way == 0 else me - QUAD
        got = kv_rows(spot)
        return remote(got, got, z_send.at[way, step], z_recv.at[way, step], to)

    def y_copy(spot):
        got = kv_rows(spot)
        return remote(got, got, y_send.at[spot], y_recv.at[spot], side)

    def y_arrival(spot):
        got = kv_rows(spot, True)
        return remote(got, got, y_send.at[spot], y_recv.at[spot], side)

    def s_copy(spot, of_side):
        got = kv_rows(spot, of_side)
        slot = spot + (line if of_side else 0)
        return remote(got, got, s_send.at[slot], s_recv.at[slot], sib)

    def s_arrival(spot, of_side):
        at = lax.rem(side_sib if of_side else sib, QUAD)
        got = cache.at[rows_of(spot * QUAD + at)]
        slot = spot + (line if of_side else 0)
        return remote(got, got, s_send.at[slot], s_recv.at[slot], sib)

    def has(way, step):
        return place >= step if way == 0 else place + step < line

    def onward(way):
        return place + 1 < line if way == 0 else place > 0

    def kv_start():
        for way in range(2):

            @pl.when(onward(way))
            def _():
                z_copy(way, 0).start()

        y_copy(place).start()
        s_copy(place, False).start()

    def z_arrival(way, step):
        spot = place - step if way == 0 else place + step
        to = me + QUAD if way == 0 else me - QUAD
        got = kv_rows(spot)
        return remote(got, got, z_send.at[way, step - 1], z_recv.at[way, step - 1], to)

    def kv_step(step):
        for way in range(2):

            @pl.when(has(way, step))
            def _():
                z_arrival(way, step).wait_recv()

                @pl.when(onward(way))
                def _():
                    z_copy(way, step).start()

                spot = place - step if way == 0 else place + step
                y_copy(spot).start()
                s_copy(spot, False).start()

    def kv_side():
        def go(spot, carry):
            y_arrival(spot).wait_recv()
            s_copy(spot, True).start()
            return carry

        lax.fori_loop(0, line, go, 0)

    def kv_ready():
        def go(spot, carry):
            s_arrival(spot, False).wait_recv()
            s_arrival(spot, True).wait_recv()
            return carry

        lax.fori_loop(0, line, go, 0)

    def mask():
        each(d_copy, "wait")
        wanted = jnp.transpose(
            jnp.broadcast_to(doc_row[...].astype(jnp.float32), (LANES, LANES))
        )[:tok_dev]

        def go(tok, total):
            before = docs[tok].astype(jnp.float32) < wanted
            return total + jnp.where(before, 1.0, 0.0)

        total = lax.fori_loop(
            0, tok_count, go, jnp.zeros((tok_dev, LANES), jnp.float32)
        )
        since = jnp.sum(total, axis=1, keepdims=True).astype(jnp.int32)
        spot = lax.broadcasted_iota(jnp.int32, (tok_dev, keys), 0) + me * tok_dev
        at = lax.broadcasted_iota(jnp.int32, (tok_dev, keys), 1)
        bias[...] = jnp.where((at >= since) & (at <= spot), 0.0, -1e30)

    turn = math.log2(math.e) / math.sqrt(HEAD)

    def attend(g):
        heads = [
            slice((g * GROUP + h) * HEAD, (g * GROUP + h + 1) * HEAD)
            for h in range(GROUP)
        ]
        asked = jnp.concatenate([query[:, head] for head in heads], axis=0)
        key = cache[:, g * HEAD : (g + 1) * HEAD]
        value = cache[:, (kv_here + g) * HEAD : (kv_here + g + 1) * HEAD]
        scores = lax.dot_general(
            asked, key, (((1,), (1,)), ((), ())), preferred_element_type=jnp.float32
        )
        scores = (
            scores.reshape(GROUP, tok_dev, keys) + bias[...][None]
        ).reshape(GROUP * tok_dev, keys)
        weights = jnp.exp2((scores - jnp.max(scores, axis=1, keepdims=True)) * turn)
        totals = jnp.sum(weights, axis=1, keepdims=True)
        mixed = jnp.dot(
            weights.astype(jnp.bfloat16), value, preferred_element_type=jnp.float32
        )
        mixed = (mixed / totals).astype(jnp.bfloat16)
        for h, head in enumerate(heads):
            piece = mixed[h * tok_dev : (h + 1) * tok_dev]
            out_ref[:, head] = piece
            out_mine[:, head] = jnp.max(
                jnp.abs(piece.astype(jnp.float32)), axis=0, keepdims=True
            )
        cols = pl.ds(g * GROUP * HEAD, GROUP * HEAD)
        out_all[me, :, cols] = out_mine[:, cols]
        each(functools.partial(o_copy, g), "start")

    def o_copy(g, step):
        cols = pl.ds(g * GROUP * HEAD, GROUP * HEAD)
        return remote(
            out_mine.at[:, cols],
            out_all.at[me, :, cols],
            o_send.at[g, step],
            o_recv.at[g, step],
            lax.rem(me + step, tok_count),
        )

    def smooth():
        for kind in range(3):
            p_copy(kind).wait()
        peak = jnp.maximum(
            jnp.maximum(mine[...], theirs[0]), jnp.maximum(theirs[1], theirs[2])
        )
        mine[...] = peak
        for i in range(rows // LANES):
            here = slice(i * LANES, (i + 1) * LANES)
            at = pl.ds(pl.multiple_of(quad * rows + i * LANES, LANES), LANES)
            channel[0, here] = as_column(mine[:, at])
            at = pl.ds(pl.multiple_of(me * rows + i * LANES, LANES), LANES)
            channel[1, here] = as_column(gain_ref[:, at])
        for which in range(3):
            for step in range(tp_count):
                if step == 0:
                    x_copy(which, 0).wait()
                else:
                    x_copy(which, step).wait_send()
                    x_copy(which, step).wait_recv()
        relaid_out.start()
        tiles = relaid.shape[1] // LANES

        def tallest(i, most):
            cols = pl.ds(pl.multiple_of(i * LANES, LANES), LANES)
            return jnp.maximum(most, jnp.abs(relaid[:, cols].astype(jnp.float32)))

        most = lax.fori_loop(0, tiles, tallest, jnp.zeros((sub, LANES), jnp.float32))
        weight_peak = jnp.max(most, axis=1, keepdims=True)
        ours = pl.ds(pl.multiple_of(tp * sub, 16), sub)
        factor = jnp.sqrt(jnp.maximum(channel[0, ours, :], 1e-05)) / jnp.sqrt(
            jnp.maximum(weight_peak, 1e-05)
        )
        smooth_ref[...] = factor
        channel[0, ours, :] = channel[1, ours, :] / factor

        def highest(i, carry):
            cols = pl.ds(pl.multiple_of(i * LANES, LANES), LANES)
            column[0, :, cols] = jnp.max(
                jnp.abs(smooth_ref[...] * relaid[:, cols].astype(jnp.float32)),
                axis=0,
                keepdims=True,
            )
            return carry

        lax.fori_loop(0, tiles, highest, 0)
        for i in range(-(-sub // LANES)):
            size = min(LANES, sub - i * LANES)
            start = pl.multiple_of(tp * sub + i * LANES, 16)
            tile = channel[0, pl.ds(start, size), :]
            if size < LANES:
                tile = jnp.concatenate(
                    [tile, jnp.zeros((LANES - size, LANES), jnp.float32)], axis=0
                )
            folded_ref[:, i * LANES : i * LANES + size] = jnp.transpose(tile)[
                0:1, :size
            ]
        for step in range(1, tp_count):
            c_copy(step).start()

    def c_copy(step):
        return remote(
            column.at[0],
            column_tp.at[step],
            c_send.at[step],
            c_recv.at[step],
            me,
            lax.rem(tp + step, tp_count),
        )

    def b_copy(stage):
        return remote(
            column.at[1 + stage],
            column_tp.at[tp_count + stage],
            b_send.at[stage],
            b_recv.at[stage],
            (sib, side)[stage],
        )

    def a_copy(step):
        return remote(
            column.at[3],
            column_line.at[step],
            a_send.at[step],
            a_recv.at[step],
            lax.rem(place + step, line) * QUAD + quad,
        )

    def columns_tp():
        joined = column[0]
        for step in range(1, tp_count):
            c_copy(step).wait()
            joined = jnp.maximum(joined, column_tp[step])
        column[1] = joined
        b_copy(0).start()

    def columns_sib():
        b_copy(0).wait()
        column[2] = jnp.maximum(column[1], column_tp[tp_count])
        b_copy(1).start()

    def columns_side():
        b_copy(1).wait()
        column[3] = jnp.maximum(column[2], column_tp[tp_count + 1])
        for step in range(1, line):
            a_copy(step).start()

    def columns_line():
        joined = column[3]
        for step in range(1, line):
            a_copy(step).wait()
            joined = jnp.maximum(joined, column_line[step])
        scale_ref[...] = jnp.maximum(joined, 1e-05) / 127.0

    last = count - 1
    lead = len(kv_chunks)
    after = {}
    todo = []

    def plan(c, task):
        if c < last:
            after.setdefault(c, []).append(task)
        else:
            todo.append(task)

    def early():
        mine[...] = jnp.max(
            jnp.abs(tokens[...].astype(jnp.float32)), axis=0, keepdims=True
        )
        for kind in range(3):
            p_copy(kind).start()

    for c in kv_chunks:
        plan(lead, functools.partial(finish, c))
    plan(lead, kv_start)
    plan(lead, mask)
    plan(lead + 1, functools.partial(kv_step, 1))
    plan(lead + 1, smooth)
    plan(lead + 2, columns_tp)
    for step in range(2, line):
        plan(lead + 2, functools.partial(kv_step, step))
    for c in range(count):
        project(c)
        if c == 0:
            early()
        if c > 0 and c < last:
            reduce(c - 1)
        if c - 2 >= lead:
            finish(c - 2)
        for task in after.get(c, ()):
            task()
    if lead + 2 < last:
        columns_sib()
    reduce(last - 1)
    for task in todo:
        task()
    kv_side()
    if lead + 2 >= last:
        columns_sib()
    kv_ready()
    columns_side()
    waiting = [c for c in range(lead, count)]
    steps = list(range(line))
    for c in waiting:
        if c == last:
            while steps:
                reduce_step(last, steps.pop(0))
        if c >= last - 1:
            finish(c)
        attend(c - lead)
        if steps and c < last:
            reduce_step(last, steps.pop(0))
    columns_line()
    for g in range(len(q_chunks)):
        each(functools.partial(o_copy, g), "wait")
    out_peak_ref[...] = jnp.max(out_all[...], axis=0)

    for step in range(1, line):
        t_copy(step).wait_send()
        if share == 2:
            m_copy(step).wait_send()
    for c in range(count):
        for kind in range(3):
            w_copy(kind, c).wait_send()

        def sent(d, carry):
            @pl.when(d > place)
            def _():
                right(c, d).wait_send()

            @pl.when(d < place)
            def _():
                left(c, d).wait_send()

            return carry

        lax.fori_loop(0, line, sent, 0)

    def kv_sent(spot, carry):
        y_copy(spot).wait_send()
        s_copy(spot, False).wait_send()
        s_copy(spot, True).wait_send()
        return carry

    lax.fori_loop(0, line, kv_sent, 0)
    for way in range(2):
        for step in range(line - 1):

            @pl.when(has(way, step) & onward(way))
            def _():
                z_copy(way, step).wait_send()

    relaid_out.wait()


def calibrate(hidden, gain, doc_row, inverse, matrices):
    tok_count, tp_count = lax.axis_size("tok"), lax.axis_size("tp")
    line = tok_count // QUAD
    tok_dev, depth = hidden.shape
    rows = matrices[0].shape[0]
    sub = rows // tp_count
    widths = [matrix.shape[1] for matrix in matrices]
    chunks = column_chunks(widths)
    count = len(chunks)
    total = sum(widths)
    share = 2 if tp_count % 2 == 0 and tok_dev % 32 == 0 else 1
    vmem = pl.BlockSpec(memory_space=pltpu.VMEM)
    dma = pltpu.SemaphoreType.DMA
    f32, bf16 = jnp.float32, jnp.bfloat16
    queries = widths[0] // (GROUP * HEAD)
    lanes = tok_dev + -tok_dev % LANES
    return pl.pallas_call(
        functools.partial(main_kernel, chunks, line, tp_count, share),
        out_shape=(
            jax.ShapeDtypeStruct((tok_dev, widths[0]), bf16),
            jax.ShapeDtypeStruct((1, widths[0]), f32),
            jax.ShapeDtypeStruct((1, total * tp_count), f32),
            jax.ShapeDtypeStruct((1, sub), f32),
            jax.ShapeDtypeStruct((sub, LANES), f32),
            jax.ShapeDtypeStruct((sub, total * tp_count), bf16),
        ),
        in_specs=[vmem] * 7,
        out_specs=(vmem,) * 5 + (pl.BlockSpec(memory_space=pl.ANY),),
        scratch_shapes=[
            pltpu.VMEM((tok_dev, depth), bf16),
            pltpu.VMEM((tok_dev, LANES), f32),
            pltpu.VMEM((tok_dev, HEAD), f32),
            pltpu.VMEM((tok_dev, HEAD), f32),
            pltpu.VMEM((1, lanes), jnp.int32),
            pltpu.VMEM((tok_count, 1, lanes), jnp.int32),
            pltpu.VMEM((tok_dev, tok_dev * tok_count), f32),
            pltpu.VMEM((line * tok_dev, QUAD * rows), bf16),
            pltpu.VMEM((1, QUAD * rows), f32),
            pltpu.VMEM((3, 1, QUAD * rows), f32),
        ]
        + [pltpu.VMEM((3, rows, width), bf16) for width in widths]
        + [pltpu.VMEM((line * tok_dev, total), f32)] * 3
        + [
            pltpu.VMEM((tok_dev, widths[0]), bf16),
            pltpu.VMEM((tok_dev * tok_count, widths[1] + widths[2]), bf16),
            pltpu.VMEM((sub, total * tp_count), bf16),
            pltpu.VMEM((2, rows, LANES), f32),
            pltpu.VMEM((4, 1, total * tp_count), f32),
            pltpu.VMEM((tp_count + 2, 1, total * tp_count), f32),
            pltpu.VMEM((line, 1, total * tp_count), f32),
            pltpu.VMEM((1, widths[0]), f32),
            pltpu.VMEM((tok_count, 1, widths[0]), f32),
        ]
        + [dma((3, count))] * 2
        + [dma((line,))] * 4
        + [dma((3, tp_count))] * 2
        + [dma((4,))]
        + [dma((count, line))] * 4
        + [dma((3,))] * 2
        + [dma((tok_count,))] * 2
        + [dma((2, line))] * 2
        + [dma((line,))] * 2
        + [dma((2 * line,))] * 2
        + [dma((tp_count,))] * 2
        + [dma((2,))] * 2
        + [dma((line,))] * 2
        + [dma((queries, tok_count))] * 2,
        compiler_params=pltpu.CompilerParams(
            collective_id=0, has_side_effects=True, vmem_limit_bytes=63 * 1024 * 1024
        ),
    )(hidden, gain, doc_row, inverse, *matrices)


def on_device(hidden, norm_gain, w_query, w_key, w_value, doc_ids):
    tp_count = lax.axis_size("tp")
    tp_index = lax.axis_index("tp")
    matrices = (w_query, w_key, w_value)
    half = HEAD // 2
    inverse = jnp.exp(
        jnp.arange(half, dtype=jnp.float32) * (-2.0 * math.log(10000.0) / HEAD)
    )
    inverse = jnp.concatenate([inverse, inverse])[None]
    attended, out_scale, every, folded, smooth, relaid = calibrate(
        hidden, norm_gain[None], doc_ids[None], inverse, matrices
    )
    out_scale = out_scale[0]
    every = every[0]
    ends = [matrix.shape[1] * tp_count for matrix in matrices]
    bounds = [ends[0], ends[0] + ends[1]]
    every_scale = jnp.split(every, bounds)
    blocks = jnp.split(relaid, bounds, axis=1)
    scales = tuple(
        lax.dynamic_slice_in_dim(scale, tp_index * matrix.shape[1], matrix.shape[1])
        for scale, matrix in zip(every_scale, matrices)
    )
    codes = tuple(
        smooth[:, :1] * block.astype(jnp.float32) / column_scale[None, :]
        for block, column_scale in zip(blocks, every_scale)
    )
    return (attended, out_scale, folded[0], *codes, *scales)


def solution(mesh):
    in_specs = (P("tok", None), P(), P("tok", "tp"), P("tok", "tp"), P("tok", "tp"), P("tok"))
    out_specs = (
        P("tok", "tp"),
        P("tp"),
        P(("tok", "tp")),
        P(("tok", "tp"), None),
        P(("tok", "tp"), None),
        P(("tok", "tp"), None),
        P("tp"),
        P("tp"),
        P("tp"),
    )
    return jax.shard_map(
        on_device, mesh=mesh, in_specs=in_specs, out_specs=out_specs, check_vma=False
    )
```

```python
import functools
import math

import jax
import jax.numpy as jnp
from jax import lax
from jax.experimental import pallas as pl
from jax.experimental.pallas import tpu as pltpu
from jax.sharding import PartitionSpec as P

HEAD = 128
KVH = 8
QHEADS = 32
GROUP = QHEADS // KVH
LANES = 128
FAR = 1 << 30

MESH = pl.DeviceIdType.MESH
QUAD = 4


def column_chunks(widths, most=GROUP * HEAD):
    return [
        (which, start, min(most, widths[which] - start))
        for which in (1, 2, 0)
        for start in range(0, widths[which], most)
    ]


def as_column(row):
    return jnp.transpose(jnp.broadcast_to(row, (LANES, LANES)))

def main_kernel(
    chunks,
    line,
    tp_count,
    share,
    hidden_ref,
    gain_ref,
    doc_ref,
    wq_ref,
    wk_ref,
    wv_ref,
    out_ref,
    out_peak_ref,
    scale_ref,
    folded_ref,
    smooth_ref,
    relaid_ref,
    normed,
    root,
    cosine,
    sine,
    doc_row,
    docs,
    bias,
    tokens,
    mine,
    theirs,
    held_q,
    held_k,
    held_v,
    partial,
    from_left,
    from_right,
    query,
    cache,
    relaid,
    channel,
    column,
    column_tp,
    column_line,
    out_mine,
    out_all,
    w_send,
    w_recv,
    t_send,
    t_recv,
    m_send,
    m_recv,
    x_send,
    x_recv,
    x_local,
    r_send,
    r_recv,
    l_send,
    l_recv,
    p_send,
    p_recv,
    d_send,
    d_recv,
    z_send,
    z_recv,
    y_send,
    y_recv,
    s_send,
    s_recv,
    c_send,
    c_recv,
    b_send,
    b_recv,
    a_send,
    a_recv,
    o_send,
    o_recv,
):
    me = lax.axis_index("tok")
    tp = lax.axis_index("tp")
    tok_count = line * QUAD
    quad = lax.rem(me, QUAD)
    place = me // QUAD
    rows = wq_ref.shape[0]
    tok_dev = hidden_ref.shape[0]
    depth = hidden_ref.shape[1]
    width = QUAD * rows
    keys = tok_dev * tok_count
    sib = me + 1 - 2 * lax.rem(me, 2)
    side = me + 2 - 4 * (quad // 2)
    side_sib = side + 1 - 2 * lax.rem(me, 2)
    own = (wq_ref, wk_ref, wv_ref)
    held = (held_q, held_k, held_v)
    widths = [ref.shape[1] for ref in own]
    sub = rows // tp_count
    count = len(chunks)
    kv_chunks = [c for c in range(count) if chunks[c][0] > 0]
    q_chunks = [c for c in range(count) if chunks[c][0] == 0]
    kv_here = widths[1] // HEAD

    def remote(src, dst, send, recv, tok, tp_to=None):
        return pltpu.make_async_remote_copy(
            src_ref=src,
            dst_ref=dst,
            send_sem=send,
            recv_sem=recv,
            device_id=(tok, tp if tp_to is None else tp_to),
            device_id_type=MESH,
        )

    def rows_of(tok):
        return pl.ds(pl.multiple_of(tok * tok_dev, 16), tok_dev)

    def meet(barrier):
        def greet(step, carry):
            other = lax.rem(me + step, tok_count)
            pl.semaphore_signal(
                barrier, inc=1, device_id=(other, tp), device_id_type=MESH
            )
            return carry

        lax.fori_loop(1, tok_count, greet, 0)
        for step in range(1, tp_count):
            other = lax.rem(tp + step, tp_count)
            pl.semaphore_signal(
                barrier, inc=1, device_id=(me, other), device_id_type=MESH
            )

    def w_copy(kind, c):
        which, start, size = chunks[c]
        cols = pl.ds(start, size)
        if kind == 2:
            src = held[which].at[1, :, cols]
        else:
            src = own[which].at[:, cols]
        return remote(
            src,
            held[which].at[kind, :, cols],
            w_send.at[kind, c],
            w_recv.at[kind, c],
            side if kind == 1 else sib,
        )

    def weights_start(c):
        w_copy(1, c).start()
        w_copy(0, c).start()

    part = tok_dev // share
    piece = lax.rem(tp, share)
    mate = tp + 1 - 2 * piece
    first = pl.multiple_of(piece * part, 16)

    def columns_of(tok):
        return pl.ds(pl.multiple_of(lax.rem(tok, QUAD) * rows, 128), rows)

    members = (me, side, sib, side_sib)

    def t_copy(step, k):
        to = lax.rem(place + step, line)
        base = to * width + lax.rem(members[k], QUAD) * rows
        return remote(
            normed.at[pl.ds(first, part), pl.ds(pl.multiple_of(base, 128), rows)],
            tokens.at[
                pl.ds(pl.multiple_of(place * tok_dev + first, 16), part),
                columns_of(members[k]),
            ],
            t_send.at[step, k],
            t_recv.at[step, k],
            to * QUAD + quad,
        )

    def m_copy(step, k):
        source = lax.rem(place - step + line, line)
        start = pl.multiple_of(source * tok_dev + piece * part, 16)
        got = tokens.at[pl.ds(start, part), columns_of(members[k])]
        return remote(got, got, m_send.at[step, k], m_recv.at[step, k], me, mate)

    wide = [sum(widths[:i]) * tp_count for i in range(3)]

    def x_copy(which, step):
        to = lax.rem(tp + step, tp_count)
        size = widths[which]
        src = own[which].at[pl.ds(pl.multiple_of(to * sub, 16), sub)]
        dst = relaid.at[:, pl.ds(pl.multiple_of(wide[which] + tp * size, 128), size)]
        if step == 0:
            return pltpu.make_async_copy(src, dst, x_local.at[which])
        return remote(src, dst, x_send.at[which, step], x_recv.at[which, step], me, to)

    relaid_out = pltpu.make_async_copy(relaid, relaid_ref, x_local.at[3])

    def d_copy(step):
        return remote(
            doc_row,
            docs.at[me],
            d_send.at[step],
            d_recv.at[step],
            lax.rem(me + step, tok_count),
        )

    def p_copy(kind):
        return remote(
            mine,
            theirs.at[kind],
            p_send.at[kind],
            p_recv.at[kind],
            (sib, side, side_sib)[kind],
        )

    def each(copy, act):
        def go(step, carry):
            getattr(copy(step), act)()
            return carry

        lax.fori_loop(1, tok_count, go, 0)

    tiles_at = math.gcd(rows // LANES, 4)

    def normalise(start, size, base, reach):
        def go(i, carry):
            for j in range(tiles_at):
                at = base + (tiles_at * i + j) * LANES
                cols = pl.ds(pl.multiple_of(at, LANES), LANES)
                block = hidden_ref[pl.ds(start, size), cols].astype(jnp.float32)
                block = block * root[pl.ds(start, size), :] * gain_ref[:, cols]
                normed[pl.ds(start, size), cols] = block.astype(jnp.bfloat16)
            return carry

        lax.fori_loop(0, reach // (tiles_at * LANES), go, 0)

    barrier = pltpu.get_barrier_semaphore()
    meet(barrier)
    doc_row[...] = jnp.full(doc_row.shape, FAR, jnp.int32)
    doc_row[:, :tok_dev] = doc_ref[...]
    docs[me] = doc_row[...]

    def squares(i, total):
        for j in range(4):
            cols = pl.ds(pl.multiple_of((4 * i + j) * LANES, LANES), LANES)
            block = hidden_ref[:, cols].astype(jnp.float32)
            total = total + block * block
        return total

    total = lax.fori_loop(
        0, depth // (4 * LANES), squares, jnp.zeros((tok_dev, LANES), jnp.float32)
    )
    mean = jnp.sum(total, axis=1, keepdims=True) / depth
    root[...] = jnp.broadcast_to(lax.rsqrt(mean + 1e-05), (tok_dev, LANES))
    pl.semaphore_wait(barrier, tok_count - 1 + tp_count - 1)

    each(d_copy, "start")
    for c in range(min(2, count)):
        weights_start(c)

    for k in range(QUAD):

        def send_tokens(i, carry):
            step = jnp.where(2 * place < line, line - i, i)
            to = lax.rem(place + step, line)
            base = to * width + lax.rem(members[k], QUAD) * rows
            normalise(first, part, base, rows)
            t_copy(step, k).start()
            return carry

        lax.fori_loop(1, line, send_tokens, 0)
    normalise(0, tok_dev, place * width, width)
    tokens[rows_of(place)] = normed[:, pl.ds(pl.multiple_of(place * width, 128), width)]

    positions = me * tok_dev + lax.broadcasted_iota(jnp.int32, (tok_dev, HEAD), 0)
    lane = lax.broadcasted_iota(jnp.int32, (tok_dev, HEAD), 1)
    turns = lax.rem(lane, HEAD // 2).astype(jnp.float32)
    angles = positions.astype(jnp.float32) * jnp.exp(
        turns * (-2.0 * math.log(10000.0) / HEAD)
    )
    cosine[...] = jnp.cos(angles)
    sine[...] = jnp.where(lane < HEAD // 2, -1.0, 1.0) * jnp.sin(angles)

    near = sorted(range(1, line), key=lambda step: min(step, line - step))
    for k in range(QUAD):
        for step in near:
            t_copy(step, k).wait_recv()
            if share == 2:
                m_copy(step, k).start()
    for which in (1, 2, 0):
        for step in range(tp_count):
            x_copy(which, step).start()

    base_of = [sum(size for _, _, size in chunks[:c]) for c in range(count)]

    def span(c):
        return slice(base_of[c], base_of[c] + chunks[c][2])

    def block(d):
        return pl.ds(pl.multiple_of(d * tok_dev, 8), tok_dev)

    def right(c, d):
        cols = span(c)
        return remote(
            partial.at[block(d), cols],
            from_left.at[block(d), cols],
            r_send.at[c, d],
            r_recv.at[c, d],
            me + QUAD,
        )

    def left(c, d):
        cols = span(c)
        return remote(
            partial.at[block(d), cols],
            from_right.at[block(d), cols],
            l_send.at[c, d],
            l_recv.at[c, d],
            me - QUAD,
        )

    def add_left(c, d):
        right(c, d).wait_recv()
        cols = span(c)
        partial[block(d), cols] = partial[block(d), cols] + from_left[block(d), cols]

    def add_right(c, d):
        left(c, d).wait_recv()
        cols = span(c)
        partial[block(d), cols] = partial[block(d), cols] + from_right[block(d), cols]

    def first_sends(c):
        @pl.when(place == 0)
        def _():
            def go(i, carry):
                right(c, line - 1 - i).start()
                return carry

            lax.fori_loop(0, line - 1, go, 0)

        @pl.when(place == line - 1)
        def _():
            def go(i, carry):
                left(c, i).start()
                return carry

            lax.fori_loop(0, line - 1, go, 0)

    def rightward(c):
        def go(i, carry):
            @pl.when((place > 0) & (line - 1 - i > place))
            def _():
                add_left(c, line - 1 - i)
                right(c, line - 1 - i).start()

            return carry

        lax.fori_loop(0, line - 1, go, 0)

    def leftward(c):
        def go(i, carry):
            @pl.when((place < line - 1) & (i < place))
            def _():
                add_right(c, i)
                left(c, i).start()

            return carry

        lax.fori_loop(0, line - 1, go, 0)

    def reduce_step(c, i):
        @pl.when(2 * place < line)
        def _():
            (rightward, leftward)[i](c)

        @pl.when(2 * place >= line)
        def _():
            (leftward, rightward)[i](c)

    def reduce(c):
        reduce_step(c, 0)
        reduce_step(c, 1)

    def finish(c):
        @pl.when(place > 0)
        def _():
            add_left(c, place)

        @pl.when(place < line - 1)
        def _():
            add_right(c, place)

        which, start, size = chunks[c]
        for head in range(size // HEAD):
            base = base_of[c] + head * HEAD
            states = partial[block(place), base : base + HEAD]
            if which < 2:
                states = (
                    states * cosine[...]
                    + pltpu.roll(states, HEAD // 2, 1) * sine[...]
                )
            at = start + head * HEAD + (widths[1] if which == 2 else 0)
            if which == 0:
                query[:, at : at + HEAD] = states.astype(jnp.bfloat16)
            else:
                cache[rows_of(me), at : at + HEAD] = states.astype(jnp.bfloat16)

    def tokens_ready(c, k):
        if c == 0 and share == 2:
            for step in near:
                m_copy(step, k).wait_recv()

    def project(c):
        which, start, size = chunks[c]
        cols = slice(start, start + size)
        tokens_ready(c, 0)
        total = jnp.dot(
            tokens[:, columns_of(me)],
            own[which][:, cols],
            preferred_element_type=jnp.float32,
        )
        w_copy(1, c).wait_recv()
        w_copy(2, c).start()
        if c + 2 < count:
            weights_start(c + 2)
        for k, kind in ((1, 1), (2, 0), (3, 2)):
            tokens_ready(c, k)
            if kind != 1:
                w_copy(kind, c).wait_recv()
            total += jnp.dot(
                tokens[:, columns_of(members[k])],
                held[which][kind, :, cols],
                preferred_element_type=jnp.float32,
            )
        partial[:, span(c)] = total
        first_sends(c)

    def kv_rows(spot, of_side=False):
        at = lax.rem(side, QUAD) if of_side else quad
        return cache.at[rows_of(spot * QUAD + at)]

    def z_copy(way, step):
        spot = place - step if way == 0 else place + step
        to = me + QUAD if way == 0 else me - QUAD
        got = kv_rows(spot)
        return remote(got, got, z_send.at[way, step], z_recv.at[way, step], to)

    def y_copy(spot):
        got = kv_rows(spot)
        return remote(got, got, y_send.at[spot], y_recv.at[spot], side)

    def y_arrival(spot):
        got = kv_rows(spot, True)
        return remote(got, got, y_send.at[spot], y_recv.at[spot], side)

    def s_copy(spot, of_side):
        got = kv_rows(spot, of_side)
        slot = spot + (line if of_side else 0)
        return remote(got, got, s_send.at[slot], s_recv.at[slot], sib)

    def s_arrival(spot, of_side):
        at = lax.rem(side_sib if of_side else sib, QUAD)
        got = cache.at[rows_of(spot * QUAD + at)]
        slot = spot + (line if of_side else 0)
        return remote(got, got, s_send.at[slot], s_recv.at[slot], sib)

    def has(way, step):
        return place >= step if way == 0 else place + step < line

    def onward(way):
        return place + 1 < line if way == 0 else place > 0

    def kv_start():
        for way in range(2):

            @pl.when(onward(way))
            def _():
                z_copy(way, 0).start()

        y_copy(place).start()
        s_copy(place, False).start()

    def z_arrival(way, step):
        spot = place - step if way == 0 else place + step
        to = me + QUAD if way == 0 else me - QUAD
        got = kv_rows(spot)
        return remote(got, got, z_send.at[way, step - 1], z_recv.at[way, step - 1], to)

    def kv_step(step):
        for way in range(2):

            @pl.when(has(way, step))
            def _():
                z_arrival(way, step).wait_recv()

                @pl.when(onward(way))
                def _():
                    z_copy(way, step).start()

                spot = place - step if way == 0 else place + step
                y_copy(spot).start()
                s_copy(spot, False).start()

    def kv_side():
        def go(spot, carry):
            y_arrival(spot).wait_recv()
            s_copy(spot, True).start()
            return carry

        lax.fori_loop(0, line, go, 0)

    def kv_ready():
        def go(spot, carry):
            s_arrival(spot, False).wait_recv()
            s_arrival(spot, True).wait_recv()
            return carry

        lax.fori_loop(0, line, go, 0)

    def mask():
        each(d_copy, "wait")
        wanted = jnp.transpose(
            jnp.broadcast_to(doc_row[...].astype(jnp.float32), (LANES, LANES))
        )[:tok_dev]

        def go(tok, total):
            before = docs[tok].astype(jnp.float32) < wanted
            return total + jnp.where(before, 1.0, 0.0)

        total = lax.fori_loop(
            0, tok_count, go, jnp.zeros((tok_dev, LANES), jnp.float32)
        )
        since = jnp.sum(total, axis=1, keepdims=True).astype(jnp.int32)
        spot = lax.broadcasted_iota(jnp.int32, (tok_dev, keys), 0) + me * tok_dev
        at = lax.broadcasted_iota(jnp.int32, (tok_dev, keys), 1)
        bias[...] = jnp.where((at >= since) & (at <= spot), 0.0, -1e30)

    turn = math.log2(math.e) / math.sqrt(HEAD)

    def attend(g):
        heads = [
            slice((g * GROUP + h) * HEAD, (g * GROUP + h + 1) * HEAD)
            for h in range(GROUP)
        ]
        asked = jnp.concatenate([query[:, head] for head in heads], axis=0)
        key = cache[:, g * HEAD : (g + 1) * HEAD]
        value = cache[:, (kv_here + g) * HEAD : (kv_here + g + 1) * HEAD]
        scores = lax.dot_general(
            asked, key, (((1,), (1,)), ((), ())), preferred_element_type=jnp.float32
        )
        scores = (
            scores.reshape(GROUP, tok_dev, keys) + bias[...][None]
        ).reshape(GROUP * tok_dev, keys)
        weights = jnp.exp2((scores - jnp.max(scores, axis=1, keepdims=True)) * turn)
        totals = jnp.sum(weights, axis=1, keepdims=True)
        mixed = jnp.dot(
            weights.astype(jnp.bfloat16), value, preferred_element_type=jnp.float32
        )
        mixed = (mixed / totals).astype(jnp.bfloat16)
        for h, head in enumerate(heads):
            piece = mixed[h * tok_dev : (h + 1) * tok_dev]
            out_ref[:, head] = piece
            out_mine[:, head] = jnp.max(
                jnp.abs(piece.astype(jnp.float32)), axis=0, keepdims=True
            )
        cols = pl.ds(g * GROUP * HEAD, GROUP * HEAD)
        out_all[me, :, cols] = out_mine[:, cols]
        each(functools.partial(o_copy, g), "start")

    def o_copy(g, step):
        cols = pl.ds(g * GROUP * HEAD, GROUP * HEAD)
        return remote(
            out_mine.at[:, cols],
            out_all.at[me, :, cols],
            o_send.at[g, step],
            o_recv.at[g, step],
            lax.rem(me + step, tok_count),
        )

    def smooth():
        for kind in range(3):
            p_copy(kind).wait()
        peak = jnp.maximum(
            jnp.maximum(mine[...], theirs[0]), jnp.maximum(theirs[1], theirs[2])
        )
        mine[...] = peak
        for i in range(rows // LANES):
            here = slice(i * LANES, (i + 1) * LANES)
            at = pl.ds(pl.multiple_of(quad * rows + i * LANES, LANES), LANES)
            channel[0, here] = as_column(mine[:, at])
            at = pl.ds(pl.multiple_of(me * rows + i * LANES, LANES), LANES)
            channel[1, here] = as_column(gain_ref[:, at])
        for which in range(3):
            for step in range(tp_count):
                if step == 0:
                    x_copy(which, 0).wait()
                else:
                    x_copy(which, step).wait_send()
                    x_copy(which, step).wait_recv()
        relaid_out.start()
        tiles = relaid.shape[1] // LANES

        def tallest(i, most):
            cols = pl.ds(pl.multiple_of(i * LANES, LANES), LANES)
            return jnp.maximum(most, jnp.abs(relaid[:, cols].astype(jnp.float32)))

        most = lax.fori_loop(0, tiles, tallest, jnp.zeros((sub, LANES), jnp.float32))
        weight_peak = jnp.max(most, axis=1, keepdims=True)
        ours = pl.ds(pl.multiple_of(tp * sub, 16), sub)
        factor = jnp.sqrt(jnp.maximum(channel[0, ours, :], 1e-05)) / jnp.sqrt(
            jnp.maximum(weight_peak, 1e-05)
        )
        smooth_ref[...] = factor
        channel[0, ours, :] = channel[1, ours, :] / factor

        def highest(i, carry):
            cols = pl.ds(pl.multiple_of(i * LANES, LANES), LANES)
            column[0, :, cols] = jnp.max(
                jnp.abs(smooth_ref[...] * relaid[:, cols].astype(jnp.float32)),
                axis=0,
                keepdims=True,
            )
            return carry

        lax.fori_loop(0, tiles, highest, 0)
        for i in range(-(-sub // LANES)):
            size = min(LANES, sub - i * LANES)
            start = pl.multiple_of(tp * sub + i * LANES, 16)
            tile = channel[0, pl.ds(start, size), :]
            if size < LANES:
                tile = jnp.concatenate(
                    [tile, jnp.zeros((LANES - size, LANES), jnp.float32)], axis=0
                )
            folded_ref[:, i * LANES : i * LANES + size] = jnp.transpose(tile)[
                0:1, :size
            ]
        for step in range(1, tp_count):
            c_copy(step).start()

    def c_copy(step):
        return remote(
            column.at[0],
            column_tp.at[step],
            c_send.at[step],
            c_recv.at[step],
            me,
            lax.rem(tp + step, tp_count),
        )

    def b_copy(stage):
        return remote(
            column.at[1 + stage],
            column_tp.at[tp_count + stage],
            b_send.at[stage],
            b_recv.at[stage],
            (sib, side)[stage],
        )

    def a_copy(step):
        return remote(
            column.at[3],
            column_line.at[step],
            a_send.at[step],
            a_recv.at[step],
            lax.rem(place + step, line) * QUAD + quad,
        )

    def columns_tp():
        joined = column[0]
        for step in range(1, tp_count):
            c_copy(step).wait()
            joined = jnp.maximum(joined, column_tp[step])
        column[1] = joined
        b_copy(0).start()

    def columns_sib():
        b_copy(0).wait()
        column[2] = jnp.maximum(column[1], column_tp[tp_count])
        b_copy(1).start()

    def columns_side():
        b_copy(1).wait()
        column[3] = jnp.maximum(column[2], column_tp[tp_count + 1])
        for step in range(1, line):
            a_copy(step).start()

    def columns_line():
        joined = column[3]
        for step in range(1, line):
            a_copy(step).wait()
            joined = jnp.maximum(joined, column_line[step])
        scale_ref[...] = jnp.maximum(joined, 1e-05) / 127.0

    last = count - 1
    lead = len(kv_chunks)
    after = {}
    todo = []

    def plan(c, task):
        if c < last:
            after.setdefault(c, []).append(task)
        else:
            todo.append(task)

    def early():
        mine[...] = jnp.max(
            jnp.abs(tokens[...].astype(jnp.float32)), axis=0, keepdims=True
        )
        for kind in range(3):
            p_copy(kind).start()

    for c in kv_chunks:
        plan(lead, functools.partial(finish, c))
    plan(lead, kv_start)
    plan(lead, mask)
    plan(lead + 1, functools.partial(kv_step, 1))
    plan(lead + 1, smooth)
    plan(lead + 2, columns_tp)
    middle = list(range(2, line - 1)) if lead + 2 < last else []
    for step in range(2, line):
        if step not in middle:
            plan(last, functools.partial(kv_step, step))
    for c in range(count):
        project(c)
        if c == lead + 2:
            for step in middle:
                kv_step(step)
        if c == 0:
            early()
        if c > 0 and c < last:
            reduce(c - 1)
        if c - 2 >= lead:
            finish(c - 2)
        for task in after.get(c, ()):
            task()
    if lead + 2 < last:
        columns_sib()
    reduce(last - 1)
    for task in todo:
        task()
    kv_side()
    if lead + 2 >= last:
        columns_sib()
    kv_ready()
    columns_side()
    waiting = [c for c in range(lead, count)]
    steps = [0, 1]
    for c in waiting:
        if c == last:
            while steps:
                reduce_step(last, steps.pop(0))
        if c >= last - 1:
            finish(c)
        attend(c - lead)
        if steps and c < last:
            reduce_step(last, steps.pop(0))
    columns_line()
    for g in range(len(q_chunks)):
        each(functools.partial(o_copy, g), "wait")
    out_peak_ref[...] = jnp.max(out_all[...], axis=0)

    for step in range(1, line):
        for k in range(QUAD):
            t_copy(step, k).wait_send()
            if share == 2:
                m_copy(step, k).wait_send()
    for c in range(count):
        for kind in range(3):
            w_copy(kind, c).wait_send()

        def sent(d, carry):
            @pl.when(d > place)
            def _():
                right(c, d).wait_send()

            @pl.when(d < place)
            def _():
                left(c, d).wait_send()

            return carry

        lax.fori_loop(0, line, sent, 0)

    def kv_sent(spot, carry):
        y_copy(spot).wait_send()
        s_copy(spot, False).wait_send()
        s_copy(spot, True).wait_send()
        return carry

    lax.fori_loop(0, line, kv_sent, 0)
    for way in range(2):
        for step in range(line - 1):

            @pl.when(has(way, step) & onward(way))
            def _():
                z_copy(way, step).wait_send()

    relaid_out.wait()


def calibrate(hidden, gain, doc_row, matrices):
    tok_count, tp_count = lax.axis_size("tok"), lax.axis_size("tp")
    line = tok_count // QUAD
    tok_dev, depth = hidden.shape
    rows = matrices[0].shape[0]
    sub = rows // tp_count
    widths = [matrix.shape[1] for matrix in matrices]
    chunks = column_chunks(widths)
    count = len(chunks)
    total = sum(widths)
    share = 2 if tp_count % 2 == 0 and tok_dev % 32 == 0 else 1
    vmem = pl.BlockSpec(memory_space=pltpu.VMEM)
    dma = pltpu.SemaphoreType.DMA
    f32, bf16 = jnp.float32, jnp.bfloat16
    queries = widths[0] // (GROUP * HEAD)
    lanes = tok_dev + -tok_dev % LANES
    return pl.pallas_call(
        functools.partial(main_kernel, chunks, line, tp_count, share),
        out_shape=(
            jax.ShapeDtypeStruct((tok_dev, widths[0]), bf16),
            jax.ShapeDtypeStruct((1, widths[0]), f32),
            jax.ShapeDtypeStruct((1, total * tp_count), f32),
            jax.ShapeDtypeStruct((1, sub), f32),
            jax.ShapeDtypeStruct((sub, LANES), f32),
            jax.ShapeDtypeStruct((sub, total * tp_count), bf16),
        ),
        in_specs=[vmem] * 6,
        out_specs=(vmem,) * 5 + (pl.BlockSpec(memory_space=pl.ANY),),
        scratch_shapes=[
            pltpu.VMEM((tok_dev, depth), bf16),
            pltpu.VMEM((tok_dev, LANES), f32),
            pltpu.VMEM((tok_dev, HEAD), f32),
            pltpu.VMEM((tok_dev, HEAD), f32),
            pltpu.VMEM((1, lanes), jnp.int32),
            pltpu.VMEM((tok_count, 1, lanes), jnp.int32),
            pltpu.VMEM((tok_dev, tok_dev * tok_count), f32),
            pltpu.VMEM((line * tok_dev, QUAD * rows), bf16),
            pltpu.VMEM((1, QUAD * rows), f32),
            pltpu.VMEM((3, 1, QUAD * rows), f32),
        ]
        + [pltpu.VMEM((3, rows, width), bf16) for width in widths]
        + [pltpu.VMEM((line * tok_dev, total), f32)] * 3
        + [
            pltpu.VMEM((tok_dev, widths[0]), bf16),
            pltpu.VMEM((tok_dev * tok_count, widths[1] + widths[2]), bf16),
            pltpu.VMEM((sub, total * tp_count), bf16),
            pltpu.VMEM((2, rows, LANES), f32),
            pltpu.VMEM((4, 1, total * tp_count), f32),
            pltpu.VMEM((tp_count + 2, 1, total * tp_count), f32),
            pltpu.VMEM((line, 1, total * tp_count), f32),
            pltpu.VMEM((1, widths[0]), f32),
            pltpu.VMEM((tok_count, 1, widths[0]), f32),
        ]
        + [dma((3, count))] * 2
        + [dma((line, QUAD))] * 4
        + [dma((3, tp_count))] * 2
        + [dma((4,))]
        + [dma((count, line))] * 4
        + [dma((3,))] * 2
        + [dma((tok_count,))] * 2
        + [dma((2, line))] * 2
        + [dma((line,))] * 2
        + [dma((2 * line,))] * 2
        + [dma((tp_count,))] * 2
        + [dma((2,))] * 2
        + [dma((line,))] * 2
        + [dma((queries, tok_count))] * 2,
        compiler_params=pltpu.CompilerParams(
            collective_id=0, has_side_effects=True, vmem_limit_bytes=63 * 1024 * 1024
        ),
    )(hidden, gain, doc_row, *matrices)


def codes_kernel(
    widths,
    tp_count,
    relaid_ref,
    smooth_ref,
    scale_ref,
    attended_ref,
    peak_ref,
    folded_ref,
    cq_ref,
    ck_ref,
    cv_ref,
    sq_ref,
    sk_ref,
    sv_ref,
    out_ref,
    out_peak_ref,
    out_folded_ref,
    inverse,
):
    tp = lax.axis_index("tp")

    @pl.when(pl.program_id(0) == 0)
    def _():
        out_ref[...] = attended_ref[...]
        out_peak_ref[...] = peak_ref[...]
        out_folded_ref[...] = folded_ref[...]
        inverse[...] = 1.0 / scale_ref[...]
        for which, ref in enumerate((sq_ref, sk_ref, sv_ref)):
            base = sum(widths[:which]) * tp_count + tp * widths[which]
            ref[...] = scale_ref[:, pl.ds(pl.multiple_of(base, 128), widths[which])]

    factor = smooth_ref[...]
    for which, ref in enumerate((cq_ref, ck_ref, cv_ref)):
        base = sum(widths[:which]) * tp_count
        for at in range(0, widths[which] * tp_count, LANES):
            cols = slice(base + at, base + at + LANES)
            ref[:, at : at + LANES] = (
                factor * relaid_ref[:, cols].astype(jnp.float32) * inverse[:, cols]
            )


def coded(relaid, smooth, scale, attended, peak, folded, widths, tp_count):
    sub, total = relaid.shape
    block = math.gcd(sub, 128)
    f32 = jnp.float32

    def striped(width):
        return pl.BlockSpec((block, width), lambda i: (i, 0))

    def whole(array):
        return pl.BlockSpec(array.shape, lambda i: (0, 0))

    full = [jax.ShapeDtypeStruct((sub, width * tp_count), f32) for width in widths]
    part = [jax.ShapeDtypeStruct((1, width), f32) for width in widths]
    rest = [
        jax.ShapeDtypeStruct(array.shape, array.dtype)
        for array in (attended, peak, folded)
    ]
    return pl.pallas_call(
        functools.partial(codes_kernel, widths, tp_count),
        grid=(sub // block,),
        out_shape=full + part + rest,
        in_specs=[striped(total), striped(LANES)]
        + [whole(array) for array in (scale, attended, peak, folded)],
        out_specs=[striped(width * tp_count) for width in widths]
        + [whole(array) for array in part + rest],
        scratch_shapes=[pltpu.VMEM((1, total), f32)],
    )(relaid, smooth, scale, attended, peak, folded)


def on_device(hidden, norm_gain, w_query, w_key, w_value, doc_ids):
    matrices = (w_query, w_key, w_value)
    attended, peak, scale, folded, smooth, relaid = calibrate(
        hidden, norm_gain[None], doc_ids[None], matrices
    )
    *rows, attended, peak, folded = coded(
        relaid,
        smooth,
        scale,
        attended,
        peak,
        folded,
        [matrix.shape[1] for matrix in matrices],
        lax.axis_size("tp"),
    )
    scales = [row[0] for row in rows[3:]]
    return (attended, peak[0], folded[0], *rows[:3], *scales)


def solution(mesh):
    in_specs = (P("tok", None), P(), P("tok", "tp"), P("tok", "tp"), P("tok", "tp"), P("tok"))
    out_specs = (
        P("tok", "tp"),
        P("tp"),
        P(("tok", "tp")),
        P(("tok", "tp"), None),
        P(("tok", "tp"), None),
        P(("tok", "tp"), None),
        P("tp"),
        P("tp"),
        P("tp"),
    )
    return jax.shard_map(
        on_device, mesh=mesh, in_specs=in_specs, out_specs=out_specs, check_vma=False
    )
```

```python
import functools
import math

import jax
import jax.numpy as jnp
from jax import lax
from jax.experimental import pallas as pl
from jax.experimental.pallas import tpu as pltpu
from jax.sharding import PartitionSpec as P

HEAD = 128
KVH = 8
QHEADS = 32
GROUP = QHEADS // KVH
LANES = 128
FAR = 1 << 30

MESH = pl.DeviceIdType.MESH
QUAD = 4


def column_chunks(widths, most=GROUP * HEAD):
    return [
        (which, start, min(most, widths[which] - start))
        for which in (1, 2, 0)
        for start in range(0, widths[which], most)
    ]


def as_column(row):
    return jnp.transpose(jnp.broadcast_to(row, (LANES, LANES)))

def main_kernel(
    chunks,
    line,
    tp_count,
    share,
    hidden_ref,
    gain_ref,
    doc_ref,
    wq_ref,
    wk_ref,
    wv_ref,
    out_ref,
    out_peak_ref,
    scale_ref,
    folded_ref,
    smooth_ref,
    relaid_ref,
    normed,
    root,
    cosine,
    sine,
    doc_row,
    docs,
    bias,
    tokens,
    mine,
    theirs,
    held_q,
    held_k,
    held_v,
    partial,
    from_left,
    from_right,
    outgoing,
    value_left,
    value_right,
    query,
    cache,
    relaid,
    channel,
    column,
    column_tp,
    column_line,
    out_mine,
    out_all,
    w_send,
    w_recv,
    t_send,
    t_recv,
    m_send,
    m_recv,
    x_send,
    x_recv,
    x_local,
    r_send,
    r_recv,
    l_send,
    l_recv,
    p_send,
    p_recv,
    d_send,
    d_recv,
    z_send,
    z_recv,
    y_send,
    y_recv,
    s_send,
    s_recv,
    q_send,
    q_recv,
    c_send,
    c_recv,
    b_send,
    b_recv,
    a_send,
    a_recv,
    o_send,
    o_recv,
):
    me = lax.axis_index("tok")
    tp = lax.axis_index("tp")
    tok_count = line * QUAD
    quad = lax.rem(me, QUAD)
    place = me // QUAD
    rows = wq_ref.shape[0]
    tok_dev = hidden_ref.shape[0]
    depth = hidden_ref.shape[1]
    width = QUAD * rows
    keys = tok_dev * tok_count
    sib = me + 1 - 2 * lax.rem(me, 2)
    side = me + 2 - 4 * (quad // 2)
    side_sib = side + 1 - 2 * lax.rem(me, 2)
    own = (wq_ref, wk_ref, wv_ref)
    held = (held_q, held_k, held_v)
    widths = [ref.shape[1] for ref in own]
    sub = rows // tp_count
    count = len(chunks)
    kv_chunks = [c for c in range(count) if chunks[c][0] > 0]
    q_chunks = [c for c in range(count) if chunks[c][0] == 0]
    kv_here = widths[1] // HEAD
    last = count - 1
    lead = len(kv_chunks)
    half = line // 2
    base = jnp.where(2 * place < line, 0, half)
    at_end = (place == 0) | (place == line - 1)

    def remote(src, dst, send, recv, tok, tp_to=None):
        return pltpu.make_async_remote_copy(
            src_ref=src,
            dst_ref=dst,
            send_sem=send,
            recv_sem=recv,
            device_id=(tok, tp if tp_to is None else tp_to),
            device_id_type=MESH,
        )

    def rows_of(tok):
        return pl.ds(pl.multiple_of(tok * tok_dev, 16), tok_dev)

    def meet(barrier):
        def greet(step, carry):
            other = lax.rem(me + step, tok_count)
            pl.semaphore_signal(
                barrier, inc=1, device_id=(other, tp), device_id_type=MESH
            )
            return carry

        lax.fori_loop(1, tok_count, greet, 0)
        for step in range(1, tp_count):
            other = lax.rem(tp + step, tp_count)
            pl.semaphore_signal(
                barrier, inc=1, device_id=(me, other), device_id_type=MESH
            )

    def w_copy(kind, c):
        which, start, size = chunks[c]
        cols = pl.ds(start, size)
        if kind == 2:
            src = held[which].at[1, :, cols]
        else:
            src = own[which].at[:, cols]
        return remote(
            src,
            held[which].at[kind, :, cols],
            w_send.at[kind, c],
            w_recv.at[kind, c],
            side if kind == 1 else sib,
        )

    ahead = 3

    def weights_start(c):
        w_copy(1, c).start()
        w_copy(0, c).start()

    part = tok_dev // share
    piece = lax.rem(tp, share)
    mate = tp + 1 - 2 * piece
    first = pl.multiple_of(piece * part, 16)

    def columns_of(tok):
        return pl.ds(pl.multiple_of(lax.rem(tok, QUAD) * rows, 128), rows)

    members = (me, side, sib, side_sib)

    def t_copy(step, k):
        to = lax.rem(place + step, line)
        base = to * width + lax.rem(members[k], QUAD) * rows
        return remote(
            normed.at[pl.ds(first, part), pl.ds(pl.multiple_of(base, 128), rows)],
            tokens.at[
                pl.ds(pl.multiple_of(place * tok_dev + first, 16), part),
                columns_of(members[k]),
            ],
            t_send.at[step, k],
            t_recv.at[step, k],
            to * QUAD + quad,
        )

    def m_copy(step, k):
        source = lax.rem(place - step + line, line)
        start = pl.multiple_of(source * tok_dev + piece * part, 16)
        got = tokens.at[pl.ds(start, part), columns_of(members[k])]
        return remote(got, got, m_send.at[step, k], m_recv.at[step, k], me, mate)

    wide = [sum(widths[:i]) * tp_count for i in range(3)]

    def x_copy(which, step):
        to = lax.rem(tp + step, tp_count)
        size = widths[which]
        src = own[which].at[pl.ds(pl.multiple_of(to * sub, 16), sub)]
        dst = relaid.at[:, pl.ds(pl.multiple_of(wide[which] + tp * size, 128), size)]
        if step == 0:
            return pltpu.make_async_copy(src, dst, x_local.at[which])
        return remote(src, dst, x_send.at[which, step], x_recv.at[which, step], me, to)

    relaid_out = pltpu.make_async_copy(relaid, relaid_ref, x_local.at[3])

    def d_copy(step):
        to = lax.rem(me + step, tok_count)
        return remote(doc_row, docs.at[me], d_send.at[0], d_recv.at[0], to)

    def d_all():
        every = docs.at[pl.ds(0, tok_count - 1)]
        return remote(every, every, d_send.at[0], d_recv.at[0], sib)

    def p_copy(kind):
        return remote(
            mine,
            theirs.at[kind],
            p_send.at[kind],
            p_recv.at[kind],
            (sib, side, side_sib)[kind],
        )

    def each(copy):
        def go(step, carry):
            copy(step).start()
            return carry

        lax.fori_loop(1, tok_count, go, 0)

    tiles_at = math.gcd(rows // LANES, 4)

    def normalise(start, size, base, reach):
        def go(i, carry):
            for j in range(tiles_at):
                at = base + (tiles_at * i + j) * LANES
                cols = pl.ds(pl.multiple_of(at, LANES), LANES)
                block = hidden_ref[pl.ds(start, size), cols].astype(jnp.float32)
                block = block * root[pl.ds(start, size), :] * gain_ref[:, cols]
                normed[pl.ds(start, size), cols] = block.astype(jnp.bfloat16)
            return carry

        lax.fori_loop(0, reach // (tiles_at * LANES), go, 0)

    barrier = pltpu.get_barrier_semaphore()
    meet(barrier)
    doc_row[...] = jnp.full(doc_row.shape, FAR, jnp.int32)
    doc_row[:, :tok_dev] = doc_ref[...]
    docs[me] = doc_row[...]

    def squares(i, total):
        for j in range(4):
            cols = pl.ds(pl.multiple_of((4 * i + j) * LANES, LANES), LANES)
            block = hidden_ref[:, cols].astype(jnp.float32)
            total = total + block * block
        return total

    total = lax.fori_loop(
        0, depth // (4 * LANES), squares, jnp.zeros((tok_dev, LANES), jnp.float32)
    )
    mean = jnp.sum(total, axis=1, keepdims=True) / depth
    root[...] = jnp.broadcast_to(lax.rsqrt(mean + 1e-05), (tok_dev, LANES))
    pl.semaphore_wait(barrier, tok_count - 1 + tp_count - 1)

    each(d_copy)
    for c in range(min(ahead, count)):
        weights_start(c)

    for k in range(QUAD):

        def send_tokens(i, carry):
            step = jnp.where(2 * place < line, line - i, i)
            to = lax.rem(place + step, line)
            base = to * width + lax.rem(members[k], QUAD) * rows
            normalise(first, part, base, rows)
            t_copy(step, k).start()
            return carry

        lax.fori_loop(1, line, send_tokens, 0)
    normalise(0, tok_dev, place * width, width)
    tokens[rows_of(place)] = normed[:, pl.ds(pl.multiple_of(place * width, 128), width)]

    lane = lax.broadcasted_iota(jnp.int32, (tok_dev, HEAD), 1)
    turns = lax.rem(lane, HEAD // 2).astype(jnp.float32)
    speed = jnp.exp(turns * (-2.0 * math.log(10000.0) / HEAD))

    def tables(j, carry):
        spot = ((base + j) * QUAD + quad) * tok_dev
        spot = spot + lax.broadcasted_iota(jnp.int32, (tok_dev, HEAD), 0)
        angles = spot.astype(jnp.float32) * speed
        cosine[j] = jnp.cos(angles)
        sine[j] = jnp.where(lane < HEAD // 2, -1.0, 1.0) * jnp.sin(angles)
        return carry

    lax.fori_loop(0, half, tables, 0)
    near = sorted(range(1, line), key=lambda step: min(step, line - step))
    for k in range(QUAD):
        for step in near:
            t_copy(step, k).wait_recv()
            if share == 2:
                m_copy(step, k).start()
    for which in (1, 2, 0):
        for step in range(tp_count):
            x_copy(which, step).start()

    base_of = [sum(size for _, _, size in chunks[:c]) for c in range(count)]

    def span(c):
        return slice(base_of[c], base_of[c] + chunks[c][2])

    def block(d):
        return pl.ds(pl.multiple_of(d * tok_dev, 8), tok_dev)

    def travels(c):
        which, start, size = chunks[c]
        if which == 2:
            return outgoing, value_left, value_right, slice(start, start + size)
        return partial, from_left, from_right, span(c)

    def right(c, d):
        held_here, landed, _, cols = travels(c)
        return remote(
            held_here.at[block(d), cols],
            landed.at[block(d), cols],
            r_send.at[c, d],
            r_recv.at[c, d],
            me + QUAD,
        )

    def left(c, d):
        held_here, _, landed, cols = travels(c)
        return remote(
            held_here.at[block(d), cols],
            landed.at[block(d), cols],
            l_send.at[c, d],
            l_recv.at[c, d],
            me - QUAD,
        )

    def added(c, d, way):
        (right, left)[way](c, d).wait_recv()
        landed, cols = travels(c)[1 + way], travels(c)[3]
        return partial[block(d), span(c)] + landed[block(d), cols].astype(jnp.float32)

    def pass_on(c, d, way):
        to, cols = travels(c)[0], travels(c)[3]
        to[block(d), cols] = added(c, d, way).astype(to.dtype)
        (right, left)[way](c, d).start()

    def sends(c, way):
        if c < last:
            return half, (lambda i: half + i) if way == 0 else (lambda i: half - 1 - i)
        if way == 0:
            return line - 1, lambda i: line - 1 - i
        return line - 1, lambda i: i

    def goes(c, d, way):
        if c < last:
            return place < line - 1 if way == 0 else place > 0
        return d > place if way == 0 else d < place

    def first_sends(c):
        for way in range(2):

            @pl.when(place == (0 if way == 0 else line - 1))
            def _():
                size, pick = sends(c, way)

                def go(i, carry):
                    (right, left)[way](c, pick(i)).start()
                    return carry

                lax.fori_loop(0, size, go, 0)

    def onward(c, i, way):
        size, pick = sends(c, way)
        inside = place > 0 if way == 0 else place < line - 1
        d = pick(i)

        @pl.when((i < size) & inside & goes(c, d, way))
        def _():
            pass_on(c, d, way)

    def weave(far, near):
        def go(nearest, i):
            if far is not None:
                onward(far, i, 1 - nearest)
            if near is not None:
                onward(near, i, nearest)

        def left_half(i, carry):
            go(0, i)
            return carry

        def right_half(i, carry):
            go(1, i)
            return carry

        top = line - 1 if last in (far, near) else half

        @pl.when(2 * place < line)
        def _():
            lax.fori_loop(0, top, left_half, 0)

        @pl.when(2 * place >= line)
        def _():
            lax.fori_loop(0, top, right_half, 0)

    def settle(c, j):
        which, start, size = chunks[c]
        d = base + j
        for head in range(size // HEAD):
            at = base_of[c] + head * HEAD
            states = partial[block(d), at : at + HEAD]
            if which < 2:
                states = (
                    states * cosine[j] + pltpu.roll(states, HEAD // 2, 1) * sine[j]
                )
            at = start + head * HEAD + (widths[1] if which == 2 else 0)
            if which == 0:
                query[j, :, at : at + HEAD] = states.astype(jnp.bfloat16)
            else:
                rows_at = rows_of(d * QUAD + quad)
                cache[rows_at, at : at + HEAD] = states.astype(jnp.bfloat16)

    def q_copy(c, j):
        which, start, size = chunks[c]
        got = query.at[j, :, pl.ds(start, size)]
        to = (base + j) * QUAD + quad
        return remote(got, got, q_send.at[c - lead, j], q_recv.at[c - lead], to)

    def finish(c):
        if c == last:
            for way in range(2):

                @pl.when(place > 0 if way == 0 else place < line - 1)
                def _():
                    partial[block(place), span(c)] = added(c, place, way)

            settle(c, place - base)
            return

        @pl.when(at_end)
        def _():
            def go(i, carry):
                j = jnp.where(place == 0, half - 1 - i, i)
                d = base + j
                for way in range(2):

                    @pl.when(place == (line - 1 if way == 0 else 0))
                    def _():
                        partial[block(d), span(c)] = added(c, d, way)

                settle(c, j)
                if chunks[c][0] == 0:

                    @pl.when(d != place)
                    def _():
                        q_copy(c, j).start()

                return carry

            lax.fori_loop(0, half, go, 0)

    def tokens_ready(c, k):
        if c == 0 and share == 2:
            for step in near:
                m_copy(step, k).wait_recv()

    def project(c):
        which, start, size = chunks[c]
        cols = slice(start, start + size)
        tokens_ready(c, 0)
        total = jnp.dot(
            tokens[:, columns_of(me)],
            own[which][:, cols],
            preferred_element_type=jnp.float32,
        )
        w_copy(1, c).wait_recv()
        w_copy(2, c).start()
        if c + ahead < count:
            weights_start(c + ahead)
        for k, kind in ((1, 1), (2, 0), (3, 2)):
            tokens_ready(c, k)
            if kind != 1:
                w_copy(kind, c).wait_recv()
            total += jnp.dot(
                tokens[:, columns_of(members[k])],
                held[which][kind, :, cols],
                preferred_element_type=jnp.float32,
            )
        partial[:, span(c)] = total
        if which == 2:
            outgoing[:, cols] = total.astype(jnp.bfloat16)
        first_sends(c)

    def kv_rows(spot, of_side=False):
        at = lax.rem(side, QUAD) if of_side else quad
        return cache.at[rows_of(spot * QUAD + at)]

    def z_copy(way, j):
        got = kv_rows(j + way * half)
        to = me - QUAD if way else me + QUAD
        return remote(got, got, z_send.at[way, j], z_recv.at[way, j], to)

    def y_copy(spot):
        got = kv_rows(spot)
        return remote(got, got, y_send.at[spot], y_recv.at[spot], side)

    def y_arrival(spot):
        got = kv_rows(spot, True)
        return remote(got, got, y_send.at[spot], y_recv.at[spot], side)

    def s_copy(spot, of_side):
        got = kv_rows(spot, of_side)
        slot = spot + (line if of_side else 0)
        return remote(got, got, s_send.at[slot], s_recv.at[slot], sib)

    def s_arrival(spot, of_side):
        at = lax.rem(side_sib if of_side else sib, QUAD)
        got = cache.at[rows_of(spot * QUAD + at)]
        slot = spot + (line if of_side else 0)
        return remote(got, got, s_send.at[slot], s_recv.at[slot], sib)

    def kv_pass(way, fresh):
        def go(j, carry):
            if not fresh:
                z_copy(way, j).wait_recv()

            @pl.when(place > 0 if way else place < line - 1)
            def _():
                z_copy(way, j).start()

            y_copy(j + way * half).start()
            s_copy(j + way * half, False).start()
            return carry

        lax.fori_loop(0, half, go, 0)

    def kv_start():
        for way in range(2):

            @pl.when(place == way * (line - 1))
            def _():
                kv_pass(way, True)

    def kv_near():
        for way in range(2):
            nearer = 2 * place >= line if way else 2 * place < line

            @pl.when(nearer & jnp.logical_not(at_end))
            def _():
                kv_pass(way, False)

    def kv_far():
        for way in range(2):

            @pl.when(2 * place < line if way else 2 * place >= line)
            def _():
                kv_pass(way, False)

    def kv_side():
        def go(spot, carry):
            y_arrival(spot).wait_recv()
            s_copy(spot, True).start()
            return carry

        lax.fori_loop(0, line, go, 0)

    def kv_ready():
        def go(spot, carry):
            s_arrival(spot, False).wait_recv()
            s_arrival(spot, True).wait_recv()
            return carry

        lax.fori_loop(0, line, go, 0)

    def mask():
        d_all().wait()
        wanted = jnp.transpose(
            jnp.broadcast_to(doc_row[...].astype(jnp.float32), (LANES, LANES))
        )[:tok_dev]

        def go(tok, total):
            before = docs[tok].astype(jnp.float32) < wanted
            return total + jnp.where(before, 1.0, 0.0)

        total = lax.fori_loop(
            0, tok_count, go, jnp.zeros((tok_dev, LANES), jnp.float32)
        )
        since = jnp.sum(total, axis=1, keepdims=True).astype(jnp.int32)
        spot = lax.broadcasted_iota(jnp.int32, (tok_dev, keys), 0) + me * tok_dev
        at = lax.broadcasted_iota(jnp.int32, (tok_dev, keys), 1)
        bias[...] = jnp.where((at >= since) & (at <= spot), 0.0, -1e30)

    turn = math.log2(math.e) / math.sqrt(HEAD)

    def attend(g):
        heads = [
            slice((g * GROUP + h) * HEAD, (g * GROUP + h + 1) * HEAD)
            for h in range(GROUP)
        ]
        if g + lead < last:

            @pl.when(jnp.logical_not(at_end))
            def _():
                q_copy(g + lead, place - base).wait_recv()

        asked = jnp.concatenate(
            [query[place - base, :, head] for head in heads], axis=0
        )
        key = cache[:, g * HEAD : (g + 1) * HEAD]
        value = cache[:, (kv_here + g) * HEAD : (kv_here + g + 1) * HEAD]
        scores = lax.dot_general(
            asked, key, (((1,), (1,)), ((), ())), preferred_element_type=jnp.float32
        )
        scores = (
            scores.reshape(GROUP, tok_dev, keys) + bias[...][None]
        ).reshape(GROUP * tok_dev, keys)
        weights = jnp.exp2((scores - jnp.max(scores, axis=1, keepdims=True)) * turn)
        totals = jnp.sum(weights, axis=1, keepdims=True)
        mixed = jnp.dot(
            weights.astype(jnp.bfloat16), value, preferred_element_type=jnp.float32
        )
        mixed = (mixed / totals).astype(jnp.bfloat16)
        for h, head in enumerate(heads):
            piece = mixed[h * tok_dev : (h + 1) * tok_dev]
            out_ref[:, head] = piece
            out_mine[:, head] = jnp.max(
                jnp.abs(piece.astype(jnp.float32)), axis=0, keepdims=True
            )
        cols = pl.ds(g * GROUP * HEAD, GROUP * HEAD)
        out_all[me, :, cols] = out_mine[:, cols]
        each(functools.partial(o_copy, g))

    def o_copy(g, step):
        cols = pl.ds(g * GROUP * HEAD, GROUP * HEAD)
        to = lax.rem(me + step, tok_count)
        return remote(
            out_mine.at[:, cols], out_all.at[me, :, cols], o_send.at[0], o_recv.at[0], to
        )

    def o_all():
        every = out_all.at[pl.ds(0, tok_count - 1)]
        return remote(every, every, o_send.at[0], o_recv.at[0], sib)

    def smooth():
        for kind in range(3):
            p_copy(kind).wait()
        peak = jnp.maximum(
            jnp.maximum(mine[...], theirs[0]), jnp.maximum(theirs[1], theirs[2])
        )
        mine[...] = peak
        for i in range(rows // LANES):
            here = slice(i * LANES, (i + 1) * LANES)
            at = pl.ds(pl.multiple_of(quad * rows + i * LANES, LANES), LANES)
            channel[0, here] = as_column(mine[:, at])
            at = pl.ds(pl.multiple_of(me * rows + i * LANES, LANES), LANES)
            channel[1, here] = as_column(gain_ref[:, at])
        for which in range(3):
            for step in range(tp_count):
                if step == 0:
                    x_copy(which, 0).wait()
                else:
                    x_copy(which, step).wait_send()
                    x_copy(which, step).wait_recv()
        relaid_out.start()
        tiles = relaid.shape[1] // LANES

        def tallest(i, most):
            cols = pl.ds(pl.multiple_of(i * LANES, LANES), LANES)
            return jnp.maximum(most, jnp.abs(relaid[:, cols].astype(jnp.float32)))

        most = lax.fori_loop(0, tiles, tallest, jnp.zeros((sub, LANES), jnp.float32))
        weight_peak = jnp.max(most, axis=1, keepdims=True)
        ours = pl.ds(pl.multiple_of(tp * sub, 16), sub)
        factor = jnp.sqrt(jnp.maximum(channel[0, ours, :], 1e-05)) / jnp.sqrt(
            jnp.maximum(weight_peak, 1e-05)
        )
        smooth_ref[...] = factor
        channel[0, ours, :] = channel[1, ours, :] / factor

        def highest(i, carry):
            cols = pl.ds(pl.multiple_of(i * LANES, LANES), LANES)
            column[0, :, cols] = jnp.max(
                jnp.abs(smooth_ref[...] * relaid[:, cols].astype(jnp.float32)),
                axis=0,
                keepdims=True,
            )
            return carry

        lax.fori_loop(0, tiles, highest, 0)
        for i in range(-(-sub // LANES)):
            size = min(LANES, sub - i * LANES)
            start = pl.multiple_of(tp * sub + i * LANES, 16)
            tile = channel[0, pl.ds(start, size), :]
            if size < LANES:
                tile = jnp.concatenate(
                    [tile, jnp.zeros((LANES - size, LANES), jnp.float32)], axis=0
                )
            folded_ref[:, i * LANES : i * LANES + size] = jnp.transpose(tile)[
                0:1, :size
            ]
        for step in range(1, tp_count):
            c_copy(step).start()

    def c_copy(step):
        return remote(
            column.at[0],
            column_tp.at[step],
            c_send.at[step],
            c_recv.at[step],
            me,
            lax.rem(tp + step, tp_count),
        )

    def b_copy(stage):
        return remote(
            column.at[1 + stage],
            column_tp.at[tp_count + stage],
            b_send.at[stage],
            b_recv.at[stage],
            (sib, side)[stage],
        )

    def a_copy(step):
        return remote(
            column.at[3],
            column_line.at[step],
            a_send.at[step],
            a_recv.at[step],
            lax.rem(place + step, line) * QUAD + quad,
        )

    def columns_tp():
        joined = column[0]
        for step in range(1, tp_count):
            c_copy(step).wait()
            joined = jnp.maximum(joined, column_tp[step])
        column[1] = joined
        b_copy(0).start()

    def columns_sib():
        b_copy(0).wait()
        column[2] = jnp.maximum(column[1], column_tp[tp_count])
        b_copy(1).start()

    def columns_side():
        b_copy(1).wait()
        column[3] = jnp.maximum(column[2], column_tp[tp_count + 1])
        for step in range(1, line):
            a_copy(step).start()

    def columns_line():
        joined = column[3]
        for step in range(1, line):
            a_copy(step).wait()
            joined = jnp.maximum(joined, column_line[step])
        scale_ref[...] = jnp.maximum(joined, 1e-05) / 127.0

    def early():
        mine[...] = jnp.max(
            jnp.abs(tokens[...].astype(jnp.float32)), axis=0, keepdims=True
        )
        for kind in range(3):
            p_copy(kind).start()

    ran = set()

    def once(act, c, *rest):
        if c <= last and (act, c) not in ran:
            ran.add((act, c))
            act(c, *rest)

    def pair(far, near):
        far = None if far > last or ("far", far) in ran else far
        near = None if near > last or ("near", near) in ran else near
        ran.update({("far", far), ("near", near)})
        if far is not None or near is not None:
            weave(far, near)

    def split_project(c, ends):
        @pl.when(at_end if ends else jnp.logical_not(at_end))
        def _():
            project(c)

    once(project, 0)
    early()
    for c in range(1, lead):
        once(project, c)
    for c in range(lead):
        pair(c - 1 if c else FAR, c)
    once(project, lead)
    pair(lead - 1, lead)
    for c in kv_chunks:
        once(finish, c)
    kv_start()
    mask()
    once(project, lead + 1)
    pair(lead, FAR)
    kv_near()
    smooth()
    once(project, lead + 2)
    if lead + 3 <= last:
        split_project(lead + 3, True)
    kv_far()
    pair(FAR, lead + 1)
    if lead < last - 1:
        once(finish, lead)
    if lead + 3 <= last:
        split_project(lead + 3, False)
        ran.add((project, lead + 3))
    pair(lead + 1, lead + 2)
    if lead + 1 < last - 1:
        once(finish, lead + 1)
    columns_tp()
    for c in range(lead, count):
        once(project, c)
        pair(c - 1, c)
    columns_sib()
    pair(last, FAR)
    kv_side()
    columns_side()
    kv_ready()
    for c in range(lead, count):
        once(finish, c)
        attend(c - lead)
    columns_line()
    o_all().wait()
    out_peak_ref[...] = jnp.max(out_all[...], axis=0)

    for step in range(1, line):
        for k in range(QUAD):
            t_copy(step, k).wait_send()
            if share == 2:
                m_copy(step, k).wait_send()
    for c in range(count):
        for kind in range(3):
            w_copy(kind, c).wait_send()

        def sent(d, carry):
            if c < last:
                to_right, to_left = d >= half, d < half
            else:
                to_right, to_left = d > place, d < place

            @pl.when(to_right & (place < line - 1))
            def _():
                right(c, d).wait_send()

            @pl.when(to_left & (place > 0))
            def _():
                left(c, d).wait_send()

            return carry

        lax.fori_loop(0, line, sent, 0)

    for c in range(lead, last):

        @pl.when(at_end)
        def _():
            def q_sent(j, carry):
                @pl.when(base + j != place)
                def _():
                    q_copy(c, j).wait_send()

                return carry

            lax.fori_loop(0, half, q_sent, 0)

    def kv_sent(spot, carry):
        y_copy(spot).wait_send()
        s_copy(spot, False).wait_send()
        s_copy(spot, True).wait_send()
        return carry

    lax.fori_loop(0, line, kv_sent, 0)
    for way in range(2):

        @pl.when(place > 0 if way else place < line - 1)
        def _():
            def z_sent(j, carry):
                z_copy(way, j).wait_send()
                return carry

            lax.fori_loop(0, half, z_sent, 0)

    relaid_out.wait()


def calibrate(hidden, gain, doc_row, matrices):
    tok_count, tp_count = lax.axis_size("tok"), lax.axis_size("tp")
    line = tok_count // QUAD
    tok_dev, depth = hidden.shape
    rows = matrices[0].shape[0]
    sub = rows // tp_count
    widths = [matrix.shape[1] for matrix in matrices]
    chunks = column_chunks(widths)
    count = len(chunks)
    total = sum(widths)
    share = 2 if tp_count % 2 == 0 and tok_dev % 32 == 0 else 1
    vmem = pl.BlockSpec(memory_space=pltpu.VMEM)
    dma = pltpu.SemaphoreType.DMA
    f32, bf16 = jnp.float32, jnp.bfloat16
    queries = widths[0] // (GROUP * HEAD)
    lanes = tok_dev + -tok_dev % LANES
    return pl.pallas_call(
        functools.partial(main_kernel, chunks, line, tp_count, share),
        out_shape=(
            jax.ShapeDtypeStruct((tok_dev, widths[0]), bf16),
            jax.ShapeDtypeStruct((1, widths[0]), f32),
            jax.ShapeDtypeStruct((1, total * tp_count), f32),
            jax.ShapeDtypeStruct((1, sub), f32),
            jax.ShapeDtypeStruct((sub, LANES), f32),
            jax.ShapeDtypeStruct((sub, total * tp_count), bf16),
        ),
        in_specs=[vmem] * 6,
        out_specs=(vmem,) * 5 + (pl.BlockSpec(memory_space=pl.ANY),),
        scratch_shapes=[
            pltpu.VMEM((tok_dev, depth), bf16),
            pltpu.VMEM((tok_dev, LANES), f32),
            pltpu.VMEM((line // 2, tok_dev, HEAD), f32),
            pltpu.VMEM((line // 2, tok_dev, HEAD), f32),
            pltpu.VMEM((1, lanes), jnp.int32),
            pltpu.VMEM((tok_count, 1, lanes), jnp.int32),
            pltpu.VMEM((tok_dev, tok_dev * tok_count), f32),
            pltpu.VMEM((line * tok_dev, QUAD * rows), bf16),
            pltpu.VMEM((1, QUAD * rows), f32),
            pltpu.VMEM((3, 1, QUAD * rows), f32),
        ]
        + [pltpu.VMEM((3, rows, width), bf16) for width in widths]
        + [pltpu.VMEM((line * tok_dev, total), f32)] * 3
        + [pltpu.VMEM((line * tok_dev, widths[2]), bf16)] * 3
        + [
            pltpu.VMEM((line // 2, tok_dev, widths[0]), bf16),
            pltpu.VMEM((tok_dev * tok_count, widths[1] + widths[2]), bf16),
            pltpu.VMEM((sub, total * tp_count), bf16),
            pltpu.VMEM((2, rows, LANES), f32),
            pltpu.VMEM((4, 1, total * tp_count), f32),
            pltpu.VMEM((tp_count + 2, 1, total * tp_count), f32),
            pltpu.VMEM((line, 1, total * tp_count), f32),
            pltpu.VMEM((1, widths[0]), f32),
            pltpu.VMEM((tok_count, 1, widths[0]), f32),
        ]
        + [dma((3, count))] * 2
        + [dma((line, QUAD))] * 4
        + [dma((3, tp_count))] * 2
        + [dma((4,))]
        + [dma((count, line))] * 4
        + [dma((3,))] * 2
        + [dma((1,))] * 2
        + [dma((2, line // 2))] * 2
        + [dma((line,))] * 2
        + [dma((2 * line,))] * 2
        + [dma((queries, line // 2)), dma((queries,))]
        + [dma((tp_count,))] * 2
        + [dma((2,))] * 2
        + [dma((line,))] * 2
        + [dma((1,))] * 2,
        compiler_params=pltpu.CompilerParams(
            collective_id=0, has_side_effects=True, vmem_limit_bytes=63 * 1024 * 1024
        ),
    )(hidden, gain, doc_row, *matrices)


def codes_kernel(
    widths,
    tp_count,
    relaid_ref,
    smooth_ref,
    scale_ref,
    attended_ref,
    peak_ref,
    folded_ref,
    cq_ref,
    ck_ref,
    cv_ref,
    sq_ref,
    sk_ref,
    sv_ref,
    out_ref,
    out_peak_ref,
    out_folded_ref,
    inverse,
):
    tp = lax.axis_index("tp")

    @pl.when(pl.program_id(0) == 0)
    def _():
        out_ref[...] = attended_ref[...]
        out_peak_ref[...] = peak_ref[...]
        out_folded_ref[...] = folded_ref[...]
        inverse[...] = 1.0 / scale_ref[...]
        for which, ref in enumerate((sq_ref, sk_ref, sv_ref)):
            base = sum(widths[:which]) * tp_count + tp * widths[which]
            ref[...] = scale_ref[:, pl.ds(pl.multiple_of(base, 128), widths[which])]

    factor = smooth_ref[...]
    for which, ref in enumerate((cq_ref, ck_ref, cv_ref)):
        base = sum(widths[:which]) * tp_count
        for at in range(0, widths[which] * tp_count, LANES):
            cols = slice(base + at, base + at + LANES)
            ref[:, at : at + LANES] = (
                factor * relaid_ref[:, cols].astype(jnp.float32) * inverse[:, cols]
            )


def coded(relaid, smooth, scale, attended, peak, folded, widths, tp_count):
    sub, total = relaid.shape
    block = math.gcd(sub, 128)
    f32 = jnp.float32

    def striped(width):
        return pl.BlockSpec((block, width), lambda i: (i, 0))

    def whole(array):
        return pl.BlockSpec(array.shape, lambda i: (0, 0))

    full = [jax.ShapeDtypeStruct((sub, width * tp_count), f32) for width in widths]
    part = [jax.ShapeDtypeStruct((1, width), f32) for width in widths]
    rest = [
        jax.ShapeDtypeStruct(array.shape, array.dtype)
        for array in (attended, peak, folded)
    ]
    return pl.pallas_call(
        functools.partial(codes_kernel, widths, tp_count),
        grid=(sub // block,),
        out_shape=full + part + rest,
        in_specs=[striped(total), striped(LANES)]
        + [whole(array) for array in (scale, attended, peak, folded)],
        out_specs=[striped(width * tp_count) for width in widths]
        + [whole(array) for array in part + rest],
        scratch_shapes=[pltpu.VMEM((1, total), f32)],
    )(relaid, smooth, scale, attended, peak, folded)


def on_device(hidden, norm_gain, w_query, w_key, w_value, doc_ids):
    matrices = (w_query, w_key, w_value)
    attended, peak, scale, folded, smooth, relaid = calibrate(
        hidden, norm_gain[None], doc_ids[None], matrices
    )
    *rows, attended, peak, folded = coded(
        relaid,
        smooth,
        scale,
        attended,
        peak,
        folded,
        [matrix.shape[1] for matrix in matrices],
        lax.axis_size("tp"),
    )
    scales = [row[0] for row in rows[3:]]
    return (attended, peak[0], folded[0], *rows[:3], *scales)


def solution(mesh):
    in_specs = (P("tok", None), P(), P("tok", "tp"), P("tok", "tp"), P("tok", "tp"), P("tok"))
    out_specs = (
        P("tok", "tp"),
        P("tp"),
        P(("tok", "tp")),
        P(("tok", "tp"), None),
        P(("tok", "tp"), None),
        P(("tok", "tp"), None),
        P("tp"),
        P("tp"),
        P("tp"),
    )
    return jax.shard_map(
        on_device, mesh=mesh, in_specs=in_specs, out_specs=out_specs, check_vma=False
    )
```

```python
import functools
import math

import jax
import jax.numpy as jnp
from jax import lax
from jax.experimental import pallas as pl
from jax.experimental.pallas import tpu as pltpu
from jax.sharding import PartitionSpec as P

HEAD = 128
KVH = 8
QHEADS = 32
GROUP = QHEADS // KVH
LANES = 128
FAR = 1 << 30

MESH = pl.DeviceIdType.MESH
QUAD = 4


def column_chunks(widths, most=GROUP * HEAD):
    return [
        (which, start, min(most, widths[which] - start))
        for which in (1, 2, 0)
        for start in range(0, widths[which], most)
    ]


def as_column(row):
    return jnp.transpose(jnp.broadcast_to(row, (LANES, LANES)))

def main_kernel(
    chunks,
    line,
    tp_count,
    share,
    hidden_ref,
    gain_ref,
    doc_ref,
    wq_from,
    wk_from,
    wv_from,
    out_ref,
    out_peak_ref,
    scale_ref,
    folded_ref,
    smooth_ref,
    relaid_ref,
    normed,
    root,
    cosine,
    sine,
    doc_row,
    docs,
    bias,
    tokens,
    mine,
    theirs,
    wq_ref,
    wk_ref,
    wv_ref,
    held_q,
    held_k,
    held_v,
    partial,
    from_left,
    from_right,
    query,
    cache,
    relaid,
    channel,
    column,
    column_tp,
    column_line,
    out_mine,
    out_all,
    w_local,
    w_send,
    w_recv,
    t_send,
    t_recv,
    m_send,
    m_recv,
    x_send,
    x_recv,
    x_local,
    r_send,
    r_recv,
    l_send,
    l_recv,
    p_send,
    p_recv,
    d_send,
    d_recv,
    z_send,
    z_recv,
    y_send,
    y_recv,
    s_send,
    s_recv,
    q_send,
    q_recv,
    c_send,
    c_recv,
    b_send,
    b_recv,
    a_send,
    a_recv,
    o_send,
    o_recv,
):
    me = lax.axis_index("tok")
    tp = lax.axis_index("tp")
    tok_count = line * QUAD
    quad = lax.rem(me, QUAD)
    place = me // QUAD
    rows = wq_ref.shape[0]
    tok_dev = hidden_ref.shape[0]
    depth = hidden_ref.shape[1]
    width = QUAD * rows
    keys = tok_dev * tok_count
    sib = me + 1 - 2 * lax.rem(me, 2)
    side = me + 2 - 4 * (quad // 2)
    side_sib = side + 1 - 2 * lax.rem(me, 2)
    own = (wq_ref, wk_ref, wv_ref)
    held = (held_q, held_k, held_v)
    widths = [ref.shape[1] for ref in own]
    sub = rows // tp_count
    count = len(chunks)
    kv_chunks = [c for c in range(count) if chunks[c][0] > 0]
    q_chunks = [c for c in range(count) if chunks[c][0] == 0]
    kv_here = widths[1] // HEAD
    last = count - 1
    lead = len(kv_chunks)
    half = line // 2
    base = jnp.where(2 * place < line, 0, half)
    at_end = (place == 0) | (place == line - 1)

    def remote(src, dst, send, recv, tok, tp_to=None):
        return pltpu.make_async_remote_copy(
            src_ref=src,
            dst_ref=dst,
            send_sem=send,
            recv_sem=recv,
            device_id=(tok, tp if tp_to is None else tp_to),
            device_id_type=MESH,
        )

    def rows_of(tok):
        return pl.ds(pl.multiple_of(tok * tok_dev, 16), tok_dev)

    def meet(barrier):
        def greet(step, carry):
            other = lax.rem(me + step, tok_count)
            pl.semaphore_signal(
                barrier, inc=1, device_id=(other, tp), device_id_type=MESH
            )
            return carry

        lax.fori_loop(1, tok_count, greet, 0)
        for step in range(1, tp_count):
            other = lax.rem(tp + step, tp_count)
            pl.semaphore_signal(
                barrier, inc=1, device_id=(me, other), device_id_type=MESH
            )

    def w_copy(kind, c):
        which, start, size = chunks[c]
        cols = pl.ds(start, size)
        if kind == 2:
            src = held[which].at[1, :, cols]
        else:
            src = own[which].at[:, cols]
        return remote(
            src,
            held[which].at[kind, :, cols],
            w_send.at[which],
            w_recv.at[kind, c],
            side if kind == 1 else sib,
        )

    ahead = 3

    def weights_start(c):
        w_copy(1, c).start()
        w_copy(0, c).start()

    part = tok_dev // share
    piece = lax.rem(tp, share)
    mate = tp + 1 - 2 * piece
    first = pl.multiple_of(piece * part, 16)

    def columns_of(tok):
        return pl.ds(pl.multiple_of(lax.rem(tok, QUAD) * rows, 128), rows)

    members = (me, side, sib, side_sib)
    cuts = 2 if rows % (2 * LANES) == 0 else 1
    slab = rows // cuts

    def channels(k):
        start = lax.rem(members[k // cuts], QUAD) * rows + (k % cuts) * slab
        return pl.multiple_of(start, 128)


    def t_copy(step, k):
        to = lax.rem(place + step, line)
        base = to * width + channels(k)
        return remote(
            normed.at[pl.ds(first, part), pl.ds(pl.multiple_of(base, 128), slab)],
            tokens.at[
                pl.ds(pl.multiple_of(place * tok_dev + first, 16), part),
                pl.ds(channels(k), slab),
            ],
            t_send.at[0],
            t_recv.at[step, k],
            to * QUAD + quad,
        )

    def m_copy(step, k):
        source = lax.rem(place - step + line, line)
        start = pl.multiple_of(source * tok_dev + piece * part, 16)
        got = tokens.at[pl.ds(start, part), pl.ds(channels(k), slab)]
        return remote(got, got, m_send.at[0], m_recv.at[step, k], me, mate)

    def tokens_sent(sem):
        every = tokens.at[pl.ds(0, (line - 1) * part)]
        remote(every, every, sem, sem, sib).wait_send()

    wide = [sum(widths[:i]) * tp_count for i in range(3)]

    def x_copy(which, step):
        to = lax.rem(tp + step, tp_count)
        size = widths[which]
        src = own[which].at[pl.ds(pl.multiple_of(to * sub, 16), sub)]
        dst = relaid.at[:, pl.ds(pl.multiple_of(wide[which] + tp * size, 128), size)]
        if step == 0:
            return pltpu.make_async_copy(src, dst, x_local.at[0])
        return remote(src, dst, x_send.at[0], x_recv.at[0], me, to)

    def x_all():
        size = sum(widths)
        every = relaid.at[:, pl.ds(0, size)]
        pltpu.make_async_copy(every, every, x_local.at[0]).wait()
        if tp_count > 1:
            every = relaid.at[:, pl.ds(0, (tp_count - 1) * size)]
            remote(every, every, x_send.at[0], x_recv.at[0], sib).wait()

    relaid_out = pltpu.make_async_copy(relaid, relaid_ref, x_local.at[1])

    def d_copy(step):
        to = lax.rem(me + step, tok_count)
        return remote(doc_row, docs.at[me], d_send.at[0], d_recv.at[0], to)

    def d_all():
        every = docs.at[pl.ds(0, tok_count - 1)]
        return remote(every, every, d_send.at[0], d_recv.at[0], sib)

    def p_copy(kind):
        return remote(
            mine,
            theirs.at[kind],
            p_send.at[0],
            p_recv.at[0],
            (sib, side, side_sib)[kind],
        )

    def each(copy):
        def go(step, carry):
            copy(step).start()
            return carry

        lax.fori_loop(1, tok_count, go, 0)

    tiles_at = math.gcd(slab // LANES, 4)

    def normalise(start, size, base, reach):
        def go(i, carry):
            for j in range(tiles_at):
                at = base + (tiles_at * i + j) * LANES
                cols = pl.ds(pl.multiple_of(at, LANES), LANES)
                block = hidden_ref[pl.ds(start, size), cols].astype(jnp.float32)
                block = block * root[pl.ds(start, size), :] * gain_ref[:, cols]
                normed[pl.ds(start, size), cols] = block.astype(jnp.bfloat16)
            return carry

        lax.fori_loop(0, reach // (tiles_at * LANES), go, 0)

    loads = [
        pltpu.make_async_copy(source, own[which], w_local.at[which])
        for which, source in enumerate((wq_from, wk_from, wv_from))
    ]
    for which in (1, 2, 0):
        loads[which].start()
    barrier = pltpu.get_barrier_semaphore()
    meet(barrier)
    doc_row[...] = jnp.full(doc_row.shape, FAR, jnp.int32)
    doc_row[:, :tok_dev] = doc_ref[...]
    docs[me] = doc_row[...]

    def squares(i, total):
        for j in range(4):
            cols = pl.ds(pl.multiple_of((4 * i + j) * LANES, LANES), LANES)
            block = hidden_ref[:, cols].astype(jnp.float32)
            total = total + block * block
        return total

    total = lax.fori_loop(
        0, depth // (4 * LANES), squares, jnp.zeros((tok_dev, LANES), jnp.float32)
    )
    mean = jnp.sum(total, axis=1, keepdims=True) / depth
    root[...] = jnp.broadcast_to(lax.rsqrt(mean + 1e-05), (tok_dev, LANES))
    pl.semaphore_wait(barrier, tok_count - 1 + tp_count - 1)

    each(d_copy)
    for load in loads:
        load.wait()
    for c in range(min(ahead, count)):
        weights_start(c)

    for k in range(QUAD * cuts):

        def send_tokens(i, carry):
            step = jnp.where(2 * place < line, line - i, i)
            to = lax.rem(place + step, line)
            normalise(first, part, to * width + channels(k), slab)
            t_copy(step, k).start()
            return carry

        lax.fori_loop(1, line, send_tokens, 0)
    normalise(0, tok_dev, place * width, width)
    tokens[rows_of(place)] = normed[:, pl.ds(pl.multiple_of(place * width, 128), width)]

    lane = lax.broadcasted_iota(jnp.int32, (tok_dev, HEAD), 1)
    turns = lax.rem(lane, HEAD // 2).astype(jnp.float32)
    speed = jnp.exp(turns * (-2.0 * math.log(10000.0) / HEAD))

    def tables(j, carry):
        spot = ((base + j) * QUAD + quad) * tok_dev
        spot = spot + lax.broadcasted_iota(jnp.int32, (tok_dev, HEAD), 0)
        angles = spot.astype(jnp.float32) * speed
        cosine[j] = jnp.cos(angles)
        sine[j] = jnp.where(lane < HEAD // 2, -1.0, 1.0) * jnp.sin(angles)
        return carry

    lax.fori_loop(0, half, tables, 0)
    near = sorted(range(1, line), key=lambda step: min(step, line - step))
    for k in range(QUAD * cuts):
        for step in near:
            t_copy(step, k).wait_recv()
            if share == 2:
                m_copy(step, k).start()
    base_of = [sum(size for _, _, size in chunks[:c]) for c in range(count)]

    def span(c):
        return slice(base_of[c], base_of[c] + chunks[c][2])

    def block(d):
        return pl.ds(pl.multiple_of(d * tok_dev, 8), tok_dev)

    def spot_of(c, d):
        return c * half + lax.rem(d, half) if c < last else last * half + d

    def sent_of(c, d):
        return c if c < last else last + d

    def right(c, d):
        here = partial.at[block(d), span(c)]
        there = from_left.at[block(d), span(c)]
        send, recv = r_send.at[sent_of(c, d)], r_recv.at[spot_of(c, d)]
        return remote(here, there, send, recv, me + QUAD)

    def left(c, d):
        here = partial.at[block(d), span(c)]
        there = from_right.at[block(d), span(c)]
        send, recv = l_send.at[sent_of(c, d)], l_recv.at[spot_of(c, d)]
        return remote(here, there, send, recv, me - QUAD)

    def added(c, d, way):
        (right, left)[way](c, d).wait_recv()
        landed = (from_left, from_right)[way]
        return partial[block(d), span(c)] + landed[block(d), span(c)]

    def pass_on(c, d, way):
        partial[block(d), span(c)] = added(c, d, way)
        (right, left)[way](c, d).start()

    def sends(c, way):
        if c < last:
            return half, (lambda i: half + i) if way == 0 else (lambda i: half - 1 - i)
        if way == 0:
            return line - 1, lambda i: line - 1 - i
        return line - 1, lambda i: i

    def goes(c, d, way):
        if c < last:
            return place < line - 1 if way == 0 else place > 0
        return d > place if way == 0 else d < place

    def first_sends(c):
        for way in range(2):

            @pl.when(place == (0 if way == 0 else line - 1))
            def _():
                size, pick = sends(c, way)

                def go(i, carry):
                    (right, left)[way](c, pick(i)).start()
                    return carry

                lax.fori_loop(0, size, go, 0)

    def onward(c, i, way):
        size, pick = sends(c, way)
        inside = place > 0 if way == 0 else place < line - 1
        d = pick(i)

        @pl.when((i < size) & inside & goes(c, d, way))
        def _():
            pass_on(c, d, way)

    def weave(far, near):
        def go(nearest, i):
            if far is not None:
                onward(far, i, 1 - nearest)
            if near is not None:
                onward(near, i, nearest)

        def left_half(i, carry):
            go(0, i)
            return carry

        def right_half(i, carry):
            go(1, i)
            return carry

        top = line - 1 if last in (far, near) else half

        @pl.when(2 * place < line)
        def _():
            lax.fori_loop(0, top, left_half, 0)

        @pl.when(2 * place >= line)
        def _():
            lax.fori_loop(0, top, right_half, 0)

    def settle(c, j):
        which, start, size = chunks[c]
        d = base + j
        for head in range(size // HEAD):
            at = base_of[c] + head * HEAD
            states = partial[block(d), at : at + HEAD]
            if which < 2:
                states = (
                    states * cosine[j] + pltpu.roll(states, HEAD // 2, 1) * sine[j]
                )
            at = start + head * HEAD + (widths[1] if which == 2 else 0)
            if which == 0:
                query[j, :, at : at + HEAD] = states.astype(jnp.bfloat16)
            else:
                rows_at = rows_of(d * QUAD + quad)
                cache[rows_at, at : at + HEAD] = states.astype(jnp.bfloat16)

    def q_copy(c, j):
        which, start, size = chunks[c]
        got = query.at[j, :, pl.ds(start, size)]
        to = (base + j) * QUAD + quad
        return remote(got, got, q_send.at[0], q_recv.at[c - lead], to)

    def finish(c):
        if c == last:
            for way in range(2):

                @pl.when(place > 0 if way == 0 else place < line - 1)
                def _():
                    partial[block(place), span(c)] = added(c, place, way)

            settle(c, place - base)
            return

        @pl.when(at_end)
        def _():
            def go(i, carry):
                j = jnp.where(place == 0, half - 1 - i, i)
                d = base + j
                for way in range(2):

                    @pl.when(place == (line - 1 if way == 0 else 0))
                    def _():
                        partial[block(d), span(c)] = added(c, d, way)

                settle(c, j)
                if chunks[c][0] == 0:

                    @pl.when(d != place)
                    def _():
                        q_copy(c, j).start()

                return carry

            lax.fori_loop(0, half, go, 0)

    def tokens_ready(c, k):
        if c == 0 and share == 2:
            for step in near:
                for piece_at in range(cuts):
                    m_copy(step, k * cuts + piece_at).wait_recv()

    def project(c):
        which, start, size = chunks[c]
        cols = slice(start, start + size)
        tokens_ready(c, 0)
        total = jnp.dot(
            tokens[:, columns_of(me)],
            own[which][:, cols],
            preferred_element_type=jnp.float32,
        )
        w_copy(1, c).wait_recv()
        w_copy(2, c).start()
        if c + ahead < count:
            weights_start(c + ahead)
        for k, kind in ((1, 1), (2, 0), (3, 2)):
            tokens_ready(c, k)
            if kind != 1:
                w_copy(kind, c).wait_recv()
            total += jnp.dot(
                tokens[:, columns_of(members[k])],
                held[which][kind, :, cols],
                preferred_element_type=jnp.float32,
            )
        partial[:, span(c)] = total
        first_sends(c)

    def kv_rows(spot, of_side=False):
        at = lax.rem(side, QUAD) if of_side else quad
        return cache.at[rows_of(spot * QUAD + at)]

    def z_copy(way, j):
        got = kv_rows(j + way * half)
        to = me - QUAD if way else me + QUAD
        return remote(got, got, z_send.at[way], z_recv.at[way, j], to)

    def y_copy(spot):
        got = kv_rows(spot)
        return remote(got, got, y_send.at[0], y_recv.at[spot], side)

    def y_arrival(spot):
        got = kv_rows(spot, True)
        return remote(got, got, y_send.at[0], y_recv.at[spot], side)

    def s_copy(spot, of_side):
        got = kv_rows(spot, of_side)
        return remote(got, got, s_send.at[0], s_recv.at[0], sib)

    def s_all():
        every = cache.at[pl.ds(0, 2 * line * tok_dev)]
        return remote(every, every, s_send.at[0], s_recv.at[0], sib)

    def kv_block(way, j, fresh):
        if not fresh:
            z_copy(way, j).wait_recv()

        @pl.when(place > 0 if way else place < line - 1)
        def _():
            z_copy(way, j).start()

        y_copy(j + way * half).start()
        s_copy(j + way * half, False).start()

    def kv_pass(way, fresh, near=None):
        def go(j, carry):
            kv_block(way, j, fresh)
            if near is not None:
                onward(near, j, 1 - way)
            return carry

        lax.fori_loop(0, half, go, 0)

    def kv_start():
        for way in range(2):

            @pl.when(place == way * (line - 1))
            def _():
                kv_pass(way, True)

    def kv_near():
        for way in range(2):
            nearer = 2 * place >= line if way else 2 * place < line

            @pl.when(nearer & jnp.logical_not(at_end))
            def _():
                kv_pass(way, False)

    def kv_far(near):
        for way in range(2):

            @pl.when(2 * place < line if way else 2 * place >= line)
            def _():
                kv_pass(way, False, near)

    def kv_side():
        def go(spot, carry):
            y_arrival(spot).wait_recv()
            s_copy(spot, True).start()
            return carry

        lax.fori_loop(0, line, go, 0)

    def kv_ready():
        s_all().wait_recv()

    def mask():
        d_all().wait()
        wanted = jnp.transpose(
            jnp.broadcast_to(doc_row[...].astype(jnp.float32), (LANES, LANES))
        )[:tok_dev]

        def go(tok, total):
            before = docs[tok].astype(jnp.float32) < wanted
            return total + jnp.where(before, 1.0, 0.0)

        total = lax.fori_loop(
            0, tok_count, go, jnp.zeros((tok_dev, LANES), jnp.float32)
        )
        since = jnp.sum(total, axis=1, keepdims=True).astype(jnp.int32)
        spot = lax.broadcasted_iota(jnp.int32, (tok_dev, keys), 0) + me * tok_dev
        at = lax.broadcasted_iota(jnp.int32, (tok_dev, keys), 1)
        bias[...] = jnp.where((at >= since) & (at <= spot), 0.0, -1e30)

    turn = math.log2(math.e) / math.sqrt(HEAD)

    def attend(g):
        heads = [
            slice((g * GROUP + h) * HEAD, (g * GROUP + h + 1) * HEAD)
            for h in range(GROUP)
        ]
        if g + lead < last:

            @pl.when(jnp.logical_not(at_end))
            def _():
                q_copy(g + lead, place - base).wait_recv()

        asked = jnp.concatenate(
            [query[place - base, :, head] for head in heads], axis=0
        )
        key = cache[:, g * HEAD : (g + 1) * HEAD]
        value = cache[:, (kv_here + g) * HEAD : (kv_here + g + 1) * HEAD]
        scores = lax.dot_general(
            asked, key, (((1,), (1,)), ((), ())), preferred_element_type=jnp.float32
        )
        scores = (
            scores.reshape(GROUP, tok_dev, keys) + bias[...][None]
        ).reshape(GROUP * tok_dev, keys)
        weights = jnp.exp2((scores - jnp.max(scores, axis=1, keepdims=True)) * turn)
        totals = jnp.sum(weights, axis=1, keepdims=True)
        mixed = jnp.dot(
            weights.astype(jnp.bfloat16), value, preferred_element_type=jnp.float32
        )
        mixed = (mixed / totals).astype(jnp.bfloat16)
        for h, head in enumerate(heads):
            piece = mixed[h * tok_dev : (h + 1) * tok_dev]
            out_ref[:, head] = piece
            out_mine[:, head] = jnp.max(
                jnp.abs(piece.astype(jnp.float32)), axis=0, keepdims=True
            )
        cols = pl.ds(g * GROUP * HEAD, GROUP * HEAD)
        out_all[me, :, cols] = out_mine[:, cols]
        each(functools.partial(o_copy, g))

    def o_copy(g, step):
        cols = pl.ds(g * GROUP * HEAD, GROUP * HEAD)
        to = lax.rem(me + step, tok_count)
        return remote(
            out_mine.at[:, cols], out_all.at[me, :, cols], o_send.at[0], o_recv.at[0], to
        )

    def o_all():
        every = out_all.at[pl.ds(0, tok_count - 1)]
        return remote(every, every, o_send.at[0], o_recv.at[0], sib)

    def smooth():
        remote(theirs, theirs, p_send.at[0], p_recv.at[0], sib).wait()
        peak = jnp.maximum(
            jnp.maximum(mine[...], theirs[0]), jnp.maximum(theirs[1], theirs[2])
        )
        mine[...] = peak
        for i in range(rows // LANES):
            here = slice(i * LANES, (i + 1) * LANES)
            at = pl.ds(pl.multiple_of(quad * rows + i * LANES, LANES), LANES)
            channel[0, here] = as_column(mine[:, at])
            at = pl.ds(pl.multiple_of(me * rows + i * LANES, LANES), LANES)
            channel[1, here] = as_column(gain_ref[:, at])
        x_all()
        relaid_out.start()
        tiles = relaid.shape[1] // LANES

        def tallest(i, most):
            cols = pl.ds(pl.multiple_of(i * LANES, LANES), LANES)
            return jnp.maximum(most, jnp.abs(relaid[:, cols].astype(jnp.float32)))

        most = lax.fori_loop(0, tiles, tallest, jnp.zeros((sub, LANES), jnp.float32))
        weight_peak = jnp.max(most, axis=1, keepdims=True)
        ours = pl.ds(pl.multiple_of(tp * sub, 16), sub)
        factor = jnp.sqrt(jnp.maximum(channel[0, ours, :], 1e-05)) / jnp.sqrt(
            jnp.maximum(weight_peak, 1e-05)
        )
        smooth_ref[...] = factor
        channel[0, ours, :] = channel[1, ours, :] / factor

        def highest(i, carry):
            cols = pl.ds(pl.multiple_of(i * LANES, LANES), LANES)
            column[0, :, cols] = jnp.max(
                jnp.abs(smooth_ref[...] * relaid[:, cols].astype(jnp.float32)),
                axis=0,
                keepdims=True,
            )
            return carry

        lax.fori_loop(0, tiles, highest, 0)
        for i in range(-(-sub // LANES)):
            size = min(LANES, sub - i * LANES)
            start = pl.multiple_of(tp * sub + i * LANES, 16)
            tile = channel[0, pl.ds(start, size), :]
            if size < LANES:
                tile = jnp.concatenate(
                    [tile, jnp.zeros((LANES - size, LANES), jnp.float32)], axis=0
                )
            folded_ref[:, i * LANES : i * LANES + size] = jnp.transpose(tile)[
                0:1, :size
            ]
        for step in range(1, tp_count):
            c_copy(step).start()

    def c_copy(step):
        return remote(
            column.at[0],
            column_tp.at[step],
            c_send.at[0],
            c_recv.at[0],
            me,
            lax.rem(tp + step, tp_count),
        )

    def b_copy(stage):
        return remote(
            column.at[1 + stage],
            column_tp.at[tp_count + stage],
            b_send.at[stage],
            b_recv.at[stage],
            (sib, side)[stage],
        )

    def a_copy(step):
        return remote(
            column.at[3],
            column_line.at[step],
            a_send.at[0],
            a_recv.at[0],
            lax.rem(place + step, line) * QUAD + quad,
        )

    def columns_tp():
        joined = column[0]
        if tp_count > 1:
            every = column_tp.at[pl.ds(0, tp_count - 1)]
            remote(every, every, c_send.at[0], c_recv.at[0], sib).wait()
        for step in range(1, tp_count):
            joined = jnp.maximum(joined, column_tp[step])
        column[1] = joined
        b_copy(0).start()

    def columns_sib():
        b_copy(0).wait()
        column[2] = jnp.maximum(column[1], column_tp[tp_count])
        b_copy(1).start()

    def columns_side():
        b_copy(1).wait()
        column[3] = jnp.maximum(column[2], column_tp[tp_count + 1])
        for step in range(1, line):
            a_copy(step).start()

    def columns_line():
        joined = column[3]
        every = column_line.at[pl.ds(0, line - 1)]
        remote(every, every, a_send.at[0], a_recv.at[0], sib).wait()
        for step in range(1, line):
            joined = jnp.maximum(joined, column_line[step])
        scale_ref[...] = jnp.maximum(joined, 1e-05) / 127.0

    def early():
        mine[...] = jnp.max(
            jnp.abs(tokens[...].astype(jnp.float32)), axis=0, keepdims=True
        )
        for kind in range(3):
            p_copy(kind).start()

    ran = set()

    def once(act, c, *rest):
        if c <= last and (act, c) not in ran:
            ran.add((act, c))
            act(c, *rest)

    def pair(far, near):
        far = None if far > last or ("far", far) in ran else far
        near = None if near > last or ("near", near) in ran else near
        ran.update({("far", far), ("near", near)})
        if far is not None or near is not None:
            weave(far, near)

    def split_project(c, ends):
        @pl.when(at_end if ends else jnp.logical_not(at_end))
        def _():
            project(c)

    once(project, 0)
    early()
    for which in (1, 2, 0):
        for step in range(tp_count):
            x_copy(which, step).start()
    for c in range(1, lead):
        once(project, c)
    for c in range(lead):
        pair(c - 1 if c else FAR, c)
    once(project, lead)
    once(finish, kv_chunks[0])
    pair(lead - 1, lead)
    once(project, lead + 1)
    for c in kv_chunks:
        once(finish, c)
    kv_start()
    mask()
    pair(lead, lead + 1)
    smooth()
    once(project, lead + 2)
    if lead < last - 1:
        once(finish, lead)
    if lead + 3 <= last:
        split_project(lead + 3, True)
    pair(lead + 1, FAR)
    if lead + 1 < last - 1:
        once(finish, lead + 1)
    kv_near()
    if lead + 3 <= last:
        split_project(lead + 3, False)
        ran.add((project, lead + 3))
    if lead + 2 < last:
        ran.add(("near", lead + 2))
        kv_far(lead + 2)
    else:
        kv_far(None)
    columns_tp()
    for c in range(lead, count):
        once(project, c)
        pair(c - 1, c)
    columns_sib()
    pair(last, FAR)
    kv_side()
    columns_side()
    kv_ready()
    swap = last - 1 > lead

    def attend_where(g, ends):
        @pl.when(at_end if ends else jnp.logical_not(at_end))
        def _():
            attend(g)

    for c in range(lead, count):
        once(finish, c)
        if swap and c == last - 1:
            attend_where(c - lead, True)
        else:
            attend(c - lead)
    if swap:
        attend_where(last - 1 - lead, False)
    columns_line()
    o_all().wait()
    out_peak_ref[...] = jnp.max(out_all[...], axis=0)

    tokens_sent(t_send.at[0])
    if share == 2:
        tokens_sent(m_send.at[0])
    for which in range(3):
        every = held[which]
        remote(every, every, w_send.at[which], w_send.at[which], sib).wait_send()
    for way in range(2):
        moves = place > 0 if way else place < line - 1

        @pl.when(moves)
        def _():
            sems = (r_send, l_send)[way]
            for c in range(last):
                every = partial.at[pl.ds(0, half * tok_dev), span(c)]
                remote(every, every, sems.at[c], sems.at[c], sib).wait_send()
            every = cache.at[pl.ds(0, half * tok_dev)]
            remote(every, every, z_send.at[way], z_send.at[way], sib).wait_send()

        def sent(d, carry):
            @pl.when(d < place if way else d > place)
            def _():
                (right, left)[way](last, d).wait_send()

            return carry

        lax.fori_loop(0, line, sent, 0)
    if last > lead and half > 1:

        @pl.when(at_end)
        def _():
            every = query.at[
                pl.ds(0, half - 1), :, pl.ds(0, (last - lead) * GROUP * HEAD)
            ]
            remote(every, every, q_send.at[0], q_send.at[0], sib).wait_send()

    s_all().wait_send()
    every = cache.at[pl.ds(0, line * tok_dev)]
    remote(every, every, y_send.at[0], y_send.at[0], sib).wait_send()
    relaid_out.wait()


def calibrate(hidden, gain, doc_row, matrices):
    tok_count, tp_count = lax.axis_size("tok"), lax.axis_size("tp")
    line = tok_count // QUAD
    tok_dev, depth = hidden.shape
    rows = matrices[0].shape[0]
    sub = rows // tp_count
    widths = [matrix.shape[1] for matrix in matrices]
    chunks = column_chunks(widths)
    count = len(chunks)
    total = sum(widths)
    share = 2 if tp_count % 2 == 0 and tok_dev % 32 == 0 else 1
    vmem = pl.BlockSpec(memory_space=pltpu.VMEM)
    dma = pltpu.SemaphoreType.DMA
    f32, bf16 = jnp.float32, jnp.bfloat16
    queries = widths[0] // (GROUP * HEAD)
    lanes = tok_dev + -tok_dev % LANES
    return pl.pallas_call(
        functools.partial(main_kernel, chunks, line, tp_count, share),
        out_shape=(
            jax.ShapeDtypeStruct((tok_dev, widths[0]), bf16),
            jax.ShapeDtypeStruct((1, widths[0]), f32),
            jax.ShapeDtypeStruct((1, total * tp_count), f32),
            jax.ShapeDtypeStruct((1, sub), f32),
            jax.ShapeDtypeStruct((sub, LANES), f32),
            jax.ShapeDtypeStruct((sub, total * tp_count), bf16),
        ),
        in_specs=[vmem] * 3 + [pl.BlockSpec(memory_space=pl.ANY)] * 3,
        out_specs=(vmem,) * 5 + (pl.BlockSpec(memory_space=pl.ANY),),
        scratch_shapes=[
            pltpu.VMEM((tok_dev, depth), bf16),
            pltpu.VMEM((tok_dev, LANES), f32),
            pltpu.VMEM((line // 2, tok_dev, HEAD), f32),
            pltpu.VMEM((line // 2, tok_dev, HEAD), f32),
            pltpu.VMEM((1, lanes), jnp.int32),
            pltpu.VMEM((tok_count, 1, lanes), jnp.int32),
            pltpu.VMEM((tok_dev, tok_dev * tok_count), f32),
            pltpu.VMEM((line * tok_dev, QUAD * rows), bf16),
            pltpu.VMEM((1, QUAD * rows), f32),
            pltpu.VMEM((3, 1, QUAD * rows), f32),
        ]
        + [pltpu.VMEM((rows, width), bf16) for width in widths]
        + [pltpu.VMEM((3, rows, width), bf16) for width in widths]
        + [pltpu.VMEM((line * tok_dev, total), f32)] * 3
        + [
            pltpu.VMEM((line // 2, tok_dev, widths[0]), bf16),
            pltpu.VMEM((tok_dev * tok_count, widths[1] + widths[2]), bf16),
            pltpu.VMEM((sub, total * tp_count), bf16),
            pltpu.VMEM((2, rows, LANES), f32),
            pltpu.VMEM((4, 1, total * tp_count), f32),
            pltpu.VMEM((tp_count + 2, 1, total * tp_count), f32),
            pltpu.VMEM((line, 1, total * tp_count), f32),
            pltpu.VMEM((1, widths[0]), f32),
            pltpu.VMEM((tok_count, 1, widths[0]), f32),
        ]
        + [dma((3,)), dma((3,)), dma((3, count))]
        + [dma((1,)), dma((line, 2 * QUAD))] * 2
        + [dma((1,))] * 2
        + [dma((2,))]
        + [dma((count - 1 + line,)), dma(((count - 1) * (line // 2) + line,))] * 2
        + [dma((1,))] * 4
        + [dma((2,)), dma((2, line // 2))]
        + [dma((1,)), dma((line,))]
        + [dma((1,))] * 2
        + [dma((1,)), dma((queries,))]
        + [dma((1,))] * 2
        + [dma((2,))] * 2
        + [dma((1,))] * 4,
        compiler_params=pltpu.CompilerParams(
            collective_id=0, has_side_effects=True, vmem_limit_bytes=63 * 1024 * 1024
        ),
    )(hidden, gain, doc_row, *matrices)


def codes_kernel(
    widths,
    tp_count,
    relaid_ref,
    smooth_ref,
    scale_ref,
    attended_ref,
    peak_ref,
    folded_ref,
    cq_ref,
    ck_ref,
    cv_ref,
    sq_ref,
    sk_ref,
    sv_ref,
    out_ref,
    out_peak_ref,
    out_folded_ref,
    inverse,
):
    tp = lax.axis_index("tp")

    @pl.when(pl.program_id(0) == 0)
    def _():
        out_ref[...] = attended_ref[...]
        out_peak_ref[...] = peak_ref[...]
        out_folded_ref[...] = folded_ref[...]
        inverse[...] = 1.0 / scale_ref[...]
        for which, ref in enumerate((sq_ref, sk_ref, sv_ref)):
            base = sum(widths[:which]) * tp_count + tp * widths[which]
            ref[...] = scale_ref[:, pl.ds(pl.multiple_of(base, 128), widths[which])]

    factor = smooth_ref[...]
    for which, ref in enumerate((cq_ref, ck_ref, cv_ref)):
        base = sum(widths[:which]) * tp_count
        for at in range(0, widths[which] * tp_count, LANES):
            cols = slice(base + at, base + at + LANES)
            ref[:, at : at + LANES] = (
                factor * relaid_ref[:, cols].astype(jnp.float32) * inverse[:, cols]
            )


def coded(relaid, smooth, scale, attended, peak, folded, widths, tp_count):
    sub, total = relaid.shape
    block = math.gcd(sub, 128)
    f32 = jnp.float32

    def striped(width):
        return pl.BlockSpec((block, width), lambda i: (i, 0))

    def whole(array):
        return pl.BlockSpec(array.shape, lambda i: (0, 0))

    full = [jax.ShapeDtypeStruct((sub, width * tp_count), f32) for width in widths]
    part = [jax.ShapeDtypeStruct((1, width), f32) for width in widths]
    rest = [
        jax.ShapeDtypeStruct(array.shape, array.dtype)
        for array in (attended, peak, folded)
    ]
    return pl.pallas_call(
        functools.partial(codes_kernel, widths, tp_count),
        grid=(sub // block,),
        out_shape=full + part + rest,
        in_specs=[striped(total), striped(LANES)]
        + [whole(array) for array in (scale, attended, peak, folded)],
        out_specs=[striped(width * tp_count) for width in widths]
        + [whole(array) for array in part + rest],
        scratch_shapes=[pltpu.VMEM((1, total), f32)],
    )(relaid, smooth, scale, attended, peak, folded)


def on_device(hidden, norm_gain, w_query, w_key, w_value, doc_ids):
    matrices = (w_query, w_key, w_value)
    attended, peak, scale, folded, smooth, relaid = calibrate(
        hidden, norm_gain[None], doc_ids[None], matrices
    )
    *rows, attended, peak, folded = coded(
        relaid,
        smooth,
        scale,
        attended,
        peak,
        folded,
        [matrix.shape[1] for matrix in matrices],
        lax.axis_size("tp"),
    )
    scales = [row[0] for row in rows[3:]]
    return (attended, peak[0], folded[0], *rows[:3], *scales)


def solution(mesh):
    in_specs = (P("tok", None), P(), P("tok", "tp"), P("tok", "tp"), P("tok", "tp"), P("tok"))
    out_specs = (
        P("tok", "tp"),
        P("tp"),
        P(("tok", "tp")),
        P(("tok", "tp"), None),
        P(("tok", "tp"), None),
        P(("tok", "tp"), None),
        P("tp"),
        P("tp"),
        P("tp"),
    )
    return jax.shard_map(
        on_device, mesh=mesh, in_specs=in_specs, out_specs=out_specs, check_vma=False
    )
```

```python
import functools
import math

import jax
import jax.numpy as jnp
from jax import lax
from jax.experimental import pallas as pl
from jax.experimental.pallas import tpu as pltpu
from jax.sharding import PartitionSpec as P

HEAD = 128
KVH = 8
QHEADS = 32
GROUP = QHEADS // KVH
LANES = 128
FAR = 1 << 30

MESH = pl.DeviceIdType.MESH
QUAD = 4


def column_chunks(widths, most=GROUP * HEAD):
    return [
        (which, start, min(most, widths[which] - start))
        for which in (1, 2, 0)
        for start in range(0, widths[which], most)
    ]


def as_column(row):
    return jnp.transpose(jnp.broadcast_to(row, (LANES, LANES)))

def main_kernel(
    chunks,
    line,
    tp_count,
    share,
    hidden_from,
    gain_from,
    doc_from,
    wq_from,
    wk_from,
    wv_from,
    out_ref,
    out_peak_ref,
    scale_ref,
    folded_ref,
    smooth_ref,
    relaid_ref,
    normed,
    root,
    cosine,
    sine,
    doc_row,
    docs,
    bias,
    tokens,
    mine,
    theirs,
    hidden_ref,
    gain_ref,
    doc_ref,
    wq_ref,
    wk_ref,
    wv_ref,
    held_q,
    held_k,
    held_v,
    partial,
    from_left,
    from_right,
    query,
    cache,
    relaid,
    channel,
    column,
    column_tp,
    column_line,
    out_mine,
    out_all,
    w_local,
    w_send,
    w_recv,
    t_send,
    t_recv,
    m_send,
    m_recv,
    x_send,
    x_recv,
    x_local,
    r_send,
    r_recv,
    l_send,
    l_recv,
    p_send,
    p_recv,
    d_send,
    d_recv,
    z_send,
    z_recv,
    y_send,
    y_recv,
    s_send,
    s_recv,
    q_send,
    q_recv,
    c_send,
    c_recv,
    b_send,
    b_recv,
    a_send,
    a_recv,
    o_send,
    o_recv,
):
    me = lax.axis_index("tok")
    tp = lax.axis_index("tp")
    tok_count = line * QUAD
    quad = lax.rem(me, QUAD)
    place = me // QUAD
    rows = wq_ref.shape[0]
    tok_dev = hidden_ref.shape[0]
    depth = hidden_ref.shape[1]
    width = QUAD * rows
    keys = tok_dev * tok_count
    sib = me + 1 - 2 * lax.rem(me, 2)
    side = me + 2 - 4 * (quad // 2)
    side_sib = side + 1 - 2 * lax.rem(me, 2)
    own = (wq_ref, wk_ref, wv_ref)
    held = (held_q, held_k, held_v)
    widths = [ref.shape[1] for ref in own]
    sub = rows // tp_count
    count = len(chunks)
    kv_chunks = [c for c in range(count) if chunks[c][0] > 0]
    q_chunks = [c for c in range(count) if chunks[c][0] == 0]
    kv_here = widths[1] // HEAD
    last = count - 1
    lead = len(kv_chunks)
    half = line // 2
    base = jnp.where(2 * place < line, 0, half)
    at_end = (place == 0) | (place == line - 1)

    def remote(src, dst, send, recv, tok, tp_to=None):
        return pltpu.make_async_remote_copy(
            src_ref=src,
            dst_ref=dst,
            send_sem=send,
            recv_sem=recv,
            device_id=(tok, tp if tp_to is None else tp_to),
            device_id_type=MESH,
        )

    def rows_of(tok):
        return pl.ds(pl.multiple_of(tok * tok_dev, 16), tok_dev)

    def meet(barrier):
        def greet(step, carry):
            other = lax.rem(me + step, tok_count)
            pl.semaphore_signal(
                barrier, inc=1, device_id=(other, tp), device_id_type=MESH
            )
            return carry

        lax.fori_loop(1, tok_count, greet, 0)
        for step in range(1, tp_count):
            other = lax.rem(tp + step, tp_count)
            pl.semaphore_signal(
                barrier, inc=1, device_id=(me, other), device_id_type=MESH
            )

    def w_copy(kind, c):
        which, start, size = chunks[c]
        cols = pl.ds(start, size)
        if kind == 2:
            src = held[which].at[1, :, cols]
        else:
            src = own[which].at[:, cols]
        return remote(
            src,
            held[which].at[kind, :, cols],
            w_send.at[which],
            w_recv.at[kind, c],
            side if kind == 1 else sib,
        )

    ahead = 3

    def weights_start(c):
        w_copy(1, c).start()
        w_copy(0, c).start()

    part = tok_dev // share
    piece = lax.rem(tp, share)
    mate = tp + 1 - 2 * piece
    first = pl.multiple_of(piece * part, 16)

    def columns_of(tok):
        return pl.ds(pl.multiple_of(lax.rem(tok, QUAD) * rows, 128), rows)

    members = (me, side, sib, side_sib)
    cuts = 2 if rows % (2 * LANES) == 0 else 1
    slab = rows // cuts

    def channels(k):
        start = lax.rem(members[k // cuts], QUAD) * rows + (k % cuts) * slab
        return pl.multiple_of(start, 128)


    def t_copy(step, k):
        to = lax.rem(place + step, line)
        base = to * width + channels(k)
        return remote(
            normed.at[pl.ds(first, part), pl.ds(pl.multiple_of(base, 128), slab)],
            tokens.at[
                pl.ds(pl.multiple_of(place * tok_dev + first, 16), part),
                pl.ds(channels(k), slab),
            ],
            t_send.at[0],
            t_recv.at[step, k],
            to * QUAD + quad,
        )

    def m_copy(step, k):
        source = lax.rem(place - step + line, line)
        start = pl.multiple_of(source * tok_dev + piece * part, 16)
        got = tokens.at[pl.ds(start, part), pl.ds(channels(k), slab)]
        return remote(got, got, m_send.at[0], m_recv.at[k], me, mate)

    def tokens_sent(sem):
        every = tokens.at[pl.ds(0, (line - 1) * part)]
        remote(every, every, sem, sem, sib).wait_send()

    wide = [sum(widths[:i]) * tp_count for i in range(3)]

    def x_copy(which, step):
        to = lax.rem(tp + step, tp_count)
        size = widths[which]
        src = own[which].at[pl.ds(pl.multiple_of(to * sub, 16), sub)]
        dst = relaid.at[:, pl.ds(pl.multiple_of(wide[which] + tp * size, 128), size)]
        if step == 0:
            return pltpu.make_async_copy(src, dst, x_local.at[0])
        return remote(src, dst, x_send.at[0], x_recv.at[0], me, to)

    def x_all():
        size = sum(widths)
        every = relaid.at[:, pl.ds(0, size)]
        pltpu.make_async_copy(every, every, x_local.at[0]).wait()
        if tp_count > 1:
            every = relaid.at[:, pl.ds(0, (tp_count - 1) * size)]
            remote(every, every, x_send.at[0], x_recv.at[0], sib).wait()

    relaid_out = pltpu.make_async_copy(relaid, relaid_ref, x_local.at[1])

    def d_copy(step):
        to = lax.rem(me + step, tok_count)
        return remote(doc_row, docs.at[me], d_send.at[0], d_recv.at[0], to)

    def d_all():
        every = docs.at[pl.ds(0, tok_count - 1)]
        return remote(every, every, d_send.at[0], d_recv.at[0], sib)

    def p_copy(kind):
        return remote(
            mine,
            theirs.at[kind],
            p_send.at[0],
            p_recv.at[0],
            (sib, side, side_sib)[kind],
        )

    def each(copy):
        def go(step, carry):
            copy(step).start()
            return carry

        lax.fori_loop(1, tok_count, go, 0)

    tiles_at = math.gcd(slab // LANES, 4)

    def normalise(start, size, base, reach):
        def go(i, carry):
            for j in range(tiles_at):
                at = base + (tiles_at * i + j) * LANES
                cols = pl.ds(pl.multiple_of(at, LANES), LANES)
                block = hidden_ref[pl.ds(start, size), cols].astype(jnp.float32)
                block = block * root[pl.ds(start, size), :] * gain_ref[:, cols]
                normed[pl.ds(start, size), cols] = block.astype(jnp.bfloat16)
            return carry

        lax.fori_loop(0, reach // (tiles_at * LANES), go, 0)

    arrays = (
        (hidden_from, hidden_ref),
        (gain_from, gain_ref),
        (doc_from, doc_ref),
        (wk_from, wk_ref),
        (wv_from, wv_ref),
        (wq_from, wq_ref),
    )
    loads = [
        pltpu.make_async_copy(source, target, w_local.at[at])
        for at, (source, target) in enumerate(arrays)
    ]
    for load in loads:
        load.start()
    barrier = pltpu.get_barrier_semaphore()
    meet(barrier)
    for load in loads[:3]:
        load.wait()
    doc_row[...] = jnp.full(doc_row.shape, FAR, jnp.int32)
    doc_row[:, :tok_dev] = doc_ref[...]
    docs[me] = doc_row[...]

    def squares(i, total):
        for j in range(4):
            cols = pl.ds(pl.multiple_of((4 * i + j) * LANES, LANES), LANES)
            block = hidden_ref[:, cols].astype(jnp.float32)
            total = total + block * block
        return total

    total = lax.fori_loop(
        0, depth // (4 * LANES), squares, jnp.zeros((tok_dev, LANES), jnp.float32)
    )
    mean = jnp.sum(total, axis=1, keepdims=True) / depth
    root[...] = jnp.broadcast_to(lax.rsqrt(mean + 1e-05), (tok_dev, LANES))
    pl.semaphore_wait(barrier, tok_count - 1 + tp_count - 1)

    each(d_copy)
    for load in loads[3:]:
        load.wait()
    for c in range(min(ahead, count)):
        weights_start(c)

    for k in range(QUAD * cuts):

        def send_tokens(i, carry):
            step = jnp.where(2 * place < line, line - i, i)
            to = lax.rem(place + step, line)
            normalise(first, part, to * width + channels(k), slab)
            t_copy(step, k).start()
            return carry

        lax.fori_loop(1, line, send_tokens, 0)
    normalise(0, tok_dev, place * width, width)
    tokens[rows_of(place)] = normed[:, pl.ds(pl.multiple_of(place * width, 128), width)]

    lane = lax.broadcasted_iota(jnp.int32, (tok_dev, HEAD), 1)
    turns = lax.rem(lane, HEAD // 2).astype(jnp.float32)
    speed = jnp.exp(turns * (-2.0 * math.log(10000.0) / HEAD))

    def tables(j, carry):
        spot = ((base + j) * QUAD + quad) * tok_dev
        spot = spot + lax.broadcasted_iota(jnp.int32, (tok_dev, HEAD), 0)
        angles = spot.astype(jnp.float32) * speed
        cosine[j] = jnp.cos(angles)
        sine[j] = jnp.where(lane < HEAD // 2, -1.0, 1.0) * jnp.sin(angles)
        return carry

    lax.fori_loop(0, half, tables, 0)
    def take_tokens(i, k):
        source = jnp.where(i < half, i, line - 1 - (i - half))
        source = jnp.where(2 * place < line, source, line - 1 - source)

        @pl.when(source != place)
        def _():
            step = lax.rem(place - source + line, line)
            t_copy(step, k).wait_recv()
            if share == 2:
                m_copy(step, k).start()

    for k in range(QUAD * cuts):

        def take(i, carry):
            take_tokens(i, k)
            return carry

        lax.fori_loop(0, line - 1, take, 0)
    for k in range(QUAD * cuts):
        take_tokens(line - 1, k)

    base_of = [sum(size for _, _, size in chunks[:c]) for c in range(count)]

    def span(c):
        return slice(base_of[c], base_of[c] + chunks[c][2])

    def block(d):
        return pl.ds(pl.multiple_of(d * tok_dev, 8), tok_dev)

    def spot_of(c, d):
        return c * half + lax.rem(d, half) if c < last else last * half + d

    def sent_of(c, d):
        return c if c < last else last + d

    def right(c, d):
        here = partial.at[block(d), span(c)]
        there = from_left.at[block(d), span(c)]
        send, recv = r_send.at[sent_of(c, d)], r_recv.at[spot_of(c, d)]
        return remote(here, there, send, recv, me + QUAD)

    def left(c, d):
        here = partial.at[block(d), span(c)]
        there = from_right.at[block(d), span(c)]
        send, recv = l_send.at[sent_of(c, d)], l_recv.at[spot_of(c, d)]
        return remote(here, there, send, recv, me - QUAD)

    def added(c, d, way):
        (right, left)[way](c, d).wait_recv()
        landed = (from_left, from_right)[way]
        return partial[block(d), span(c)] + landed[block(d), span(c)]

    def pass_on(c, d, way):
        partial[block(d), span(c)] = added(c, d, way)
        (right, left)[way](c, d).start()

    def sends(c, way):
        if c < last:
            return half, (lambda i: half + i) if way == 0 else (lambda i: half - 1 - i)
        if way == 0:
            return line - 1, lambda i: line - 1 - i
        return line - 1, lambda i: i

    def goes(c, d, way):
        if c < last:
            return place < line - 1 if way == 0 else place > 0
        return d > place if way == 0 else d < place

    def first_sends(c):
        for way in range(2):

            @pl.when(place == (0 if way == 0 else line - 1))
            def _():
                size, pick = sends(c, way)

                def go(i, carry):
                    (right, left)[way](c, pick(i)).start()
                    return carry

                lax.fori_loop(0, size, go, 0)

    def onward(c, i, way):
        size, pick = sends(c, way)
        inside = place > 0 if way == 0 else place < line - 1
        d = pick(i)

        @pl.when((i < size) & inside & goes(c, d, way))
        def _():
            pass_on(c, d, way)

    def weave(far, near):
        def go(nearest, i):
            if far is not None:
                onward(far, i, 1 - nearest)
            if near is not None:
                onward(near, i, nearest)

        def left_half(i, carry):
            go(0, i)
            return carry

        def right_half(i, carry):
            go(1, i)
            return carry

        top = line - 1 if last in (far, near) else half

        @pl.when(2 * place < line)
        def _():
            lax.fori_loop(0, top, left_half, 0)

        @pl.when(2 * place >= line)
        def _():
            lax.fori_loop(0, top, right_half, 0)

    def settle(c, j):
        which, start, size = chunks[c]
        d = base + j
        for head in range(size // HEAD):
            at = base_of[c] + head * HEAD
            states = partial[block(d), at : at + HEAD]
            if which < 2:
                states = (
                    states * cosine[j] + pltpu.roll(states, HEAD // 2, 1) * sine[j]
                )
            at = start + head * HEAD + (widths[1] if which == 2 else 0)
            if which == 0:
                query[j, :, at : at + HEAD] = states.astype(jnp.bfloat16)
            else:
                rows_at = rows_of(d * QUAD + quad)
                cache[rows_at, at : at + HEAD] = states.astype(jnp.bfloat16)

    def q_copy(c, j):
        which, start, size = chunks[c]
        got = query.at[j, :, pl.ds(start, size)]
        to = (base + j) * QUAD + quad
        return remote(got, got, q_send.at[0], q_recv.at[c - lead], to)

    def finish(c):
        if c == last:
            for way in range(2):

                @pl.when(place > 0 if way == 0 else place < line - 1)
                def _():
                    partial[block(place), span(c)] = added(c, place, way)

            settle(c, place - base)
            return

        @pl.when(at_end)
        def _():
            def go(i, carry):
                j = jnp.where(place == 0, half - 1 - i, i)
                d = base + j
                for way in range(2):

                    @pl.when(place == (line - 1 if way == 0 else 0))
                    def _():
                        partial[block(d), span(c)] = added(c, d, way)

                settle(c, j)
                if chunks[c][0] == 0:

                    @pl.when(d != place)
                    def _():
                        q_copy(c, j).start()

                return carry

            lax.fori_loop(0, half, go, 0)

    def tokens_ready(c, k):
        if c == 0 and share == 2:
            for at in range(k * cuts, (k + 1) * cuts):
                every = tokens.at[pl.ds(0, (line - 1) * part), pl.ds(0, slab)]
                remote(every, every, m_recv.at[at], m_recv.at[at], sib).wait_recv()

    def project(c):
        which, start, size = chunks[c]
        cols = slice(start, start + size)
        tokens_ready(c, 0)
        total = jnp.dot(
            tokens[:, columns_of(me)],
            own[which][:, cols],
            preferred_element_type=jnp.float32,
        )
        w_copy(1, c).wait_recv()
        w_copy(2, c).start()
        if c + ahead < count:
            weights_start(c + ahead)
        for k, kind in ((1, 1), (2, 0), (3, 2)):
            tokens_ready(c, k)
            if kind != 1:
                w_copy(kind, c).wait_recv()
            total += jnp.dot(
                tokens[:, columns_of(members[k])],
                held[which][kind, :, cols],
                preferred_element_type=jnp.float32,
            )
        partial[:, span(c)] = total
        first_sends(c)

    def kv_rows(spot, of_side=False):
        at = lax.rem(side, QUAD) if of_side else quad
        return cache.at[rows_of(spot * QUAD + at)]

    def z_copy(way, j):
        got = kv_rows(j + way * half)
        to = me - QUAD if way else me + QUAD
        return remote(got, got, z_send.at[way], z_recv.at[way, j], to)

    def y_copy(spot):
        got = kv_rows(spot)
        return remote(got, got, y_send.at[0], y_recv.at[spot], side)

    def y_arrival(spot):
        got = kv_rows(spot, True)
        return remote(got, got, y_send.at[0], y_recv.at[spot], side)

    def s_copy(spot, of_side):
        got = kv_rows(spot, of_side)
        return remote(got, got, s_send.at[0], s_recv.at[0], sib)

    def s_all():
        every = cache.at[pl.ds(0, 2 * line * tok_dev)]
        return remote(every, every, s_send.at[0], s_recv.at[0], sib)

    def kv_block(way, j, fresh):
        if not fresh:
            z_copy(way, j).wait_recv()

        @pl.when(place > 0 if way else place < line - 1)
        def _():
            z_copy(way, j).start()

        y_copy(j + way * half).start()
        s_copy(j + way * half, False).start()

    def kv_pass(way, fresh, near=None):
        def go(j, carry):
            kv_block(way, j, fresh)
            if near is not None:
                onward(near, j, 1 - way)
            return carry

        lax.fori_loop(0, half, go, 0)

    def kv_start():
        for way in range(2):

            @pl.when(place == way * (line - 1))
            def _():
                kv_pass(way, True)

    def kv_near():
        for way in range(2):
            nearer = 2 * place >= line if way else 2 * place < line

            @pl.when(nearer & jnp.logical_not(at_end))
            def _():
                kv_pass(way, False)

    def kv_far(near):
        for way in range(2):

            @pl.when(2 * place < line if way else 2 * place >= line)
            def _():
                kv_pass(way, False, near)

    def kv_side():
        def go(spot, carry):
            y_arrival(spot).wait_recv()
            s_copy(spot, True).start()
            return carry

        lax.fori_loop(0, line, go, 0)

    def kv_ready():
        s_all().wait_recv()

    def mask():
        d_all().wait()
        wanted = jnp.transpose(
            jnp.broadcast_to(doc_row[...].astype(jnp.float32), (LANES, LANES))
        )[:tok_dev]

        def go(tok, total):
            before = docs[tok].astype(jnp.float32) < wanted
            return total + jnp.where(before, 1.0, 0.0)

        total = lax.fori_loop(
            0, tok_count, go, jnp.zeros((tok_dev, LANES), jnp.float32)
        )
        since = jnp.sum(total, axis=1, keepdims=True).astype(jnp.int32)
        spot = lax.broadcasted_iota(jnp.int32, (tok_dev, keys), 0) + me * tok_dev
        at = lax.broadcasted_iota(jnp.int32, (tok_dev, keys), 1)
        bias[...] = jnp.where((at >= since) & (at <= spot), 0.0, -1e30)

    turn = math.log2(math.e) / math.sqrt(HEAD)

    def attend(g):
        heads = [
            slice((g * GROUP + h) * HEAD, (g * GROUP + h + 1) * HEAD)
            for h in range(GROUP)
        ]
        if g + lead < last:

            @pl.when(jnp.logical_not(at_end))
            def _():
                q_copy(g + lead, place - base).wait_recv()

        asked = jnp.concatenate(
            [query[place - base, :, head] for head in heads], axis=0
        )
        key = cache[:, g * HEAD : (g + 1) * HEAD]
        value = cache[:, (kv_here + g) * HEAD : (kv_here + g + 1) * HEAD]
        scores = lax.dot_general(
            asked, key, (((1,), (1,)), ((), ())), preferred_element_type=jnp.float32
        )
        scores = (
            scores.reshape(GROUP, tok_dev, keys) + bias[...][None]
        ).reshape(GROUP * tok_dev, keys)
        weights = jnp.exp2((scores - jnp.max(scores, axis=1, keepdims=True)) * turn)
        totals = jnp.sum(weights, axis=1, keepdims=True)
        mixed = jnp.dot(
            weights.astype(jnp.bfloat16), value, preferred_element_type=jnp.float32
        )
        mixed = (mixed / totals).astype(jnp.bfloat16)
        for h, head in enumerate(heads):
            piece = mixed[h * tok_dev : (h + 1) * tok_dev]
            out_ref[:, head] = piece
            out_mine[:, head] = jnp.max(
                jnp.abs(piece.astype(jnp.float32)), axis=0, keepdims=True
            )
        cols = pl.ds(g * GROUP * HEAD, GROUP * HEAD)
        out_all[me, :, cols] = out_mine[:, cols]
        each(functools.partial(o_copy, g))

    def o_copy(g, step):
        cols = pl.ds(g * GROUP * HEAD, GROUP * HEAD)
        to = lax.rem(me + step, tok_count)
        return remote(
            out_mine.at[:, cols], out_all.at[me, :, cols], o_send.at[0], o_recv.at[0], to
        )

    def o_all():
        every = out_all.at[pl.ds(0, tok_count - 1)]
        return remote(every, every, o_send.at[0], o_recv.at[0], sib)

    def smooth():
        remote(theirs, theirs, p_send.at[0], p_recv.at[0], sib).wait()
        peak = jnp.maximum(
            jnp.maximum(mine[...], theirs[0]), jnp.maximum(theirs[1], theirs[2])
        )
        mine[...] = peak
        for i in range(rows // LANES):
            here = slice(i * LANES, (i + 1) * LANES)
            at = pl.ds(pl.multiple_of(quad * rows + i * LANES, LANES), LANES)
            channel[0, here] = as_column(mine[:, at])
            at = pl.ds(pl.multiple_of(me * rows + i * LANES, LANES), LANES)
            channel[1, here] = as_column(gain_ref[:, at])
        x_all()
        relaid_out.start()
        tiles = relaid.shape[1] // LANES

        def tallest(i, most):
            cols = pl.ds(pl.multiple_of(i * LANES, LANES), LANES)
            return jnp.maximum(most, jnp.abs(relaid[:, cols].astype(jnp.float32)))

        most = lax.fori_loop(0, tiles, tallest, jnp.zeros((sub, LANES), jnp.float32))
        weight_peak = jnp.max(most, axis=1, keepdims=True)
        ours = pl.ds(pl.multiple_of(tp * sub, 16), sub)
        factor = jnp.sqrt(jnp.maximum(channel[0, ours, :], 1e-05)) / jnp.sqrt(
            jnp.maximum(weight_peak, 1e-05)
        )
        smooth_ref[...] = factor
        channel[0, ours, :] = channel[1, ours, :] / factor

        def highest(i, carry):
            cols = pl.ds(pl.multiple_of(i * LANES, LANES), LANES)
            column[0, :, cols] = jnp.max(
                jnp.abs(smooth_ref[...] * relaid[:, cols].astype(jnp.float32)),
                axis=0,
                keepdims=True,
            )
            return carry

        lax.fori_loop(0, tiles, highest, 0)
        for i in range(-(-sub // LANES)):
            size = min(LANES, sub - i * LANES)
            start = pl.multiple_of(tp * sub + i * LANES, 16)
            tile = channel[0, pl.ds(start, size), :]
            if size < LANES:
                tile = jnp.concatenate(
                    [tile, jnp.zeros((LANES - size, LANES), jnp.float32)], axis=0
                )
            folded_ref[:, i * LANES : i * LANES + size] = jnp.transpose(tile)[
                0:1, :size
            ]
        for step in range(1, tp_count):
            c_copy(step).start()

    def c_copy(step):
        return remote(
            column.at[0],
            column_tp.at[step],
            c_send.at[0],
            c_recv.at[0],
            me,
            lax.rem(tp + step, tp_count),
        )

    def b_copy(stage):
        return remote(
            column.at[1 + stage],
            column_tp.at[tp_count + stage],
            b_send.at[stage],
            b_recv.at[stage],
            (sib, side)[stage],
        )

    def a_copy(step):
        return remote(
            column.at[3],
            column_line.at[step],
            a_send.at[0],
            a_recv.at[0],
            lax.rem(place + step, line) * QUAD + quad,
        )

    def columns_tp():
        joined = column[0]
        if tp_count > 1:
            every = column_tp.at[pl.ds(0, tp_count - 1)]
            remote(every, every, c_send.at[0], c_recv.at[0], sib).wait()
        for step in range(1, tp_count):
            joined = jnp.maximum(joined, column_tp[step])
        column[1] = joined
        b_copy(0).start()

    def columns_sib():
        b_copy(0).wait()
        column[2] = jnp.maximum(column[1], column_tp[tp_count])
        b_copy(1).start()

    def columns_side():
        b_copy(1).wait()
        column[3] = jnp.maximum(column[2], column_tp[tp_count + 1])
        for step in range(1, line):
            a_copy(step).start()

    def columns_line():
        joined = column[3]
        every = column_line.at[pl.ds(0, line - 1)]
        remote(every, every, a_send.at[0], a_recv.at[0], sib).wait()
        for step in range(1, line):
            joined = jnp.maximum(joined, column_line[step])
        scale_ref[...] = jnp.maximum(joined, 1e-05) / 127.0

    def early():
        mine[...] = jnp.max(
            jnp.abs(tokens[...].astype(jnp.float32)), axis=0, keepdims=True
        )
        for kind in range(3):
            p_copy(kind).start()

    ran = set()

    def once(act, c, *rest):
        if c <= last and (act, c) not in ran:
            ran.add((act, c))
            act(c, *rest)

    def pair(far, near):
        far = None if far > last or ("far", far) in ran else far
        near = None if near > last or ("near", near) in ran else near
        ran.update({("far", far), ("near", near)})
        if far is not None or near is not None:
            weave(far, near)

    def split_project(c, ends):
        @pl.when(at_end if ends else jnp.logical_not(at_end))
        def _():
            project(c)

    once(project, 0)
    early()
    for which in (1, 2, 0):
        for step in range(tp_count):
            x_copy(which, step).start()
    for c in range(1, lead):
        once(project, c)
    for c in range(lead):
        pair(c - 1 if c else FAR, c)
    once(project, lead)
    once(finish, kv_chunks[0])
    pair(lead - 1, lead)
    once(project, lead + 1)
    for c in kv_chunks:
        once(finish, c)
    kv_start()
    mask()
    pair(lead, lead + 1)
    smooth()
    once(project, lead + 2)
    if lead < last - 1:
        once(finish, lead)
    if lead + 3 <= last:
        split_project(lead + 3, True)
    pair(lead + 1, FAR)
    if lead + 1 < last - 1:
        once(finish, lead + 1)
    kv_near()
    if lead + 3 <= last:
        split_project(lead + 3, False)
        ran.add((project, lead + 3))
    if lead + 2 < last:
        ran.add(("near", lead + 2))
        kv_far(lead + 2)
    else:
        kv_far(None)
    columns_tp()
    for c in range(lead, count):
        once(project, c)
        pair(c - 1, c)
    kv_side()
    columns_sib()
    kv_ready()
    if lead == last:
        pair(last, FAR)
    swap = last - 1 > lead

    def attend_where(g, ends):
        @pl.when(at_end if ends else jnp.logical_not(at_end))
        def _():
            attend(g)

    for c in range(lead, count):
        if lead < c == last - 2:
            once(finish, last - 1)
        once(finish, c)
        if swap and c == last - 1:
            attend_where(c - lead, True)
        else:
            attend(c - lead)
        if c == lead:
            pair(last, FAR)
            columns_side()
    if swap:
        attend_where(last - 1 - lead, False)
    columns_line()
    o_all().wait()
    out_peak_ref[...] = jnp.max(out_all[...], axis=0)

    tokens_sent(t_send.at[0])
    if share == 2:
        tokens_sent(m_send.at[0])
    for which in range(3):
        every = held[which]
        remote(every, every, w_send.at[which], w_send.at[which], sib).wait_send()
    for way in range(2):
        moves = place > 0 if way else place < line - 1

        @pl.when(moves)
        def _():
            sems = (r_send, l_send)[way]
            for c in range(last):
                every = partial.at[pl.ds(0, half * tok_dev), span(c)]
                remote(every, every, sems.at[c], sems.at[c], sib).wait_send()
            every = cache.at[pl.ds(0, half * tok_dev)]
            remote(every, every, z_send.at[way], z_send.at[way], sib).wait_send()

        def sent(d, carry):
            @pl.when(d < place if way else d > place)
            def _():
                (right, left)[way](last, d).wait_send()

            return carry

        lax.fori_loop(0, line, sent, 0)
    if last > lead and half > 1:

        @pl.when(at_end)
        def _():
            every = query.at[
                pl.ds(0, half - 1), :, pl.ds(0, (last - lead) * GROUP * HEAD)
            ]
            remote(every, every, q_send.at[0], q_send.at[0], sib).wait_send()

    s_all().wait_send()
    every = cache.at[pl.ds(0, line * tok_dev)]
    remote(every, every, y_send.at[0], y_send.at[0], sib).wait_send()
    relaid_out.wait()


def calibrate(hidden, gain, doc_row, matrices):
    tok_count, tp_count = lax.axis_size("tok"), lax.axis_size("tp")
    line = tok_count // QUAD
    tok_dev, depth = hidden.shape
    rows = matrices[0].shape[0]
    sub = rows // tp_count
    widths = [matrix.shape[1] for matrix in matrices]
    chunks = column_chunks(widths)
    count = len(chunks)
    total = sum(widths)
    share = 2 if tp_count % 2 == 0 and tok_dev % 32 == 0 else 1
    vmem = pl.BlockSpec(memory_space=pltpu.VMEM)
    dma = pltpu.SemaphoreType.DMA
    f32, bf16 = jnp.float32, jnp.bfloat16
    queries = widths[0] // (GROUP * HEAD)
    lanes = tok_dev + -tok_dev % LANES
    return pl.pallas_call(
        functools.partial(main_kernel, chunks, line, tp_count, share),
        out_shape=(
            jax.ShapeDtypeStruct((tok_dev, widths[0]), bf16),
            jax.ShapeDtypeStruct((1, widths[0]), f32),
            jax.ShapeDtypeStruct((1, total * tp_count), f32),
            jax.ShapeDtypeStruct((1, sub), f32),
            jax.ShapeDtypeStruct((sub, LANES), f32),
            jax.ShapeDtypeStruct((sub, total * tp_count), bf16),
        ),
        in_specs=[pl.BlockSpec(memory_space=pl.ANY)] * 6,
        out_specs=(vmem,) * 5 + (pl.BlockSpec(memory_space=pl.ANY),),
        scratch_shapes=[
            pltpu.VMEM((tok_dev, depth), bf16),
            pltpu.VMEM((tok_dev, LANES), f32),
            pltpu.VMEM((line // 2, tok_dev, HEAD), f32),
            pltpu.VMEM((line // 2, tok_dev, HEAD), f32),
            pltpu.VMEM((1, lanes), jnp.int32),
            pltpu.VMEM((tok_count, 1, lanes), jnp.int32),
            pltpu.VMEM((tok_dev, tok_dev * tok_count), f32),
            pltpu.VMEM((line * tok_dev, QUAD * rows), bf16),
            pltpu.VMEM((1, QUAD * rows), f32),
            pltpu.VMEM((3, 1, QUAD * rows), f32),
        ]
        + [pltpu.VMEM(array.shape, array.dtype) for array in (hidden, gain, doc_row)]
        + [pltpu.VMEM((rows, width), bf16) for width in widths]
        + [pltpu.VMEM((3, rows, width), bf16) for width in widths]
        + [pltpu.VMEM((line * tok_dev, total), f32)] * 3
        + [
            pltpu.VMEM((line // 2, tok_dev, widths[0]), bf16),
            pltpu.VMEM((tok_dev * tok_count, widths[1] + widths[2]), bf16),
            pltpu.VMEM((sub, total * tp_count), bf16),
            pltpu.VMEM((2, rows, LANES), f32),
            pltpu.VMEM((4, 1, total * tp_count), f32),
            pltpu.VMEM((tp_count + 2, 1, total * tp_count), f32),
            pltpu.VMEM((line, 1, total * tp_count), f32),
            pltpu.VMEM((1, widths[0]), f32),
            pltpu.VMEM((tok_count, 1, widths[0]), f32),
        ]
        + [dma((6,)), dma((3,)), dma((3, count))]
        + [dma((1,)), dma((line, 2 * QUAD)), dma((1,)), dma((2 * QUAD,))]
        + [dma((1,))] * 2
        + [dma((2,))]
        + [dma((count - 1 + line,)), dma(((count - 1) * (line // 2) + line,))] * 2
        + [dma((1,))] * 4
        + [dma((2,)), dma((2, line // 2))]
        + [dma((1,)), dma((line,))]
        + [dma((1,))] * 2
        + [dma((1,)), dma((queries,))]
        + [dma((1,))] * 2
        + [dma((2,))] * 2
        + [dma((1,))] * 4,
        compiler_params=pltpu.CompilerParams(
            collective_id=0, has_side_effects=True, vmem_limit_bytes=63 * 1024 * 1024
        ),
    )(hidden, gain, doc_row, *matrices)


def codes_kernel(
    widths,
    tp_count,
    relaid_ref,
    smooth_ref,
    scale_ref,
    attended_ref,
    peak_ref,
    folded_ref,
    cq_ref,
    ck_ref,
    cv_ref,
    sq_ref,
    sk_ref,
    sv_ref,
    out_ref,
    out_peak_ref,
    out_folded_ref,
    inverse,
):
    tp = lax.axis_index("tp")

    @pl.when(pl.program_id(0) == 0)
    def _():
        out_ref[...] = attended_ref[...]
        out_peak_ref[...] = peak_ref[...]
        out_folded_ref[...] = folded_ref[...]
        inverse[...] = 1.0 / scale_ref[...]
        for which, ref in enumerate((sq_ref, sk_ref, sv_ref)):
            base = sum(widths[:which]) * tp_count + tp * widths[which]
            ref[...] = scale_ref[:, pl.ds(pl.multiple_of(base, 128), widths[which])]

    factor = smooth_ref[...]
    for which, ref in enumerate((cq_ref, ck_ref, cv_ref)):
        base = sum(widths[:which]) * tp_count
        for at in range(0, widths[which] * tp_count, LANES):
            cols = slice(base + at, base + at + LANES)
            ref[:, at : at + LANES] = (
                factor * relaid_ref[:, cols].astype(jnp.float32) * inverse[:, cols]
            )


def coded(relaid, smooth, scale, attended, peak, folded, widths, tp_count):
    sub, total = relaid.shape
    block = math.gcd(sub, 128)
    f32 = jnp.float32

    def striped(width):
        return pl.BlockSpec((block, width), lambda i: (i, 0))

    def whole(array):
        return pl.BlockSpec(array.shape, lambda i: (0, 0))

    full = [jax.ShapeDtypeStruct((sub, width * tp_count), f32) for width in widths]
    part = [jax.ShapeDtypeStruct((1, width), f32) for width in widths]
    rest = [
        jax.ShapeDtypeStruct(array.shape, array.dtype)
        for array in (attended, peak, folded)
    ]
    return pl.pallas_call(
        functools.partial(codes_kernel, widths, tp_count),
        grid=(sub // block,),
        out_shape=full + part + rest,
        in_specs=[striped(total), striped(LANES)]
        + [whole(array) for array in (scale, attended, peak, folded)],
        out_specs=[striped(width * tp_count) for width in widths]
        + [whole(array) for array in part + rest],
        scratch_shapes=[pltpu.VMEM((1, total), f32)],
    )(relaid, smooth, scale, attended, peak, folded)


def on_device(hidden, norm_gain, w_query, w_key, w_value, doc_ids):
    matrices = (w_query, w_key, w_value)
    attended, peak, scale, folded, smooth, relaid = calibrate(
        hidden, norm_gain[None], doc_ids[None], matrices
    )
    *rows, attended, peak, folded = coded(
        relaid,
        smooth,
        scale,
        attended,
        peak,
        folded,
        [matrix.shape[1] for matrix in matrices],
        lax.axis_size("tp"),
    )
    scales = [row[0] for row in rows[3:]]
    return (attended, peak[0], folded[0], *rows[:3], *scales)


def solution(mesh):
    in_specs = (P("tok", None), P(), P("tok", "tp"), P("tok", "tp"), P("tok", "tp"), P("tok"))
    out_specs = (
        P("tok", "tp"),
        P("tp"),
        P(("tok", "tp")),
        P(("tok", "tp"), None),
        P(("tok", "tp"), None),
        P(("tok", "tp"), None),
        P("tp"),
        P("tp"),
        P("tp"),
    )
    return jax.shard_map(
        on_device, mesh=mesh, in_specs=in_specs, out_specs=out_specs, check_vma=False
    )
```

```python
import functools
import math

import jax
import jax.numpy as jnp
from jax import lax
from jax.experimental import pallas as pl
from jax.experimental.pallas import tpu as pltpu
from jax.sharding import PartitionSpec as P

HEAD = 128
KVH = 8
QHEADS = 32
GROUP = QHEADS // KVH
LANES = 128
FAR = 1 << 30

MESH = pl.DeviceIdType.MESH
QUAD = 4


def column_chunks(widths, most=GROUP * HEAD):
    return [
        (which, start, min(most, widths[which] - start))
        for which in (1, 2, 0)
        for start in range(0, widths[which], most)
    ]


def as_column(row):
    return jnp.transpose(jnp.broadcast_to(row, (LANES, LANES)))

def main_kernel(
    chunks,
    line,
    tp_count,
    share,
    hidden_from,
    gain_from,
    doc_from,
    wq_from,
    wk_from,
    wv_from,
    out_ref,
    out_peak_ref,
    scale_ref,
    folded_ref,
    smooth_ref,
    relaid_ref,
    normed,
    root,
    cosine,
    sine,
    doc_row,
    docs,
    bias,
    tokens,
    mine,
    theirs,
    hidden_ref,
    gain_ref,
    doc_ref,
    wq_ref,
    wk_ref,
    wv_ref,
    held_q,
    held_k,
    held_v,
    partial,
    from_left,
    from_right,
    query,
    cache,
    relaid,
    channel,
    column,
    column_tp,
    column_line,
    out_mine,
    out_all,
    w_local,
    w_send,
    w_recv,
    t_send,
    t_recv,
    m_send,
    m_recv,
    x_send,
    x_recv,
    x_local,
    r_send,
    r_recv,
    l_send,
    l_recv,
    p_send,
    p_recv,
    d_send,
    d_recv,
    z_send,
    z_recv,
    y_send,
    y_recv,
    s_send,
    s_recv,
    q_send,
    q_recv,
    c_send,
    c_recv,
    b_send,
    b_recv,
    a_send,
    a_recv,
    o_send,
    o_recv,
):
    me = lax.axis_index("tok")
    tp = lax.axis_index("tp")
    tok_count = line * QUAD
    quad = lax.rem(me, QUAD)
    place = me // QUAD
    rows = wq_ref.shape[0]
    tok_dev = hidden_ref.shape[0]
    depth = hidden_ref.shape[1]
    width = QUAD * rows
    keys = tok_dev * tok_count
    sib = me + 1 - 2 * lax.rem(me, 2)
    side = me + 2 - 4 * (quad // 2)
    side_sib = side + 1 - 2 * lax.rem(me, 2)
    own = (wq_ref, wk_ref, wv_ref)
    held = (held_q, held_k, held_v)
    widths = [ref.shape[1] for ref in own]
    sub = rows // tp_count
    count = len(chunks)
    kv_chunks = [c for c in range(count) if chunks[c][0] > 0]
    q_chunks = [c for c in range(count) if chunks[c][0] == 0]
    kv_here = widths[1] // HEAD
    last = count - 1
    lead = len(kv_chunks)
    half = line // 2
    base = jnp.where(2 * place < line, 0, half)
    at_end = (place == 0) | (place == line - 1)

    def remote(src, dst, send, recv, tok, tp_to=None):
        return pltpu.make_async_remote_copy(
            src_ref=src,
            dst_ref=dst,
            send_sem=send,
            recv_sem=recv,
            device_id=(tok, tp if tp_to is None else tp_to),
            device_id_type=MESH,
        )

    def rows_of(tok):
        return pl.ds(pl.multiple_of(tok * tok_dev, 16), tok_dev)

    def meet(barrier):
        def greet(step, carry):
            other = lax.rem(me + step, tok_count)
            pl.semaphore_signal(
                barrier, inc=1, device_id=(other, tp), device_id_type=MESH
            )
            return carry

        lax.fori_loop(1, tok_count, greet, 0)
        for step in range(1, tp_count):
            other = lax.rem(tp + step, tp_count)
            pl.semaphore_signal(
                barrier, inc=1, device_id=(me, other), device_id_type=MESH
            )

    def w_copy(kind, c):
        which, start, size = chunks[c]
        cols = pl.ds(start, size)
        if kind == 2:
            src = held[which].at[1, :, cols]
        else:
            src = own[which].at[:, cols]
        return remote(
            src,
            held[which].at[kind, :, cols],
            w_send.at[which],
            w_recv.at[kind, c],
            side if kind == 1 else sib,
        )

    ahead = 3

    def weights_start(c):
        w_copy(1, c).start()
        w_copy(0, c).start()

    part = tok_dev // share
    piece = lax.rem(tp, share)
    mate = tp + 1 - 2 * piece
    first = pl.multiple_of(piece * part, 16)

    def columns_of(tok):
        return pl.ds(pl.multiple_of(lax.rem(tok, QUAD) * rows, 128), rows)

    members = (me, side, sib, side_sib)
    cuts = 2 if rows % (2 * LANES) == 0 else 1
    slab = rows // cuts

    def channels(k):
        start = lax.rem(members[k // cuts], QUAD) * rows + (k % cuts) * slab
        return pl.multiple_of(start, 128)


    def t_copy(step, k):
        to = lax.rem(place + step, line)
        base = to * width + channels(k)
        return remote(
            normed.at[pl.ds(first, part), pl.ds(pl.multiple_of(base, 128), slab)],
            tokens.at[
                pl.ds(pl.multiple_of(place * tok_dev + first, 16), part),
                pl.ds(channels(k), slab),
            ],
            t_send.at[0],
            t_recv.at[step, k],
            to * QUAD + quad,
        )

    def m_copy(step, k):
        source = lax.rem(place - step + line, line)
        start = pl.multiple_of(source * tok_dev + piece * part, 16)
        got = tokens.at[pl.ds(start, part), pl.ds(channels(k), slab)]
        return remote(got, got, m_send.at[0], m_recv.at[k], me, mate)

    def tokens_sent(sem):
        every = tokens.at[pl.ds(0, (line - 1) * part)]
        remote(every, every, sem, sem, sib).wait_send()

    wide = [sum(widths[:i]) * tp_count for i in range(3)]

    def x_copy(which, step):
        to = lax.rem(tp + step, tp_count)
        size = widths[which]
        src = own[which].at[pl.ds(pl.multiple_of(to * sub, 16), sub)]
        dst = relaid.at[:, pl.ds(pl.multiple_of(wide[which] + tp * size, 128), size)]
        if step == 0:
            return pltpu.make_async_copy(src, dst, x_local.at[0])
        return remote(src, dst, x_send.at[0], x_recv.at[0], me, to)

    def x_all():
        size = sum(widths)
        every = relaid.at[:, pl.ds(0, size)]
        pltpu.make_async_copy(every, every, x_local.at[0]).wait()
        if tp_count > 1:
            every = relaid.at[:, pl.ds(0, (tp_count - 1) * size)]
            remote(every, every, x_send.at[0], x_recv.at[0], sib).wait()

    relaid_out = pltpu.make_async_copy(relaid, relaid_ref, x_local.at[1])

    def d_copy(step):
        to = lax.rem(me + step, tok_count)
        return remote(doc_row, docs.at[me], d_send.at[0], d_recv.at[0], to)

    def d_all():
        every = docs.at[pl.ds(0, tok_count - 1)]
        return remote(every, every, d_send.at[0], d_recv.at[0], sib)

    def p_copy(kind):
        return remote(
            mine,
            theirs.at[kind],
            p_send.at[0],
            p_recv.at[0],
            (sib, side, side_sib)[kind],
        )

    def each(copy):
        def go(step, carry):
            copy(step).start()
            return carry

        lax.fori_loop(1, tok_count, go, 0)

    tiles_at = math.gcd(slab // LANES, 4)

    def normalise(start, size, base, reach):
        def go(i, carry):
            for j in range(tiles_at):
                at = base + (tiles_at * i + j) * LANES
                cols = pl.ds(pl.multiple_of(at, LANES), LANES)
                block = hidden_ref[pl.ds(start, size), cols].astype(jnp.float32)
                block = block * root[pl.ds(start, size), :] * gain_ref[:, cols]
                normed[pl.ds(start, size), cols] = block.astype(jnp.bfloat16)
            return carry

        lax.fori_loop(0, reach // (tiles_at * LANES), go, 0)

    arrays = (
        (hidden_from, hidden_ref),
        (gain_from, gain_ref),
        (doc_from, doc_ref),
        (wk_from, wk_ref),
        (wv_from, wv_ref),
        (wq_from, wq_ref),
    )
    loads = [
        pltpu.make_async_copy(source, target, w_local.at[at])
        for at, (source, target) in enumerate(arrays)
    ]
    for load in loads:
        load.start()
    barrier = pltpu.get_barrier_semaphore()
    meet(barrier)
    for load in loads[:3]:
        load.wait()
    doc_row[...] = jnp.full(doc_row.shape, FAR, jnp.int32)
    doc_row[:, :tok_dev] = doc_ref[...]
    docs[me] = doc_row[...]

    def squares(i, total):
        for j in range(4):
            cols = pl.ds(pl.multiple_of((4 * i + j) * LANES, LANES), LANES)
            block = hidden_ref[:, cols].astype(jnp.float32)
            total = total + block * block
        return total

    total = lax.fori_loop(
        0, depth // (4 * LANES), squares, jnp.zeros((tok_dev, LANES), jnp.float32)
    )
    mean = jnp.sum(total, axis=1, keepdims=True) / depth
    root[...] = jnp.broadcast_to(lax.rsqrt(mean + 1e-05), (tok_dev, LANES))
    pl.semaphore_wait(barrier, tok_count - 1 + tp_count - 1)

    each(d_copy)
    for load in loads[3:]:
        load.wait()
    for c in range(min(ahead, count)):
        weights_start(c)

    for k in range(QUAD * cuts):

        def send_tokens(i, carry):
            step = jnp.where(2 * place < line, line - i, i)
            to = lax.rem(place + step, line)
            normalise(first, part, to * width + channels(k), slab)
            t_copy(step, k).start()
            return carry

        lax.fori_loop(1, line, send_tokens, 0)
    normalise(0, tok_dev, place * width, width)
    tokens[rows_of(place)] = normed[:, pl.ds(pl.multiple_of(place * width, 128), width)]

    lane = lax.broadcasted_iota(jnp.int32, (tok_dev, HEAD), 1)
    turns = lax.rem(lane, HEAD // 2).astype(jnp.float32)
    speed = jnp.exp(turns * (-2.0 * math.log(10000.0) / HEAD))

    def tables(j, carry):
        spot = ((base + j) * QUAD + quad) * tok_dev
        spot = spot + lax.broadcasted_iota(jnp.int32, (tok_dev, HEAD), 0)
        angles = spot.astype(jnp.float32) * speed
        cosine[j] = jnp.cos(angles)
        sine[j] = jnp.where(lane < HEAD // 2, -1.0, 1.0) * jnp.sin(angles)
        return carry

    lax.fori_loop(0, half, tables, 0)
    def take_tokens(i, k):
        source = jnp.where(i < half, i, line - 1 - (i - half))
        source = jnp.where(2 * place < line, source, line - 1 - source)

        @pl.when(source != place)
        def _():
            step = lax.rem(place - source + line, line)
            t_copy(step, k).wait_recv()
            if share == 2:
                m_copy(step, k).start()

    for k in range(QUAD * cuts):

        def take(i, carry):
            take_tokens(i, k)
            return carry

        lax.fori_loop(0, line - 1, take, 0)
    for k in range(QUAD * cuts):
        take_tokens(line - 1, k)

    base_of = [sum(size for _, _, size in chunks[:c]) for c in range(count)]

    def span(c):
        return slice(base_of[c], base_of[c] + chunks[c][2])

    def block(d):
        return pl.ds(pl.multiple_of(d * tok_dev, 8), tok_dev)

    def spot_of(c, d):
        return c * half + lax.rem(d, half) if c < last else last * half + d

    def sent_of(c, d):
        return c if c < last else last + d

    def right(c, d):
        here = partial.at[block(d), span(c)]
        there = from_left.at[block(d), span(c)]
        send, recv = r_send.at[sent_of(c, d)], r_recv.at[spot_of(c, d)]
        return remote(here, there, send, recv, me + QUAD)

    def left(c, d):
        here = partial.at[block(d), span(c)]
        there = from_right.at[block(d), span(c)]
        send, recv = l_send.at[sent_of(c, d)], l_recv.at[spot_of(c, d)]
        return remote(here, there, send, recv, me - QUAD)

    def added(c, d, way):
        (right, left)[way](c, d).wait_recv()
        landed = (from_left, from_right)[way]
        return partial[block(d), span(c)] + landed[block(d), span(c)]

    def pass_on(c, d, way):
        partial[block(d), span(c)] = added(c, d, way)
        (right, left)[way](c, d).start()

    def sends(c, way):
        if c < last:
            return half, (lambda i: half + i) if way == 0 else (lambda i: half - 1 - i)
        if way == 0:
            return line - 1, lambda i: line - 1 - i
        return line - 1, lambda i: i

    def goes(c, d, way):
        if c < last:
            return place < line - 1 if way == 0 else place > 0
        return d > place if way == 0 else d < place

    def first_sends(c, between):
        for stage in range(2):
            for way in range(2):

                @pl.when(place == (0 if way == 0 else line - 1))
                def _():
                    size, pick = sends(c, way)

                    def go(i, carry):
                        (right, left)[way](c, pick(i)).start()
                        return carry

                    lax.fori_loop(stage, size if stage else 1, go, 0)

            if stage == 0 and between is not None:
                between()

    def onward(c, i, way):
        size, pick = sends(c, way)
        inside = place > 0 if way == 0 else place < line - 1
        d = pick(i)

        @pl.when((i < size) & inside & goes(c, d, way))
        def _():
            pass_on(c, d, way)

    def weave(far, near):
        def go(nearest, i):
            if far is not None:
                onward(far, i, 1 - nearest)
            if near is not None:
                onward(near, i, nearest)

        def left_half(i, carry):
            go(0, i)
            return carry

        def right_half(i, carry):
            go(1, i)
            return carry

        top = line - 1 if last in (far, near) else half

        @pl.when(2 * place < line)
        def _():
            lax.fori_loop(0, top, left_half, 0)

        @pl.when(2 * place >= line)
        def _():
            lax.fori_loop(0, top, right_half, 0)

    def settle(c, j):
        which, start, size = chunks[c]
        d = base + j
        for head in range(size // HEAD):
            at = base_of[c] + head * HEAD
            states = partial[block(d), at : at + HEAD]
            if which < 2:
                states = (
                    states * cosine[j] + pltpu.roll(states, HEAD // 2, 1) * sine[j]
                )
            at = start + head * HEAD + (widths[1] if which == 2 else 0)
            if which == 0:
                query[j, :, at : at + HEAD] = states.astype(jnp.bfloat16)
            else:
                rows_at = rows_of(d * QUAD + quad)
                cache[rows_at, at : at + HEAD] = states.astype(jnp.bfloat16)

    def q_copy(c, j):
        which, start, size = chunks[c]
        got = query.at[j, :, pl.ds(start, size)]
        to = (base + j) * QUAD + quad
        return remote(got, got, q_send.at[0], q_recv.at[c - lead], to)

    def finish(c):
        if c == last:
            for way in range(2):

                @pl.when(place > 0 if way == 0 else place < line - 1)
                def _():
                    partial[block(place), span(c)] = added(c, place, way)

            settle(c, place - base)
            return

        @pl.when(at_end)
        def _():
            def go(i, carry):
                j = jnp.where(place == 0, half - 1 - i, i)
                d = base + j
                for way in range(2):

                    @pl.when(place == (line - 1 if way == 0 else 0))
                    def _():
                        partial[block(d), span(c)] = added(c, d, way)

                settle(c, j)
                if chunks[c][0] == 0:

                    @pl.when(d != place)
                    def _():
                        q_copy(c, j).start()

                return carry

            lax.fori_loop(0, half, go, 0)

    def tokens_ready(c, k):
        if c == 0 and share == 2:
            for at in range(k * cuts, (k + 1) * cuts):
                every = tokens.at[pl.ds(0, (line - 1) * part), pl.ds(0, slab)]
                remote(every, every, m_recv.at[at], m_recv.at[at], sib).wait_recv()

    def project(c, between=None):
        which, start, size = chunks[c]
        cols = slice(start, start + size)
        tokens_ready(c, 0)
        total = jnp.dot(
            tokens[:, columns_of(me)],
            own[which][:, cols],
            preferred_element_type=jnp.float32,
        )
        w_copy(1, c).wait_recv()
        w_copy(2, c).start()
        if c + ahead < count:
            weights_start(c + ahead)
        for k, kind in ((1, 1), (2, 0), (3, 2)):
            tokens_ready(c, k)
            if kind != 1:
                w_copy(kind, c).wait_recv()
            total += jnp.dot(
                tokens[:, columns_of(members[k])],
                held[which][kind, :, cols],
                preferred_element_type=jnp.float32,
            )
        partial[:, span(c)] = total
        first_sends(c, between)

    def kv_rows(spot, of_side=False):
        at = lax.rem(side, QUAD) if of_side else quad
        return cache.at[rows_of(spot * QUAD + at)]

    def z_copy(way, j):
        got = kv_rows(j + way * half)
        to = me - QUAD if way else me + QUAD
        return remote(got, got, z_send.at[way], z_recv.at[way, j], to)

    def y_copy(spot):
        got = kv_rows(spot)
        return remote(got, got, y_send.at[0], y_recv.at[spot], side)

    def y_arrival(spot):
        got = kv_rows(spot, True)
        return remote(got, got, y_send.at[0], y_recv.at[spot], side)

    def s_copy(spot, of_side):
        got = kv_rows(spot, of_side)
        return remote(got, got, s_send.at[0], s_recv.at[0], sib)

    def s_all():
        every = cache.at[pl.ds(0, 2 * line * tok_dev)]
        return remote(every, every, s_send.at[0], s_recv.at[0], sib)

    def kv_block(way, j, fresh):
        if not fresh:
            z_copy(way, j).wait_recv()

        @pl.when(place > 0 if way else place < line - 1)
        def _():
            z_copy(way, j).start()

        y_copy(j + way * half).start()
        s_copy(j + way * half, False).start()

    def kv_pass(way, fresh, near=None):
        def go(j, carry):
            kv_block(way, j, fresh)
            if near is not None:
                onward(near, j, 1 - way)
            return carry

        lax.fori_loop(0, half, go, 0)

    def kv_start():
        for way in range(2):

            @pl.when(place == way * (line - 1))
            def _():
                kv_pass(way, True)

    def kv_near():
        for way in range(2):
            nearer = 2 * place >= line if way else 2 * place < line

            @pl.when(nearer & jnp.logical_not(at_end))
            def _():
                kv_pass(way, False)

    def kv_far(near):
        for way in range(2):

            @pl.when(2 * place < line if way else 2 * place >= line)
            def _():
                kv_pass(way, False, near)

    def kv_side():
        def go(spot, carry):
            y_arrival(spot).wait_recv()
            s_copy(spot, True).start()
            return carry

        lax.fori_loop(0, line, go, 0)

    def kv_ready():
        s_all().wait_recv()

    def mask():
        d_all().wait()
        wanted = jnp.transpose(
            jnp.broadcast_to(doc_row[...].astype(jnp.float32), (LANES, LANES))
        )[:tok_dev]

        def go(tok, total):
            before = docs[tok].astype(jnp.float32) < wanted
            return total + jnp.where(before, 1.0, 0.0)

        total = lax.fori_loop(
            0, tok_count, go, jnp.zeros((tok_dev, LANES), jnp.float32)
        )
        since = jnp.sum(total, axis=1, keepdims=True).astype(jnp.int32)
        spot = lax.broadcasted_iota(jnp.int32, (tok_dev, keys), 0) + me * tok_dev
        at = lax.broadcasted_iota(jnp.int32, (tok_dev, keys), 1)
        bias[...] = jnp.where((at >= since) & (at <= spot), 0.0, -1e30)

    turn = math.log2(math.e) / math.sqrt(HEAD)

    def attend(g):
        heads = [
            slice((g * GROUP + h) * HEAD, (g * GROUP + h + 1) * HEAD)
            for h in range(GROUP)
        ]
        if g + lead < last:

            @pl.when(jnp.logical_not(at_end))
            def _():
                q_copy(g + lead, place - base).wait_recv()

        key = cache[:, g * HEAD : (g + 1) * HEAD]
        value = cache[:, (kv_here + g) * HEAD : (kv_here + g + 1) * HEAD]

        def scored(some):
            asked = jnp.concatenate(
                [query[place - base, :, head] for head in some], axis=0
            )
            scores = lax.dot_general(
                asked, key, (((1,), (1,)), ((), ())), preferred_element_type=jnp.float32
            )
            scores = scores.reshape(len(some), tok_dev, keys) + bias[...][None]
            return scores.reshape(len(some) * tok_dev, keys)

        def mixed_of(some, scores):
            weights = jnp.exp2((scores - jnp.max(scores, axis=1, keepdims=True)) * turn)
            totals = jnp.sum(weights, axis=1, keepdims=True)
            mixed = jnp.dot(
                weights.astype(jnp.bfloat16), value, preferred_element_type=jnp.float32
            )
            mixed = (mixed / totals).astype(jnp.bfloat16)
            for h, head in enumerate(some):
                piece = mixed[h * tok_dev : (h + 1) * tok_dev]
                out_ref[:, head] = piece
                out_mine[:, head] = jnp.max(
                    jnp.abs(piece.astype(jnp.float32)), axis=0, keepdims=True
                )

        pairs = [heads[: GROUP // 2], heads[GROUP // 2 :]]
        held_scores = [scored(some) for some in pairs]
        for some, scores in zip(pairs, held_scores):
            mixed_of(some, scores)
        cols = pl.ds(g * GROUP * HEAD, GROUP * HEAD)
        out_all[me, :, cols] = out_mine[:, cols]
        each(functools.partial(o_copy, g))

    def o_copy(g, step):
        cols = pl.ds(g * GROUP * HEAD, GROUP * HEAD)
        to = lax.rem(me + step, tok_count)
        return remote(
            out_mine.at[:, cols], out_all.at[me, :, cols], o_send.at[0], o_recv.at[0], to
        )

    def o_all():
        every = out_all.at[pl.ds(0, tok_count - 1)]
        return remote(every, every, o_send.at[0], o_recv.at[0], sib)

    def smooth():
        remote(theirs, theirs, p_send.at[0], p_recv.at[0], sib).wait()
        peak = jnp.maximum(
            jnp.maximum(mine[...], theirs[0]), jnp.maximum(theirs[1], theirs[2])
        )
        mine[...] = peak
        for i in range(rows // LANES):
            here = slice(i * LANES, (i + 1) * LANES)
            at = pl.ds(pl.multiple_of(quad * rows + i * LANES, LANES), LANES)
            channel[0, here] = as_column(mine[:, at])
            at = pl.ds(pl.multiple_of(me * rows + i * LANES, LANES), LANES)
            channel[1, here] = as_column(gain_ref[:, at])
        x_all()
        relaid_out.start()
        tiles = relaid.shape[1] // LANES

        def tallest(i, most):
            cols = pl.ds(pl.multiple_of(i * LANES, LANES), LANES)
            return jnp.maximum(most, jnp.abs(relaid[:, cols].astype(jnp.float32)))

        most = lax.fori_loop(0, tiles, tallest, jnp.zeros((sub, LANES), jnp.float32))
        weight_peak = jnp.max(most, axis=1, keepdims=True)
        ours = pl.ds(pl.multiple_of(tp * sub, 16), sub)
        factor = jnp.sqrt(jnp.maximum(channel[0, ours, :], 1e-05)) / jnp.sqrt(
            jnp.maximum(weight_peak, 1e-05)
        )
        smooth_ref[...] = factor
        channel[0, ours, :] = channel[1, ours, :] / factor

        def highest(i, carry):
            cols = pl.ds(pl.multiple_of(i * LANES, LANES), LANES)
            column[0, :, cols] = jnp.max(
                jnp.abs(smooth_ref[...] * relaid[:, cols].astype(jnp.float32)),
                axis=0,
                keepdims=True,
            )
            return carry

        lax.fori_loop(0, tiles, highest, 0)
        for i in range(-(-sub // LANES)):
            size = min(LANES, sub - i * LANES)
            start = pl.multiple_of(tp * sub + i * LANES, 16)
            tile = channel[0, pl.ds(start, size), :]
            if size < LANES:
                tile = jnp.concatenate(
                    [tile, jnp.zeros((LANES - size, LANES), jnp.float32)], axis=0
                )
            folded_ref[:, i * LANES : i * LANES + size] = jnp.transpose(tile)[
                0:1, :size
            ]
        for step in range(1, tp_count):
            c_copy(step).start()

    def c_copy(step):
        return remote(
            column.at[0],
            column_tp.at[step],
            c_send.at[0],
            c_recv.at[0],
            me,
            lax.rem(tp + step, tp_count),
        )

    def b_copy(stage):
        return remote(
            column.at[1 + stage],
            column_tp.at[tp_count + stage],
            b_send.at[stage],
            b_recv.at[stage],
            (sib, side)[stage],
        )

    def a_copy(step):
        return remote(
            column.at[3],
            column_line.at[step],
            a_send.at[0],
            a_recv.at[0],
            lax.rem(place + step, line) * QUAD + quad,
        )

    def columns_tp():
        joined = column[0]
        if tp_count > 1:
            every = column_tp.at[pl.ds(0, tp_count - 1)]
            remote(every, every, c_send.at[0], c_recv.at[0], sib).wait()
        for step in range(1, tp_count):
            joined = jnp.maximum(joined, column_tp[step])
        column[1] = joined
        b_copy(0).start()

    def columns_sib():
        b_copy(0).wait()
        column[2] = jnp.maximum(column[1], column_tp[tp_count])
        b_copy(1).start()

    def columns_side():
        b_copy(1).wait()
        column[3] = jnp.maximum(column[2], column_tp[tp_count + 1])
        for step in range(1, line):
            a_copy(step).start()

    def columns_line():
        joined = column[3]
        every = column_line.at[pl.ds(0, line - 1)]
        remote(every, every, a_send.at[0], a_recv.at[0], sib).wait()
        for step in range(1, line):
            joined = jnp.maximum(joined, column_line[step])
        scale_ref[...] = jnp.maximum(joined, 1e-05) / 127.0

    def early():
        mine[...] = jnp.max(
            jnp.abs(tokens[...].astype(jnp.float32)), axis=0, keepdims=True
        )
        for kind in range(3):
            p_copy(kind).start()

    ran = set()

    def once(act, c, *rest):
        if c <= last and (act, c) not in ran:
            ran.add((act, c))
            act(c, *rest)

    def pair(far, near):
        far = None if far > last or ("far", far) in ran else far
        near = None if near > last or ("near", near) in ran else near
        ran.update({("far", far), ("near", near)})
        if far is not None or near is not None:
            weave(far, near)

    def split_project(c, ends, between=None):
        @pl.when(at_end if ends else jnp.logical_not(at_end))
        def _():
            project(c, between)

    once(project, 0)
    early()
    for which in (1, 2, 0):
        for step in range(tp_count):
            x_copy(which, step).start()
    for c in range(1, lead):
        once(project, c)
    for c in range(lead):
        pair(c - 1 if c else FAR, c)
    once(project, lead)
    once(finish, kv_chunks[0])
    pair(lead - 1, lead)
    once(project, lead + 1)
    for c in kv_chunks:
        once(finish, c)
    kv_start()
    mask()
    pair(lead, lead + 1)
    smooth()
    once(project, lead + 2)
    due = functools.partial(once, finish, lead) if lead < last - 1 else None
    if lead + 3 <= last:
        split_project(lead + 3, True, due)
    elif due is not None:
        due()
    pair(lead + 1, FAR)
    if lead + 1 < last - 1:
        once(finish, lead + 1)
    kv_near()
    if lead + 3 <= last:
        split_project(lead + 3, False)
        ran.add((project, lead + 3))
    if lead + 2 < last:
        ran.add(("near", lead + 2))
        kv_far(lead + 2)
    else:
        kv_far(None)
    columns_tp()
    for c in range(lead, count):
        once(project, c)
        pair(c - 1, c)
    kv_side()
    columns_sib()
    kv_ready()
    if lead == last:
        pair(last, FAR)
    swap = last - 1 > lead

    def attend_where(g, ends):
        @pl.when(at_end if ends else jnp.logical_not(at_end))
        def _():
            attend(g)

    for c in range(lead, count):
        if lead < c == last - 2:
            once(finish, last - 1)
        once(finish, c)
        if swap and c == last - 1:
            attend_where(c - lead, True)
        else:
            attend(c - lead)
        if c == lead:
            pair(last, FAR)
            columns_side()
    if swap:
        attend_where(last - 1 - lead, False)
    columns_line()
    o_all().wait()
    out_peak_ref[...] = jnp.max(out_all[...], axis=0)

    tokens_sent(t_send.at[0])
    if share == 2:
        tokens_sent(m_send.at[0])
    for which in range(3):
        every = held[which]
        remote(every, every, w_send.at[which], w_send.at[which], sib).wait_send()
    for way in range(2):
        moves = place > 0 if way else place < line - 1

        @pl.when(moves)
        def _():
            sems = (r_send, l_send)[way]
            for c in range(last):
                every = partial.at[pl.ds(0, half * tok_dev), span(c)]
                remote(every, every, sems.at[c], sems.at[c], sib).wait_send()
            every = cache.at[pl.ds(0, half * tok_dev)]
            remote(every, every, z_send.at[way], z_send.at[way], sib).wait_send()

        def sent(d, carry):
            @pl.when(d < place if way else d > place)
            def _():
                (right, left)[way](last, d).wait_send()

            return carry

        lax.fori_loop(0, line, sent, 0)
    if last > lead and half > 1:

        @pl.when(at_end)
        def _():
            every = query.at[
                pl.ds(0, half - 1), :, pl.ds(0, (last - lead) * GROUP * HEAD)
            ]
            remote(every, every, q_send.at[0], q_send.at[0], sib).wait_send()

    s_all().wait_send()
    every = cache.at[pl.ds(0, line * tok_dev)]
    remote(every, every, y_send.at[0], y_send.at[0], sib).wait_send()
    relaid_out.wait()


def calibrate(hidden, gain, doc_row, matrices):
    tok_count, tp_count = lax.axis_size("tok"), lax.axis_size("tp")
    line = tok_count // QUAD
    tok_dev, depth = hidden.shape
    rows = matrices[0].shape[0]
    sub = rows // tp_count
    widths = [matrix.shape[1] for matrix in matrices]
    chunks = column_chunks(widths)
    count = len(chunks)
    total = sum(widths)
    share = 2 if tp_count % 2 == 0 and tok_dev % 32 == 0 else 1
    vmem = pl.BlockSpec(memory_space=pltpu.VMEM)
    dma = pltpu.SemaphoreType.DMA
    f32, bf16 = jnp.float32, jnp.bfloat16
    queries = widths[0] // (GROUP * HEAD)
    lanes = tok_dev + -tok_dev % LANES
    return pl.pallas_call(
        functools.partial(main_kernel, chunks, line, tp_count, share),
        out_shape=(
            jax.ShapeDtypeStruct((tok_dev, widths[0]), bf16),
            jax.ShapeDtypeStruct((1, widths[0]), f32),
            jax.ShapeDtypeStruct((1, total * tp_count), f32),
            jax.ShapeDtypeStruct((1, sub), f32),
            jax.ShapeDtypeStruct((sub, LANES), f32),
            jax.ShapeDtypeStruct((sub, total * tp_count), bf16),
        ),
        in_specs=[pl.BlockSpec(memory_space=pl.ANY)] * 6,
        out_specs=(vmem,) * 5 + (pl.BlockSpec(memory_space=pl.ANY),),
        scratch_shapes=[
            pltpu.VMEM((tok_dev, depth), bf16),
            pltpu.VMEM((tok_dev, LANES), f32),
            pltpu.VMEM((line // 2, tok_dev, HEAD), f32),
            pltpu.VMEM((line // 2, tok_dev, HEAD), f32),
            pltpu.VMEM((1, lanes), jnp.int32),
            pltpu.VMEM((tok_count, 1, lanes), jnp.int32),
            pltpu.VMEM((tok_dev, tok_dev * tok_count), f32),
            pltpu.VMEM((line * tok_dev, QUAD * rows), bf16),
            pltpu.VMEM((1, QUAD * rows), f32),
            pltpu.VMEM((3, 1, QUAD * rows), f32),
        ]
        + [pltpu.VMEM(array.shape, array.dtype) for array in (hidden, gain, doc_row)]
        + [pltpu.VMEM((rows, width), bf16) for width in widths]
        + [pltpu.VMEM((3, rows, width), bf16) for width in widths]
        + [pltpu.VMEM((line * tok_dev, total), f32)] * 3
        + [
            pltpu.VMEM((line // 2, tok_dev, widths[0]), bf16),
            pltpu.VMEM((tok_dev * tok_count, widths[1] + widths[2]), bf16),
            pltpu.VMEM((sub, total * tp_count), bf16),
            pltpu.VMEM((2, rows, LANES), f32),
            pltpu.VMEM((4, 1, total * tp_count), f32),
            pltpu.VMEM((tp_count + 2, 1, total * tp_count), f32),
            pltpu.VMEM((line, 1, total * tp_count), f32),
            pltpu.VMEM((1, widths[0]), f32),
            pltpu.VMEM((tok_count, 1, widths[0]), f32),
        ]
        + [dma((6,)), dma((3,)), dma((3, count))]
        + [dma((1,)), dma((line, 2 * QUAD)), dma((1,)), dma((2 * QUAD,))]
        + [dma((1,))] * 2
        + [dma((2,))]
        + [dma((count - 1 + line,)), dma(((count - 1) * (line // 2) + line,))] * 2
        + [dma((1,))] * 4
        + [dma((2,)), dma((2, line // 2))]
        + [dma((1,)), dma((line,))]
        + [dma((1,))] * 2
        + [dma((1,)), dma((queries,))]
        + [dma((1,))] * 2
        + [dma((2,))] * 2
        + [dma((1,))] * 4,
        compiler_params=pltpu.CompilerParams(
            collective_id=0, has_side_effects=True, vmem_limit_bytes=63 * 1024 * 1024
        ),
    )(hidden, gain, doc_row, *matrices)


def codes_kernel(
    widths,
    tp_count,
    relaid_ref,
    smooth_ref,
    scale_ref,
    attended_ref,
    peak_ref,
    folded_ref,
    cq_ref,
    ck_ref,
    cv_ref,
    sq_ref,
    sk_ref,
    sv_ref,
    out_ref,
    out_peak_ref,
    out_folded_ref,
    inverse,
):
    tp = lax.axis_index("tp")

    @pl.when(pl.program_id(0) == 0)
    def _():
        out_ref[...] = attended_ref[...]
        out_peak_ref[...] = peak_ref[...]
        out_folded_ref[...] = folded_ref[...]
        inverse[...] = 1.0 / scale_ref[...]
        for which, ref in enumerate((sq_ref, sk_ref, sv_ref)):
            base = sum(widths[:which]) * tp_count + tp * widths[which]
            ref[...] = scale_ref[:, pl.ds(pl.multiple_of(base, 128), widths[which])]

    factor = smooth_ref[...]
    for which, ref in enumerate((cq_ref, ck_ref, cv_ref)):
        base = sum(widths[:which]) * tp_count
        for at in range(0, widths[which] * tp_count, LANES):
            cols = slice(base + at, base + at + LANES)
            ref[:, at : at + LANES] = (
                factor * relaid_ref[:, cols].astype(jnp.float32) * inverse[:, cols]
            )


def coded(relaid, smooth, scale, attended, peak, folded, widths, tp_count):
    sub, total = relaid.shape
    block = math.gcd(sub, 128)
    f32 = jnp.float32

    def striped(width):
        return pl.BlockSpec((block, width), lambda i: (i, 0))

    def whole(array):
        return pl.BlockSpec(array.shape, lambda i: (0, 0))

    full = [jax.ShapeDtypeStruct((sub, width * tp_count), f32) for width in widths]
    part = [jax.ShapeDtypeStruct((1, width), f32) for width in widths]
    rest = [
        jax.ShapeDtypeStruct(array.shape, array.dtype)
        for array in (attended, peak, folded)
    ]
    return pl.pallas_call(
        functools.partial(codes_kernel, widths, tp_count),
        grid=(sub // block,),
        out_shape=full + part + rest,
        in_specs=[striped(total), striped(LANES)]
        + [whole(array) for array in (scale, attended, peak, folded)],
        out_specs=[striped(width * tp_count) for width in widths]
        + [whole(array) for array in part + rest],
        scratch_shapes=[pltpu.VMEM((1, total), f32)],
    )(relaid, smooth, scale, attended, peak, folded)


def on_device(hidden, norm_gain, w_query, w_key, w_value, doc_ids):
    matrices = (w_query, w_key, w_value)
    attended, peak, scale, folded, smooth, relaid = calibrate(
        hidden, norm_gain[None], doc_ids[None], matrices
    )
    *rows, attended, peak, folded = coded(
        relaid,
        smooth,
        scale,
        attended,
        peak,
        folded,
        [matrix.shape[1] for matrix in matrices],
        lax.axis_size("tp"),
    )
    scales = [row[0] for row in rows[3:]]
    return (attended, peak[0], folded[0], *rows[:3], *scales)


def solution(mesh):
    in_specs = (P("tok", None), P(), P("tok", "tp"), P("tok", "tp"), P("tok", "tp"), P("tok"))
    out_specs = (
        P("tok", "tp"),
        P("tp"),
        P(("tok", "tp")),
        P(("tok", "tp"), None),
        P(("tok", "tp"), None),
        P(("tok", "tp"), None),
        P("tp"),
        P("tp"),
        P("tp"),
    )
    return jax.shard_map(
        on_device, mesh=mesh, in_specs=in_specs, out_specs=out_specs, check_vma=False
    )
```
